32 devices in a mesh: node: 4 (over z), local: 8 (over y, x, core).
Axes of the slice: x: 2, y: 2, z: 4, core: 2. Of those that a mesh axis runs over, the one named last changes fastest.
Arguments:
- x: bfloat16 [64, 128, 512], P(('node', 'local'))
- y_cot: bfloat16 [64, 128, 512], P(('node', 'local'))
- ln1_gain: bfloat16 [2, 512], P(None, ('node', 'local'))
- ln1_bias: bfloat16 [2, 512], P(None, ('node', 'local'))
- qkv_weight: bfloat16 [2, 512, 8, 192], P(None, ('node', 'local'))
- qkv_bias: bfloat16 [2, 1536], P(None, ('node', 'local'))
- out_weight: bfloat16 [2, 512, 512], P(None, ('node', 'local'))
- out_bias: bfloat16 [2, 512], P(None, ('node', 'local'))
- ln2_gain: bfloat16 [2, 512], P(None, ('node', 'local'))
- ln2_bias: bfloat16 [2, 512], P(None, ('node', 'local'))
- up_weight: bfloat16 [2, 512, 2048], P(None, ('node', 'local'))
- up_bias: bfloat16 [2, 2048], P(None, ('node', 'local'))
- down_weight: bfloat16 [2, 2048, 512], P(None, ('node', 'local'))
- down_bias: bfloat16 [2, 512], P(None, ('node', 'local'))
Outputs:
- output 1: bfloat16 [64, 128, 512], P(('node', 'local'))
- output 2: bfloat16 [64, 128, 512], P(('node', 'local'))
- output 3: bfloat16 [2, 512], P(None, ('node', 'local'))
- output 4: bfloat16 [2, 512], P(None, ('node', 'local'))
- output 5: bfloat16 [2, 512, 8, 192], P(None, ('node', 'local'))
- output 6: bfloat16 [2, 1536], P(None, ('node', 'local'))
- output 7: bfloat16 [2, 512, 512], P(None, ('node', 'local'))
- output 8: bfloat16 [2, 512], P(None, ('node', 'local'))
- output 9: bfloat16 [2, 512], P(None, ('node', 'local'))
- output 10: bfloat16 [2, 512], P(None, ('node', 'local'))
- output 11: bfloat16 [2, 512, 2048], P(None, ('node', 'local'))
- output 12: bfloat16 [2, 2048], P(None, ('node', 'local'))
- output 13: bfloat16 [2, 2048, 512], P(None, ('node', 'local'))
- output 14: bfloat16 [2, 512], P(None, ('node', 'local'))
All inputs are finite; a program needn't handle non-finite values.
Results may differ from the reference program's by a relative error of at most 0.017538.
Values are sent between devices in bfloat16 or wider.
A program may use at most 1 GiB of HBM per device.

```python
import jax
import jax.numpy as jnp
from jax import lax

D_MODEL = 512
HEADS = 8
SEQ_LEN = 128
BATCH = 64
LAYERS = 2
HEAD_DIM = D_MODEL // HEADS
ROT_DIM = HEAD_DIM // 4
FF_DIM = 4 * D_MODEL
EPSILON = 1e-5


def slow_waves(rng_key, frequencies):
    amp_key, phase_key = jax.random.split(rng_key)
    positions = jnp.arange(SEQ_LEN, dtype=jnp.float32)[None, :, None] / SEQ_LEN
    wave_sum = jnp.zeros((BATCH, SEQ_LEN, D_MODEL), jnp.float32)
    for wave_idx, frequency in enumerate(frequencies):
        amplitude = jax.random.normal(jax.random.fold_in(amp_key, wave_idx), (BATCH, 1, D_MODEL), jnp.float32)
        phase_off = jax.random.uniform(jax.random.fold_in(phase_key, wave_idx), (BATCH, 1, D_MODEL), jnp.float32, 0.0, 6.283185307179586)
        wave_sum = wave_sum + amplitude * jnp.cos(6.283185307179586 * frequency * positions + phase_off)
    return wave_sum * (2.0 / len(frequencies)) ** 0.5


def normal_draw(rng_key, out_shape, spread, offset=0.0):
    return (offset + spread * jax.random.normal(rng_key, out_shape, jnp.float32)).astype(jnp.bfloat16)


def setup_inputs(seed: int = 0) -> dict:
    sub_keys = jax.random.split(jax.random.key(seed), 16)
    white_noise = jax.random.normal(sub_keys[0], (BATCH, SEQ_LEN, D_MODEL), jnp.float32)
    x = (0.8 * slow_waves(sub_keys[1], (0.5, 1.0, 2.0, 3.0)) + 0.6 * white_noise).astype(jnp.bfloat16)
    y_cot = normal_draw(sub_keys[2], (BATCH, SEQ_LEN, D_MODEL), (BATCH * SEQ_LEN) ** -0.25)
    width_scale = D_MODEL ** -0.5
    return {
        'x': x,
        'y_cot': y_cot,
        'ln1_gain': normal_draw(sub_keys[3], (LAYERS, D_MODEL), 0.25, 1.0),
        'ln1_bias': normal_draw(sub_keys[4], (LAYERS, D_MODEL), 0.25),
        'qkv_weight': normal_draw(sub_keys[5], (LAYERS, D_MODEL, HEADS, 3 * HEAD_DIM), width_scale),
        'qkv_bias': normal_draw(sub_keys[6], (LAYERS, 3 * D_MODEL), 0.3),
        'out_weight': normal_draw(sub_keys[7], (LAYERS, D_MODEL, D_MODEL), 1.5 * width_scale),
        'out_bias': normal_draw(sub_keys[8], (LAYERS, D_MODEL), 0.3),
        'ln2_gain': normal_draw(sub_keys[9], (LAYERS, D_MODEL), 0.25, 1.0),
        'ln2_bias': normal_draw(sub_keys[10], (LAYERS, D_MODEL), 0.25),
        'up_weight': normal_draw(sub_keys[11], (LAYERS, D_MODEL, FF_DIM), width_scale),
        'up_bias': normal_draw(sub_keys[12], (LAYERS, FF_DIM), 0.3),
        'down_weight': normal_draw(sub_keys[13], (LAYERS, FF_DIM, D_MODEL), FF_DIM ** -0.5),
        'down_bias': normal_draw(sub_keys[14], (LAYERS, D_MODEL), 0.3),
    }


def to_bf16(values):
    return values.astype(jnp.bfloat16).astype(jnp.float32)


def rope_tables():
    inv_freq = 1.0 / (10000.0 ** (jnp.arange(0, ROT_DIM, 2, dtype=jnp.float32) / ROT_DIM))
    angles = jnp.arange(SEQ_LEN, dtype=jnp.float32)[:, None] * inv_freq[None, :]
    angles = jnp.concatenate([angles, angles], axis=-1)
    return jnp.cos(angles), jnp.sin(angles)


def apply_rotary(vectors, cos_tab, sin_tab):
    half_dim = ROT_DIM // 2
    rot_part = vectors[..., :ROT_DIM]
    pass_part = vectors[..., ROT_DIM:]
    turned = jnp.concatenate([-rot_part[..., half_dim:], rot_part[..., :half_dim]], axis=-1)
    rot_part = rot_part * cos_tab[:, None, :] + turned * sin_tab[:, None, :]
    return jnp.concatenate([rot_part, pass_part], axis=-1)


def layer_norm(hidden, ln_gain, ln_bias):
    center = hidden - jnp.mean(hidden, axis=-1, keepdims=True)
    variance = jnp.mean(center * center, axis=-1, keepdims=True)
    return center * lax.rsqrt(variance + EPSILON) * ln_gain + ln_bias


def layer_forward(hidden, weights, cos_tab, sin_tab):
    (ln1_gain, ln1_bias, qkv_weight, qkv_bias, out_weight, out_bias,
     ln2_gain, ln2_bias, up_weight, up_bias, down_weight, down_bias) = weights
    normed_attn = to_bf16(layer_norm(hidden, ln1_gain, ln1_bias))
    normed_mlp = to_bf16(layer_norm(hidden, ln2_gain, ln2_bias))
    qkv_all = jnp.einsum('sd,dhe->she', normed_attn, qkv_weight) + qkv_bias.reshape(HEADS, 3 * HEAD_DIM)
    query_rot = to_bf16(apply_rotary(qkv_all[..., :HEAD_DIM], cos_tab, sin_tab))
    key_rot = to_bf16(apply_rotary(qkv_all[..., HEAD_DIM:2 * HEAD_DIM], cos_tab, sin_tab))
    values = to_bf16(qkv_all[..., 2 * HEAD_DIM:])
    scores = jnp.einsum('qhd,khd->hqk', query_rot, key_rot) * HEAD_DIM ** -0.5
    causal = jnp.arange(SEQ_LEN)[:, None] >= jnp.arange(SEQ_LEN)[None, :]
    scores = jnp.where(causal[None], scores, -1e30)
    attn_probs = to_bf16(jax.nn.softmax(scores, axis=-1))
    context = to_bf16(jnp.einsum('hqk,khd->qhd', attn_probs, values))
    attn_out = jnp.einsum('qhd,hde->qe', context, out_weight.reshape(HEADS, HEAD_DIM, D_MODEL)) + out_bias
    mlp_act = to_bf16(jax.nn.gelu(jnp.dot(normed_mlp, up_weight) + up_bias, approximate=False))
    mlp_out = jnp.dot(mlp_act, down_weight) + down_bias
    return hidden + attn_out + mlp_out


def reference(x, y_cot, ln1_gain, ln1_bias, qkv_weight, qkv_bias, out_weight, out_bias,
              ln2_gain, ln2_bias, up_weight, up_bias, down_weight, down_bias):
    stacked = tuple(tensor.astype(jnp.float32) for tensor in (
        ln1_gain, ln1_bias, qkv_weight, qkv_bias, out_weight, out_bias,
        ln2_gain, ln2_bias, up_weight, up_bias, down_weight, down_bias))
    cos_tab, sin_tab = rope_tables()

    def both_layers(x_seq, params):
        hidden = x_seq
        for layer_idx in range(LAYERS):
            hidden = to_bf16(layer_forward(hidden, [tensor[layer_idx] for tensor in params], cos_tab, sin_tab))
        return hidden

    def seq_step(grad_sums, seq_pair):
        x_seq, cot_seq = seq_pair
        seq_out, pullback = jax.vjp(both_layers, x_seq.astype(jnp.float32), stacked)
        x_bar, param_bars = pullback(cot_seq.astype(jnp.float32))
        grad_sums = tuple(grad_sum + part_grad for grad_sum, part_grad in zip(grad_sums, param_bars))
        return grad_sums, (seq_out.astype(jnp.bfloat16), x_bar.astype(jnp.bfloat16))

    zero_sums = tuple(jnp.zeros_like(tensor) for tensor in stacked)
    grad_sums, (y_out, x_grad) = lax.scan(seq_step, zero_sums, (x, y_cot))
    grad_list = [grad_sum.astype(jnp.bfloat16) for grad_sum in grad_sums]
    return (y_out, x_grad, grad_list[0], grad_list[1], grad_list[2], grad_list[3], grad_list[4], grad_list[5],
            grad_list[6], grad_list[7], grad_list[8], grad_list[9], grad_list[10], grad_list[11])
```

```python
import functools
import jax
import jax.numpy as jnp
from jax import lax
from jax.experimental import pallas as pl
from jax.experimental.pallas import tpu as pltpu
from jax.sharding import PartitionSpec as P

EPSILON = 1e-5
MESH = pl.DeviceIdType.MESH
LAYERS = 2
ROWS = 16
SMALL = 16


def positions():
    z = lax.axis_index('node')
    l = lax.axis_index('local')
    c = l % 2
    x = (l // 2) % 2
    y = l // 4
    partner = (z, l + 1 - 2 * c)
    x_nbr = (z, l + 2 - 4 * x)
    y_nbr = (z, (l + 4) % 8)
    z_others = [z + 1 - 2 * (z % 2), (z + 2) % 4, 3 - z]
    return z, l, c, x, y, partner, x_nbr, y_nbr, z_others


def entry_barrier(pos):
    z, l, c, x, y, partner, x_nbr, y_nbr, z_others = pos
    barrier = pltpu.get_barrier_semaphore()
    for dev in [partner, x_nbr, y_nbr] + [(zo, l) for zo in z_others]:
        pl.semaphore_signal(barrier, inc=1, device_id=dev, device_id_type=MESH)
    pl.semaphore_wait(barrier, 6)


class Copies:
    def __init__(self, send_sems, recv_sems):
        self.send_sems, self.recv_sems, self.used = send_sems, recv_sems, 0
        self.open_sends = []

    def make(self, src, dst, dev):
        idx = self.used
        self.used += 1
        return pltpu.make_async_remote_copy(src_ref=src, dst_ref=dst, send_sem=self.send_sems.at[idx],
                                            recv_sem=self.recv_sems.at[idx], device_id=dev, device_id_type=MESH)

    def start(self, src, dst, dev):
        copy = self.make(src, dst, dev)
        copy.start()
        self.open_sends.append(copy)
        return copy

    def finish(self):
        for copy in self.open_sends:
            copy.wait_send()
        self.open_sends = []


def small_reduce_steps(copies, pos, src, bufs, out):
    z, l, c, x, y, partner, x_nbr, y_nbr, z_others = pos
    held = src
    for step, dev in enumerate((partner, x_nbr, y_nbr)):
        copy = copies.start(held, bufs.at[2 * step], dev)
        yield
        copy.wait_recv()
        bufs[2 * step + 1] = held[...] + bufs[2 * step]
        held = bufs.at[2 * step + 1]
    sends = [copies.start(held, bufs.at[6 + k], (zo, l)) for k, zo in enumerate(z_others)]
    yield
    for copy in sends:
        copy.wait_recv()
    out[...] = (held[...] + bufs[6]) + (bufs[7] + bufs[8])
    yield


def gather_steps(copies, pos, own, full, lo, width):
    z, l, c, x, y, partner, x_nbr, y_nbr, z_others = pos
    half = width // 2
    cols, cols_a, cols_b = pl.ds(lo, width), pl.ds(lo, half), pl.ds(lo + half, half)
    z_order = [z] + z_others

    def block(zz, yy, xx, cc):
        return full.at[zz, yy, xx, cc, :, cols]

    def column(yy, xx):
        return full.at[:, yy, xx, c, :, cols]

    mine, own_cols = block(z, y, x, c), own.at[:, cols]
    from_z, from_x, from_y, diag = [None] * 4, [None] * 4, [None] * 4, []
    from_x[0] = copies.start(own_cols, mine, x_nbr)
    from_y[0] = copies.start(own_cols, mine, y_nbr)
    for k in (1, 2, 3):
        from_z[k] = copies.start(own_cols, mine, (z_order[k], l))
    full[z, y, x, c, :, cols] = own[:, cols]
    yield
    to_partner = []

    def forward_cross(k):
        zz = z_order[k]
        from_x[k].wait_recv()
        got = full.at[zz, y, 1 - x, c, :, cols_a]
        diag.append(copies.start(got, got, y_nbr))
        from_y[k].wait_recv()
        got = full.at[zz, 1 - y, x, c, :, cols_b]
        diag.append(copies.start(got, got, x_nbr))

    def forward_z(k):
        from_z[k].wait_recv()
        got = block(z_order[k], y, x, c)
        from_x[k] = copies.start(got, got, x_nbr)
        from_y[k] = copies.start(got, got, y_nbr)

    def forward_partner(yy, xx):
        got = column(yy, xx)
        to_partner.append(copies.start(got, got, partner))

    forward_z(1)
    yield
    forward_cross(0)
    yield
    forward_z(2)
    yield
    forward_z(3)
    forward_partner(y, x)
    yield
    for k in (1, 2, 3):
        forward_cross(k)
        yield
    forward_partner(y, 1 - x)
    forward_partner(1 - y, x)
    for copy in diag:
        copy.wait_recv()
    forward_partner(1 - y, 1 - x)
    yield
    for copy in to_partner:
        copy.wait_recv()
    yield


def scatter_chunk_steps(copies, pos, grads, part0, partx, party, last, partz, out, lo, width):
    z, l, c, x, y, partner, x_nbr, y_nbr, z_others = pos
    half = width // 2
    cols, cols_a, cols_b = pl.ds(lo, width), pl.ds(lo, half), pl.ds(lo + half, half)
    hcols = pl.ds(lo // 2, half)
    swap = copies.make(grads.at[:, :, :, 1 - c, :, cols], part0.at[:, :, :, :, cols], partner)
    swap.start()
    yield
    swap.wait()
    part0[:, :, :, :, cols] = part0[:, :, :, :, cols] + grads[:, :, :, c, :, cols]
    send_a = copies.start(part0.at[:, :, 1 - x, :, cols_a], partx.at[:, :, :, hcols], x_nbr)
    send_b = copies.start(part0.at[:, 1 - y, :, :, cols_b], party.at[:, :, :, hcols], y_nbr)
    yield
    send_a.wait_recv()
    partx[:, :, :, hcols] = partx[:, :, :, hcols] + part0[:, :, x, :, cols_a]
    send_a = copies.start(partx.at[:, 1 - y, :, hcols], last.at[:, :, cols_a], y_nbr)
    send_b.wait_recv()
    party[:, :, :, hcols] = party[:, :, :, hcols] + part0[:, y, :, :, cols_b]
    send_b = copies.start(party.at[:, 1 - x, :, hcols], last.at[:, :, cols_b], x_nbr)
    yield
    send_a.wait_recv()
    send_b.wait_recv()
    last[:, :, cols_a] = last[:, :, cols_a] + partx[:, y, :, hcols]
    last[:, :, cols_b] = last[:, :, cols_b] + party[:, x, :, hcols]
    sends = [copies.start(last.at[zo, :, cols], partz.at[k, :, cols], (zo, l)) for k, zo in enumerate(z_others)]
    yield
    for copy in sends:
        copy.wait_recv()
    total = (last[z, :, cols] + partz[0, :, cols]) + (partz[1, :, cols] + partz[2, :, cols])
    out[:, cols] = total.astype(out.dtype)
    yield


class ScatterQueue:
    def __init__(self):
        self.waiting = [[], [], [], []]

    def add(self, chunk):
        next(chunk)
        self.waiting[0].append(chunk)

    def pump(self, *stages):
        for stage in stages:
            if self.waiting[stage]:
                chunk = self.waiting[stage].pop(0)
                next(chunk)
                if stage < 3:
                    self.waiting[stage + 1].append(chunk)

    def drain(self, lag, between):
        while any(self.waiting):
            next(between, None)
            for stage in range(4):
                if len(self.waiting[stage]) >= lag or not any(self.waiting[:stage]):
                    self.pump(stage)


def dot(first, second):
    return lax.dot_general(first, second, (((1,), (0,)), ((), ())), preferred_element_type=jnp.float32)


def dot_bt(first, second):
    return lax.dot_general(first, second, (((1,), (1,)), ((), ())), preferred_element_type=jnp.float32)


def dot_at(first, second):
    return lax.dot_general(first, second, (((0,), (0,)), ((), ())), preferred_element_type=jnp.float32)


WIDE = 512
PAIR = 128
SEQ = 128
OUT, UP, DOWN = 3 * WIDE, 4 * WIDE, 8 * WIDE


def normalised(hidden32):
    center = hidden32 - jnp.mean(hidden32, axis=-1, keepdims=True)
    rstd = lax.rsqrt(jnp.mean(center * center, axis=-1, keepdims=True) + EPSILON)
    return center * rstd, rstd


def weight(full, layer, lo, width=WIDE):
    return full[layer, :, :, :, :, :, lo:lo + width].reshape(WIDE, width)


def rotate(piece, tabs):
    cos_t, up_t, down_t = tabs
    return piece * cos_t[...] + pltpu.roll(piece, PAIR - 8, 1) * up_t[...] + pltpu.roll(piece, 8, 1) * down_t[...]


def rotate_back(piece, tabs):
    cos_t, up_t, down_t = tabs
    return piece * cos_t[...] + pltpu.roll(piece * up_t[...], 8, 1) + pltpu.roll(piece * down_t[...], PAIR - 8, 1)


def first_head():
    return lax.broadcasted_iota(jnp.int32, (SEQ, PAIR), 1) < PAIR // 2


def head_masks():
    first = first_head()
    return (jnp.where(first, 1.0, 0.0).astype(jnp.bfloat16), jnp.where(first, 0.0, 1.0).astype(jnp.bfloat16))


def attention_blocks(tokens):
    for s in range(tokens // SEQ):
        for j in range(WIDE // PAIR):
            yield s, j, pl.ds(s * SEQ, SEQ), pl.ds(j * PAIR, PAIR)


def layer_forward(layer, hidden, full, small, tabs, saved, hooks):
    n1, n2, qkv, probs, ctx, slope, act = saved
    tokens = hidden.shape[0]

    def vec(row):
        return small[pl.ds(layer * SMALL + row, 1), :]

    hidden32 = hidden[...].astype(jnp.float32)
    scaled, _ = normalised(hidden32)
    n1[...] = (scaled * vec(0) + vec(1)).astype(jnp.bfloat16)
    n2[...] = (scaled * vec(3) + vec(4)).astype(jnp.bfloat16)
    hooks('norm')
    for t in range(3):
        part = dot(n1[...], weight(full, layer, t * WIDE)) + vec(10 + t)
        for j in range(WIDE // PAIR):
            piece = part[:, j * PAIR:(j + 1) * PAIR]
            if t < 2:
                piece = rotate(piece, tabs)
            qkv[t, :, j * PAIR:(j + 1) * PAIR] = piece.astype(jnp.bfloat16)
    hooks('qkv')
    causal = (lax.broadcasted_iota(jnp.int32, (SEQ, SEQ), 0) >= lax.broadcasted_iota(jnp.int32, (SEQ, SEQ), 1))
    masks, first = head_masks(), first_head()
    for s, j, rows, cols in attention_blocks(tokens):
        query, key, value = qkv[0, rows, cols], qkv[1, rows, cols], qkv[2, rows, cols]
        heads = []
        for h in range(2):
            scores = dot_bt(query * masks[h], key) * 0.125
            scores = jnp.where(causal, scores, -1e30)
            weights = jnp.exp(scores - jnp.max(scores, axis=-1, keepdims=True))
            weights = weights / jnp.sum(weights, axis=-1, keepdims=True)
            probs[s, j, h] = weights
            heads.append(dot(weights.astype(jnp.bfloat16), value))
        ctx[rows, cols] = jnp.where(first, heads[0], heads[1]).astype(jnp.bfloat16)
        if j == 3:
            hooks('attn')
    total = hidden32 + (dot(ctx[...], weight(full, layer, OUT)) + vec(2))
    hooks('out')
    mlp = None
    for k in range(4):
        pre = dot(n2[...], weight(full, layer, UP + k * WIDE)) + vec(6 + k)
        bell = lax.erf(pre * 0.7071067811865476) + 1.0
        act[:, k * WIDE:(k + 1) * WIDE] = (0.5 * pre * bell).astype(jnp.bfloat16)
        slope[:, k * WIDE:(k + 1) * WIDE] = 0.5 * bell + pre * (jnp.exp(-0.5 * pre * pre) * 0.3989422804014327)
        term = dot(act[:, k * WIDE:(k + 1) * WIDE], weight(full, layer, DOWN + k * WIDE))
        mlp = term if mlp is None else mlp + term
        hooks('mlp')
    return (total + (mlp + vec(5))).astype(jnp.bfloat16)


def layer_backward(layer, hidden, d_out, full, small, tabs, saved, grads, small_grads, hooks):
    n1, n2, qkv, probs, ctx, slope, act = saved
    tokens = hidden.shape[0]

    def vec(row):
        return small[pl.ds(layer * SMALL + row, 1), :]

    def put_small(row, value):
        small_grads[pl.ds(layer * SMALL + row, 1), :] = jnp.sum(value, axis=0, keepdims=True)

    def put(lo, value):
        grads[:, :, :, :, :, lo:lo + WIDE] = value.reshape(grads.shape[:5] + (WIDE,))

    d_out32 = d_out[...].astype(jnp.float32)
    put_small(2, d_out32)
    put_small(5, d_out32)
    for k in range(4):
        put(DOWN + k * WIDE, dot_at(act[:, k * WIDE:(k + 1) * WIDE], d_out[...]))
        if k % 2:
            hooks('down', DOWN + (k - 1) * WIDE)
    d_n2 = None
    for k in range(4):
        d_act = dot_bt(d_out[...], weight(full, layer, DOWN + k * WIDE)).astype(jnp.bfloat16)
        d_pre = d_act.astype(jnp.float32) * slope[:, k * WIDE:(k + 1) * WIDE]
        put_small(6 + k, d_pre)
        act[:, k * WIDE:(k + 1) * WIDE] = d_pre.astype(jnp.bfloat16)
        d_pre_bf = act[:, k * WIDE:(k + 1) * WIDE]
        put(UP + k * WIDE, dot_at(n2[...], d_pre_bf))
        term = dot_bt(d_pre_bf, weight(full, layer, UP + k * WIDE))
        d_n2 = term if d_n2 is None else d_n2 + term
        if k % 2:
            hooks('up', UP + (k - 1) * WIDE)
    d_n2 = d_n2.astype(jnp.bfloat16)
    put(OUT, dot_at(ctx[...], d_out[...]))
    ctx[...] = dot_bt(d_out[...], weight(full, layer, OUT)).astype(jnp.bfloat16)
    hooks('dctx')
    masks, first = head_masks(), first_head()
    for s, j, rows, cols in attention_blocks(tokens):
        query, key, value = qkv[0, rows, cols], qkv[1, rows, cols], qkv[2, rows, cols]
        d_ctx = ctx[rows, cols]
        d_q, d_k, d_v = [], [], []
        for h in range(2):
            weights = probs[s, j, h]
            d_probs = dot_bt(d_ctx * masks[h], value).astype(jnp.bfloat16).astype(jnp.float32)
            d_v.append(dot_at(weights.astype(jnp.bfloat16), d_ctx))
            inner = jnp.sum(d_probs * weights, axis=-1, keepdims=True)
            d_scores = (weights * (d_probs - inner) * 0.125).astype(jnp.bfloat16)
            d_q.append(dot(d_scores, key))
            d_k.append(dot_at(d_scores, query))
        qkv[0, rows, cols] = jnp.where(first, d_q[0], d_q[1]).astype(jnp.bfloat16)
        qkv[1, rows, cols] = jnp.where(first, d_k[0], d_k[1]).astype(jnp.bfloat16)
        qkv[2, rows, cols] = jnp.where(first, d_v[0], d_v[1]).astype(jnp.bfloat16)
        if j == 3:
            hooks('dattn')
    d_n1 = None
    for t in (2, 1, 0):
        pieces = []
        for j in range(WIDE // PAIR):
            piece = qkv[t, :, j * PAIR:(j + 1) * PAIR].astype(jnp.float32)
            pieces.append(rotate_back(piece, tabs) if t < 2 else piece)
        d_part = jnp.concatenate(pieces, axis=1)
        put_small(10 + t, d_part)
        qkv[t] = d_part.astype(jnp.bfloat16)
        put(t * WIDE, dot_at(n1[...], qkv[t]))
        term = dot_bt(qkv[t], weight(full, layer, t * WIDE))
        d_n1 = term if d_n1 is None else d_n1 + term
        if t != 1:
            hooks('dqkv', (t // 2) * 2 * WIDE)
    d_n1 = d_n1.astype(jnp.bfloat16).astype(jnp.float32)
    d_n2 = d_n2.astype(jnp.float32)
    scaled, rstd = normalised(hidden[...].astype(jnp.float32))
    put_small(0, d_n1 * scaled)
    put_small(1, d_n1)
    put_small(3, d_n2 * scaled)
    put_small(4, d_n2)
    d_scaled = d_n1 * vec(0) + d_n2 * vec(3)
    d_hidden = rstd * (d_scaled - jnp.mean(d_scaled, axis=-1, keepdims=True)
                       - scaled * jnp.mean(d_scaled * scaled, axis=-1, keepdims=True))
    return (d_out32 + d_hidden).astype(jnp.bfloat16)


def gather_program(pieces, done):
    for _ in range(5):
        next(pieces[0])
        yield
    for i, piece in enumerate(pieces):
        following = pieces[i + 1:i + 2]
        for _ in range(5):
            for later in following:
                next(later)
            next(piece)
            yield
        done.append(i)
        yield


def step_kernel(chunk, x, y_cot, own, small_own, tab_cos, tab_up, tab_down,
                y_out, x_grad, out, small_out,
                full, grads, part0, partx, party, last, partz, small, small_grads, small_bufs, small_grad_bufs,
                n1, n2, qkv, probs, ctx, slope, act, hidden1, d_hidden1, send_sems, recv_sems):
    tabs = (tab_cos, tab_up, tab_down)
    saved = (n1, n2, qkv, probs, ctx, slope, act)
    pos = positions()
    entry_barrier(pos)
    copies = Copies(send_sems, recv_sems)

    small_gen = small_reduce_steps(copies, pos, small_own, small_bufs, small)
    done = []
    gather = gather_program([gather_steps(copies, pos, own.at[i], full.at[i], lo, width)
                             for i in range(LAYERS) for lo, width in ((0, UP), (UP, 2 * UP))], done)

    def gather_until(piece):
        while piece not in done:
            next(gather)

    next(gather)
    next(small_gen)
    small_grads[...] = jnp.zeros_like(small_grads)
    for _ in range(4):
        next(gather)
        next(small_gen)
    gather_until(0)

    def forward_hooks(layer):
        def hooks(name):
            if name == 'qkv':
                next(gather)
            elif name == 'attn':
                next(gather)
            elif name == 'out':
                gather_until(2 * layer + 1)
            elif name == 'mlp' and layer == 0:
                next(gather)
        return hooks

    hidden1[...] = layer_forward(0, x, full, small, tabs, saved, forward_hooks(0))
    gather_until(2)
    y_out[...] = layer_forward(1, hidden1, full, small, tabs, saved, forward_hooks(1))

    queue = ScatterQueue()

    def add(layer, lo):
        queue.add(scatter_chunk_steps(copies, pos, grads, part0.at[layer], partx.at[layer], party.at[layer],
                                      last.at[layer], partz.at[layer], out.at[layer], lo, chunk))

    def hooks_from(layer, plan):
        calls = iter(plan)

        def hooks(name, lo=None):
            wanted, stages = next(calls)
            assert name == wanted
            if lo is not None:
                add(layer, lo)
            queue.pump(*stages)
        return hooks

    backward1 = [('down', ()), ('down', (0,)), ('up', (0,)), ('up', (0,)), ('dctx', (0,)), ('dattn', ()), ('dattn', (1,)),
                 ('dqkv', ()), ('dqkv', (0,))]
    again0 = [('norm', (0,)), ('qkv', ()), ('attn', ()), ('attn', ()), ('out', (1,)),
              ('mlp', ()), ('mlp', ()), ('mlp', ()), ('mlp', (1,))]
    backward0 = [('down', ()), ('down', (0, 2)), ('up', (0, 1)), ('up', (0, 2)), ('dctx', (0, 1)), ('dattn', (2,)),
                 ('dattn', (1, 3)), ('dqkv', ()), ('dqkv', (0,))]
    d_hidden1[...] = layer_backward(1, hidden1, y_cot, full, small, tabs, saved, grads, small_grads,
                                    hooks_from(1, backward1))
    layer_forward(0, x, full, small, tabs, saved, hooks_from(0, again0))
    x_grad[...] = layer_backward(0, x, d_hidden1, full, small, tabs, saved, grads, small_grads,
                                 hooks_from(0, backward0))
    small_gen = small_reduce_steps(copies, pos, small_grads, small_grad_bufs, small_out)
    queue.drain(2, small_gen)
    for _ in small_gen:
        pass
    copies.finish()


def step_call(x, y_cot, own, small, tabs, chunk=1024):
    layers, rows, width = own.shape
    tokens, d_model = x.shape
    vmem = pl.BlockSpec(memory_space=pltpu.VMEM)
    bf16, f32 = jnp.bfloat16, jnp.float32
    n_sems = 7 * 2 + 4 * layers // 2 * 23 + 8 * layers * (width // chunk) + 8
    blocks = tokens // SEQ
    return pl.pallas_call(
        functools.partial(step_kernel, chunk),
        out_shape=(jax.ShapeDtypeStruct(x.shape, bf16), jax.ShapeDtypeStruct(x.shape, bf16),
                   jax.ShapeDtypeStruct(own.shape, bf16), jax.ShapeDtypeStruct(small.shape, f32)),
        in_specs=[vmem] * 7, out_specs=(vmem,) * 4,
        scratch_shapes=[
            pltpu.VMEM((layers, 4, 2, 2, 2, rows, width), bf16),
            pltpu.VMEM((4, 2, 2, 2, rows, width), f32),
            pltpu.VMEM((layers, 4, 2, 2, rows, width), f32),
            pltpu.VMEM((layers, 4, 2, rows, width // 2), f32),
            pltpu.VMEM((layers, 4, 2, rows, width // 2), f32),
            pltpu.VMEM((layers, 4, rows, width), f32),
            pltpu.VMEM((layers, 3, rows, width), f32),
            pltpu.VMEM(small.shape, f32),
            pltpu.VMEM(small.shape, f32),
            pltpu.VMEM((9,) + small.shape, f32),
            pltpu.VMEM((9,) + small.shape, f32),
            pltpu.VMEM((tokens, d_model), bf16),
            pltpu.VMEM((tokens, d_model), bf16),
            pltpu.VMEM((3, tokens, d_model), bf16),
            pltpu.VMEM((blocks, 4, 2, SEQ, SEQ), f32),
            pltpu.VMEM((tokens, d_model), bf16),
            pltpu.VMEM((tokens, 4 * d_model), f32),
            pltpu.VMEM((tokens, 4 * d_model), bf16),
            pltpu.VMEM((tokens, d_model), bf16),
            pltpu.VMEM((tokens, d_model), bf16),
            pltpu.SemaphoreType.DMA((n_sems,)), pltpu.SemaphoreType.DMA((n_sems,))],
        compiler_params=pltpu.CompilerParams(collective_id=0, has_side_effects=True,
                                             vmem_limit_bytes=67043328),
    )(x, y_cot, own, small, *tabs)


def rope_tables(seq_len, rot_dim, copies):
    inv_freq = 1.0 / (10000.0 ** (jnp.arange(0, rot_dim, 2, dtype=jnp.float32) / rot_dim))
    angles = jnp.arange(seq_len, dtype=jnp.float32)[:, None] * inv_freq[None, :]
    cos, sin = jnp.cos(angles), jnp.sin(angles)
    none = jnp.zeros_like(sin)
    rest = jnp.zeros((seq_len, 4 * rot_dim - rot_dim), jnp.float32)
    parts = ([cos, cos, rest + 1.0], [-sin, none, rest], [none, sin, rest])
    return [jnp.tile(jnp.concatenate(p, axis=-1), (copies, 2)) for p in parts]


def pack_own(qkv_weight, out_weight, up_weight, down_weight):
    layers, rows = out_weight.shape[0], out_weight.shape[1]
    devices = out_weight.shape[2] // rows
    d_model = out_weight.shape[2]
    up_perm = up_weight.reshape(layers, rows, devices, 4, rows).transpose(0, 1, 3, 2, 4).reshape(layers, rows, -1)
    down_perm = down_weight.reshape(layers, 4, rows, d_model).transpose(0, 2, 1, 3).reshape(layers, rows, -1)
    heads = qkv_weight.shape[2]
    qkv_perm = qkv_weight.reshape(layers, rows, heads, 3, -1).transpose(0, 1, 3, 2, 4).reshape(layers, rows, -1)
    return jnp.concatenate([qkv_perm, out_weight, up_perm, down_perm], axis=-1)


def unpack_own(packed, d_model, num_heads):
    layers, rows, _ = packed.shape
    devices = d_model // rows
    qkv = packed[..., :3 * d_model].reshape(layers, rows, 3, num_heads, -1).transpose(0, 1, 3, 2, 4)
    qkv = qkv.reshape(layers, rows, num_heads, -1)
    out = packed[..., 3 * d_model:4 * d_model]
    up = packed[..., 4 * d_model:8 * d_model].reshape(layers, rows, 4, devices, rows).transpose(0, 1, 3, 2, 4)
    down = packed[..., 8 * d_model:].reshape(layers, rows, 4, d_model).transpose(0, 2, 1, 3)
    return qkv, out, up.reshape(layers, rows, -1), down.reshape(layers, 4 * rows, d_model)


def pack_small(rank, d_model, heads, ln1_gain, ln1_bias, qkv_bias, out_bias, ln2_gain, ln2_bias, up_bias, down_bias):
    layers, part = ln1_gain.shape
    vectors = jnp.stack([ln1_gain, ln1_bias, out_bias, ln2_gain, ln2_bias, down_bias], axis=1)
    rows = jnp.concatenate([vectors, up_bias.reshape(layers, 4, part)], axis=1).astype(jnp.float32)
    wide = lax.dynamic_update_slice(jnp.zeros((layers, 10, d_model), jnp.float32), rows, (0, 0, rank * part))
    flat = lax.dynamic_update_slice(jnp.zeros((layers, 3 * d_model), jnp.float32),
                                    qkv_bias.astype(jnp.float32), (0, rank * 3 * part))
    pad = jnp.zeros((layers, SMALL - 13, d_model), jnp.float32)
    flat = flat.reshape(layers, heads, 3, -1).transpose(0, 2, 1, 3).reshape(layers, 3, d_model)
    return jnp.concatenate([wide, flat, pad], axis=1).reshape(layers * SMALL, d_model)


def unpack_small_own(rank, part, heads, small):
    layers, d_model = small.shape[0] // SMALL, small.shape[1]
    small = small.reshape(layers, SMALL, d_model).astype(jnp.bfloat16)
    own = lax.dynamic_slice(small[:, :10], (0, 0, rank * part), (layers, 10, part))
    flat = small[:, 10:13].reshape(layers, 3, heads, -1).transpose(0, 2, 1, 3).reshape(layers, -1)
    qkv_bias = lax.dynamic_slice(flat, (0, rank * 3 * part), (layers, 3 * part))
    return [own[:, i] for i in range(6)], qkv_bias, own[:, 6:10].reshape(layers, 4 * part)


def solution(mesh):
    shard_axes = ('node', 'local')
    act_spec = P(shard_axes)
    param_spec = P(None, shard_axes)

    def device_step(x, y_cot, ln1_gain, ln1_bias, qkv_weight, qkv_bias, out_weight, out_bias,
                    ln2_gain, ln2_bias, up_weight, up_bias, down_weight, down_bias):
        num_layers, d_model, num_heads = out_weight.shape[0], x.shape[2], qkv_weight.shape[2]
        part = out_bias.shape[1]
        rank = lax.axis_index('node') * 8 + lax.axis_index('local')
        tabs = rope_tables(x.shape[1], qkv_weight.shape[3] // 12, x.shape[0])
        own = pack_own(qkv_weight, out_weight, up_weight, down_weight)
        small = pack_small(rank, d_model, num_heads, ln1_gain, ln1_bias, qkv_bias, out_bias, ln2_gain, ln2_bias, up_bias, down_bias)
        y_out, x_grad, packed, small_sum = step_call(x.reshape(-1, d_model), y_cot.reshape(-1, d_model), own, small, tabs)
        qkv_g, out_g, up_g, down_g = unpack_own(packed, d_model, num_heads)
        (gain1, bias1, out_b, gain2, bias2, down_b), qkv_b, up_b = unpack_small_own(rank, part, num_heads, small_sum)
        return (y_out.reshape(x.shape), x_grad.reshape(x.shape), gain1, bias1, qkv_g, qkv_b, out_g, out_b,
                gain2, bias2, up_g, up_b, down_g, down_b)

    return jax.shard_map(device_step, mesh=mesh,
                         in_specs=(act_spec, act_spec) + (param_spec,) * 12,
                         out_specs=(act_spec, act_spec) + (param_spec,) * 12,
                         check_vma=False)
```

```python
import functools
import jax
import numpy as np
import jax.numpy as jnp
from jax import lax
from jax.experimental import pallas as pl
from jax.experimental.pallas import tpu as pltpu
from jax.sharding import PartitionSpec as P

EPSILON = 1e-5
MESH = pl.DeviceIdType.MESH
LAYERS = 2
ROWS = 16
SMALL = 16


def positions():
    z = lax.axis_index('node')
    l = lax.axis_index('local')
    c = l % 2
    x = (l // 2) % 2
    y = l // 4
    partner = (z, l + 1 - 2 * c)
    x_nbr = (z, l + 2 - 4 * x)
    y_nbr = (z, (l + 4) % 8)
    z_others = [z + 1 - 2 * (z % 2), (z + 2) % 4, 3 - z]
    return z, l, c, x, y, partner, x_nbr, y_nbr, z_others


def entry_barrier(pos):
    z, l, c, x, y, partner, x_nbr, y_nbr, z_others = pos
    barrier = pltpu.get_barrier_semaphore()
    for dev in [partner, x_nbr, y_nbr] + [(zo, l) for zo in z_others]:
        pl.semaphore_signal(barrier, inc=1, device_id=dev, device_id_type=MESH)
    pl.semaphore_wait(barrier, 6)


class Copies:
    def __init__(self, send_sems, recv_sems):
        self.send_sems, self.recv_sems, self.used = send_sems, recv_sems, 0
        self.open_sends = []

    def make(self, src, dst, dev):
        idx = self.used
        self.used += 1
        return pltpu.make_async_remote_copy(src_ref=src, dst_ref=dst, send_sem=self.send_sems.at[idx],
                                            recv_sem=self.recv_sems.at[idx], device_id=dev, device_id_type=MESH)

    def start(self, src, dst, dev):
        copy = self.make(src, dst, dev)
        copy.start()
        self.open_sends.append(copy)
        return copy

    def finish(self):
        for copy in self.open_sends:
            copy.wait_send()
        self.open_sends = []


def small_reduce_steps(copies, pos, src, bufs, out):
    z, l, c, x, y, partner, x_nbr, y_nbr, z_others = pos
    held = src
    for step, dev in enumerate((partner, x_nbr, y_nbr)):
        copy = copies.start(held, bufs.at[2 * step], dev)
        yield
        copy.wait_recv()
        bufs[2 * step + 1] = held[...] + bufs[2 * step]
        held = bufs.at[2 * step + 1]
    sends = [copies.start(held, bufs.at[6 + k], (zo, l)) for k, zo in enumerate(z_others)]
    yield
    for copy in sends:
        copy.wait_recv()
    out[...] = (held[...] + bufs[6]) + (bufs[7] + bufs[8])
    yield


def gather_steps(copies, pos, own, full, lo, width):
    z, l, c, x, y, partner, x_nbr, y_nbr, z_others = pos
    half = width // 2
    cols, cols_a, cols_b = pl.ds(lo, width), pl.ds(lo, half), pl.ds(lo + half, half)
    after = ((z + 1) % 4, l)
    z_order = [z, (z + 3) % 4, (z + 2) % 4, (z + 1) % 4]

    def block(zz, yy, xx, cc):
        return full.at[zz, yy, xx, cc, :, cols]

    from_z, from_x, from_y, diag, to_partner = [None] * 4, [None] * 4, [None] * 4, [], []

    def spread(k, got, place):
        if k < 3:
            from_z[k + 1] = copies.start(got, place, after)
        from_x[k] = copies.start(got, place, x_nbr)
        from_y[k] = copies.start(got, place, y_nbr)

    def forward_z(k):
        from_z[k].wait_recv()
        got = block(z_order[k], y, x, c)
        spread(k, got, got)

    def forward_cross(k):
        zz = z_order[k]
        from_x[k].wait_recv()
        got = full.at[zz, y, 1 - x, c, :, cols_a]
        diag.append(copies.start(got, got, y_nbr))
        from_y[k].wait_recv()
        got = full.at[zz, 1 - y, x, c, :, cols_b]
        diag.append(copies.start(got, got, x_nbr))

    def forward_partner(yy, xx):
        got = full.at[:, yy, xx, c, :, cols]
        to_partner.append(copies.start(got, got, partner))

    spread(0, own.at[:, cols], block(z, y, x, c))
    full[z, y, x, c, :, cols] = own[:, cols]
    yield
    forward_z(1)
    yield
    forward_cross(0)
    yield
    forward_z(2)
    yield
    forward_cross(1)
    yield
    forward_z(3)
    forward_partner(y, x)
    yield
    forward_cross(2)
    yield
    forward_cross(3)
    forward_partner(y, 1 - x)
    forward_partner(1 - y, x)
    yield
    for copy in diag:
        copy.wait_recv()
    forward_partner(1 - y, 1 - x)
    yield
    for copy in to_partner:
        copy.wait_recv()
    yield


STEP_TIMES = (0, 4, 4.5, 8, 8.5, 12, 13, 16, 19, 22)


def gather_program(pieces, starts, small_gen, done):
    events = [(start + time, i, step) for i, start in enumerate(starts) for step, time in enumerate(STEP_TIMES)]
    events += [(time, -1, step) for step, time in enumerate((0.5, 3, 6, 8, 11))]
    for _, i, step in sorted(events):
        if i < 0:
            next(small_gen)
        else:
            next(pieces[i])
            if step + 1 == len(STEP_TIMES):
                done.append(i)
        yield


def scatter_chunk_steps(copies, pos, grads, part0, partx, party, last, partz, out, lo, width):
    z, l, c, x, y, partner, x_nbr, y_nbr, z_others = pos
    half = width // 2
    cols, cols_a, cols_b = pl.ds(lo, width), pl.ds(lo, half), pl.ds(lo + half, half)
    hcols = pl.ds(lo // 2, half)
    swap = copies.make(grads.at[:, :, :, 1 - c, :, cols], part0.at[:, :, :, :, cols], partner)
    swap.start()
    yield
    swap.wait()
    part0[:, :, :, :, cols] = part0[:, :, :, :, cols] + grads[:, :, :, c, :, cols]
    send_a = copies.start(part0.at[:, :, 1 - x, :, cols_a], partx.at[:, :, :, hcols], x_nbr)
    send_b = copies.start(part0.at[:, 1 - y, :, :, cols_b], party.at[:, :, :, hcols], y_nbr)
    yield
    send_a.wait_recv()
    partx[:, :, :, hcols] = partx[:, :, :, hcols] + part0[:, :, x, :, cols_a]
    send_a = copies.start(partx.at[:, 1 - y, :, hcols], last.at[:, :, cols_a], y_nbr)
    send_b.wait_recv()
    party[:, :, :, hcols] = party[:, :, :, hcols] + part0[:, y, :, :, cols_b]
    send_b = copies.start(party.at[:, 1 - x, :, hcols], last.at[:, :, cols_b], x_nbr)
    yield
    send_a.wait_recv()
    send_b.wait_recv()
    last[:, :, cols_a] = last[:, :, cols_a] + partx[:, y, :, hcols]
    last[:, :, cols_b] = last[:, :, cols_b] + party[:, x, :, hcols]
    sends = [copies.start(last.at[zo, :, cols], partz.at[k, :, cols], (zo, l)) for k, zo in enumerate(z_others)]
    yield
    for copy in sends:
        copy.wait_recv()
    total = (last[z, :, cols] + partz[0, :, cols]) + (partz[1, :, cols] + partz[2, :, cols])
    out[:, cols] = total.astype(out.dtype)
    yield


class ScatterQueue:
    def __init__(self):
        self.waiting = [[], [], [], []]

    def add(self, chunk):
        next(chunk)
        self.waiting[0].append(chunk)

    def pump(self, *stages):
        for stage in stages:
            if self.waiting[stage]:
                chunk = self.waiting[stage].pop(0)
                next(chunk)
                if stage < 3:
                    self.waiting[stage + 1].append(chunk)

    def drain(self, lag, between):
        while any(self.waiting):
            next(between, None)
            for stage in range(4):
                if len(self.waiting[stage]) >= lag or not any(self.waiting[:stage]):
                    self.pump(stage)


def dot(first, second):
    return lax.dot_general(first, second, (((1,), (0,)), ((), ())), preferred_element_type=jnp.float32)


def dot_bt(first, second):
    return lax.dot_general(first, second, (((1,), (1,)), ((), ())), preferred_element_type=jnp.float32)


def dot_at(first, second):
    return lax.dot_general(first, second, (((0,), (0,)), ((), ())), preferred_element_type=jnp.float32)


WIDE = 512
PAIR = 128
SEQ = 128
OUT, UP, ACOLS = 3 * WIDE, 4 * WIDE, 8 * WIDE


def normalised(hidden32):
    center = hidden32 - jnp.mean(hidden32, axis=-1, keepdims=True)
    rstd = lax.rsqrt(jnp.mean(center * center, axis=-1, keepdims=True) + EPSILON)
    return center * rstd, rstd


def weight(full, layer, lo, width=WIDE):
    return full[layer, :, :, :, :, :, lo:lo + width].reshape(WIDE, width)


def down_weight_part(full, layer, k):
    return full[layer, k].reshape(WIDE, WIDE)


def rotate(piece, tab):
    piece = piece.reshape(-1, SEQ, PAIR)
    up, down = pltpu.roll(piece, PAIR - 8, 2), pltpu.roll(piece, 8, 2)
    return (piece * tab[0] + up * tab[1] + down * tab[2]).reshape(-1, PAIR)


def rotate_back(piece, tab):
    piece = piece.reshape(-1, SEQ, PAIR)
    turned = (piece * tab[0] + pltpu.roll(piece * tab[1], 8, 2) + pltpu.roll(piece * tab[2], PAIR - 8, 2))
    return turned.reshape(-1, PAIR)


def low_half(rows):
    return lax.broadcasted_iota(jnp.int32, (rows, PAIR), 1) < PAIR // 2


def head_masks():
    first = low_half(SEQ)
    return (jnp.where(first, 1.0, 0.0).astype(jnp.bfloat16), jnp.where(first, 0.0, 1.0).astype(jnp.bfloat16))


def attention_blocks(tokens):
    for s in range(tokens // SEQ):
        for j in range(WIDE // PAIR):
            yield s, j, pl.ds(s * SEQ, SEQ), pl.ds(j * PAIR, PAIR)


def layer_forward(layer, hidden, weights, small, tab, saved, hooks):
    n1, n2, qkv, probs, ctx, slope, act, d_qkv = saved
    wide_w, down_w = weights
    tokens = hidden.shape[0]

    def vec(row):
        return small[pl.ds(layer * SMALL + row, 1), :]

    hidden32 = hidden[...].astype(jnp.float32)
    scaled, _ = normalised(hidden32)
    n1[...] = (scaled * vec(0) + vec(1)).astype(jnp.bfloat16)
    n2[...] = (scaled * vec(3) + vec(4)).astype(jnp.bfloat16)
    hooks('norm')
    low = low_half(tokens)
    qkv_bias = jnp.concatenate([vec(10), vec(11), vec(12)], axis=1)
    group = 6 * PAIR
    for i in range(2):
        part = dot(n1[...], weight(wide_w, layer, i * group, group)) + qkv_bias[:, i * group:(i + 1) * group]
        for jj in range(2):
            first, second, third = (part[:, (3 * jj + m) * PAIR:(3 * jj + m + 1) * PAIR] for m in range(3))
            cols = pl.ds((2 * i + jj) * PAIR, PAIR)
            query = jnp.where(low, first, second)
            key = jnp.where(low, pltpu.roll(first, PAIR // 2, 1), pltpu.roll(third, PAIR // 2, 1))
            qkv[0, :, cols] = rotate(query, tab).astype(jnp.bfloat16)
            qkv[1, :, cols] = rotate(key, tab).astype(jnp.bfloat16)
            qkv[2, :, cols] = jnp.where(low, second, third).astype(jnp.bfloat16)
    hooks('qkv')
    causal = (lax.broadcasted_iota(jnp.int32, (SEQ, SEQ), 0) >= lax.broadcasted_iota(jnp.int32, (SEQ, SEQ), 1))
    masks, low = head_masks(), low_half(SEQ)
    for s, j, rows, cols in attention_blocks(tokens):
        query, key, value = qkv[0, rows, cols], qkv[1, rows, cols], qkv[2, rows, cols]
        heads = []
        for h in range(2):
            scores = dot_bt(query * masks[h], key) * 0.125
            scores = jnp.where(causal, scores, -1e30)
            attn = jnp.exp(scores - jnp.max(scores, axis=-1, keepdims=True))
            attn = attn / jnp.sum(attn, axis=-1, keepdims=True)
            probs[s, j, h] = attn
            heads.append(dot(attn.astype(jnp.bfloat16), value))
        ctx[rows, cols] = jnp.where(low, heads[0], heads[1]).astype(jnp.bfloat16)
        if j == 3:
            hooks('attn')
    total = hidden32 + (dot(ctx[...], weight(wide_w, layer, OUT)) + vec(2))
    hooks('out')
    mlp = None
    for k in range(4):
        pre = dot(n2[...], weight(wide_w, layer, UP + k * WIDE)) + vec(6 + k)
        bell = lax.erf(pre * 0.7071067811865476) + 1.0
        act[:, k * WIDE:(k + 1) * WIDE] = (0.5 * pre * bell).astype(jnp.bfloat16)
        slope[:, k * WIDE:(k + 1) * WIDE] = 0.5 * bell + pre * (jnp.exp(-0.5 * pre * pre) * 0.3989422804014327)
        if k == 0:
            hooks('up')
        term = dot(act[:, k * WIDE:(k + 1) * WIDE], down_weight_part(down_w, layer, k))
        mlp = term if mlp is None else mlp + term
        hooks('mlp')
    return (total + (mlp + vec(5))).astype(jnp.bfloat16)


def layer_backward(layer, hidden, d_out, weights, small, tab, saved, grads, small_grads, hooks):
    n1, n2, qkv, probs, ctx, slope, act, d_qkv = saved
    wide_w, down_w = weights
    wide_g, down_g = grads
    tokens = hidden.shape[0]

    def vec(row):
        return small[pl.ds(layer * SMALL + row, 1), :]

    def put_small(row, value):
        small_grads[pl.ds(layer * SMALL + row, 1), :] = jnp.sum(value, axis=0, keepdims=True)

    def put(lo, value):
        wide_g[:, :, :, :, :, lo:lo + WIDE] = value.reshape(wide_g.shape[:5] + (WIDE,))

    d_out32 = d_out[...].astype(jnp.float32)
    put_small(2, d_out32)
    put_small(5, d_out32)
    half = WIDE // 2
    for k in range(2):
        value = dot_at(act[...], d_out[:, k * half:(k + 1) * half])
        down_g[:, :, :, :, :, k * half:(k + 1) * half] = value.reshape(down_g.shape[:5] + (half,))
        hooks('down', (1, k * half))
    d_n2 = None
    for k in range(4):
        d_act = dot_bt(d_out[...], down_weight_part(down_w, layer, k)).astype(jnp.bfloat16)
        d_pre = d_act.astype(jnp.float32) * slope[:, k * WIDE:(k + 1) * WIDE]
        put_small(6 + k, d_pre)
        act[:, k * WIDE:(k + 1) * WIDE] = d_pre.astype(jnp.bfloat16)
        d_pre_bf = act[:, k * WIDE:(k + 1) * WIDE]
        put(UP + k * WIDE, dot_at(n2[...], d_pre_bf))
        term = dot_bt(d_pre_bf, weight(wide_w, layer, UP + k * WIDE))
        d_n2 = term if d_n2 is None else d_n2 + term
        if k % 2:
            hooks('up', (0, UP + (k - 1) * WIDE))
    d_n2 = d_n2.astype(jnp.bfloat16)
    put(OUT, dot_at(ctx[...], d_out[...]))
    ctx[...] = dot_bt(d_out[...], weight(wide_w, layer, OUT)).astype(jnp.bfloat16)
    hooks('dctx')
    masks, low = head_masks(), low_half(SEQ)
    for s, j, rows, cols in attention_blocks(tokens):
        query, key, value = qkv[0, rows, cols], qkv[1, rows, cols], qkv[2, rows, cols]
        d_ctx = ctx[rows, cols]
        d_q, d_k, d_v = [], [], []
        for h in range(2):
            attn = probs[s, j, h]
            d_probs = dot_bt(d_ctx * masks[h], value).astype(jnp.bfloat16).astype(jnp.float32)
            d_v.append(dot_at(attn.astype(jnp.bfloat16), d_ctx))
            inner = jnp.sum(d_probs * attn, axis=-1, keepdims=True)
            d_scores = (attn * (d_probs - inner) * 0.125).astype(jnp.bfloat16)
            d_q.append(dot(d_scores, key))
            d_k.append(dot_at(d_scores, query))
        qkv[0, rows, cols] = jnp.where(low, d_q[0], d_q[1]).astype(jnp.bfloat16)
        qkv[1, rows, cols] = jnp.where(low, d_k[0], d_k[1]).astype(jnp.bfloat16)
        qkv[2, rows, cols] = jnp.where(low, d_v[0], d_v[1]).astype(jnp.bfloat16)
        if j == 3:
            hooks('dattn')
    low = low_half(tokens)
    for j in range(WIDE // PAIR):
        cols = pl.ds(j * PAIR, PAIR)
        d_query, d_key, d_value = (qkv[t, :, cols].astype(jnp.float32) for t in range(3))
        d_query = rotate_back(d_query, tab)
        d_key = pltpu.roll(rotate_back(d_key, tab), PAIR // 2, 1)
        parts = (jnp.where(low, d_query, d_key), jnp.where(low, d_value, d_query), jnp.where(low, d_key, d_value))
        for m, part in enumerate(parts):
            lo = (3 * j + m) * PAIR
            row = layer * SMALL + 10 + lo // WIDE
            small_grads[pl.ds(row, 1), pl.ds(lo % WIDE, PAIR)] = jnp.sum(part, axis=0, keepdims=True)
            d_qkv[:, lo:lo + PAIR] = part.astype(jnp.bfloat16)
    d_n1 = None
    for t in (2, 1, 0):
        piece = d_qkv[:, t * WIDE:(t + 1) * WIDE]
        put(t * WIDE, dot_at(n1[...], piece))
        term = dot_bt(piece, weight(wide_w, layer, t * WIDE))
        d_n1 = term if d_n1 is None else d_n1 + term
        if t != 1:
            hooks('dqkv', (0, (t // 2) * 2 * WIDE))
    d_n1 = d_n1.astype(jnp.bfloat16).astype(jnp.float32)
    d_n2 = d_n2.astype(jnp.float32)
    scaled, rstd = normalised(hidden[...].astype(jnp.float32))
    put_small(0, d_n1 * scaled)
    put_small(1, d_n1)
    put_small(3, d_n2 * scaled)
    put_small(4, d_n2)
    d_scaled = d_n1 * vec(0) + d_n2 * vec(3)
    d_hidden = rstd * (d_scaled - jnp.mean(d_scaled, axis=-1, keepdims=True)
                       - scaled * jnp.mean(d_scaled * scaled, axis=-1, keepdims=True))
    return (d_out32 + d_hidden).astype(jnp.bfloat16)


def places(rank, part, width):
    shift = lax.broadcasted_iota(jnp.int32, (part, width), 1) - lax.broadcasted_iota(jnp.int32, (part, width), 0)
    return jnp.where(shift == rank * part, 1.0, 0.0).astype(jnp.bfloat16)


VECTOR_ROWS = ((0, 1), (1, 1), (10, 3), (2, 1), (3, 1), (4, 1), (6, 4), (5, 1))


def place_small(rank, vectors, small_own):
    small_own[...] = jnp.zeros_like(small_own)
    for ref, (row, count) in zip(vectors, VECTOR_ROWS):
        wide = dot(ref[...], places(rank, ref.shape[1], count * WIDE))
        for layer in range(LAYERS):
            for i in range(count):
                small_own[pl.ds(layer * SMALL + row + i, 1), :] = wide[layer:layer + 1, i * WIDE:(i + 1) * WIDE]


def step_kernel(x, y_cot, qkv_own, out_own, up_own, down_own, *refs):
    (gain1, bias1, qkv_b, out_b, gain2, bias2, up_b, down_b, tab,
     y_out, x_grad, wide_out, down_out, small_out,
     wide_own, wide_w, down_w, wide_g, down_g) = refs[:19]
    wide_parts, down_parts = refs[19:24], refs[24:29]
    (small_own, small, small_grads, small_bufs, small_grad_bufs,
     n1, n2, qkv, probs, ctx, slope, act, d_qkv, hidden1, d_hidden1, send_sems, recv_sems) = refs[29:]
    saved = (n1, n2, qkv, probs, ctx, slope, act, d_qkv)
    weights, grads = (wide_w, down_w), (wide_g, down_g)
    pos = positions()
    rank = pos[0] * 8 + pos[1]
    wide_own[:, :, :OUT] = qkv_own[...]
    wide_own[:, :, OUT:UP] = out_own[...]
    wide_own[:, :, UP:] = up_own[...]
    place_small(rank, (gain1, bias1, qkv_b, out_b, gain2, bias2, up_b, down_b), small_own)
    small_grads[...] = jnp.zeros_like(small_grads)
    entry_barrier(pos)
    copies = Copies(send_sems, recv_sems)

    small_gen = small_reduce_steps(copies, pos, small_own, small_bufs, small)
    done = []
    pieces = []
    for i in range(LAYERS):
        pieces.append(gather_steps(copies, pos, wide_own.at[i], wide_w.at[i], 0, UP))
        pieces.append(gather_steps(copies, pos, wide_own.at[i], wide_w.at[i], UP, UP))
        pieces.append(gather_steps(copies, pos, down_own.at[i], down_w.at[i], 0, WIDE))
    gather = gather_program(pieces, (0, 1, 6, 14, 22, 31), small_gen, done)

    def gather_until(piece):
        while piece not in done:
            next(gather)

    def gather_pump(count):
        for _ in range(count):
            next(gather, None)

    gather_until(0)

    def forward_hooks(layer):
        def hooks(name):
            if name == 'out':
                gather_until(3 * layer + 1)
            elif name == 'up':
                gather_until(3 * layer + 2)
            else:
                gather_pump(2)
        return hooks

    hidden1[...] = layer_forward(0, x, weights, small, tab, saved, forward_hooks(0))
    gather_until(3)
    y_out[...] = layer_forward(1, hidden1, weights, small, tab, saved, forward_hooks(1))
    gather_until(5)

    queue = ScatterQueue()

    def add(layer, kind, lo):
        parts = (wide_parts, down_parts)[kind]
        out = (wide_out, down_out)[kind]
        queue.add(scatter_chunk_steps(copies, pos, grads[kind], *(ref.at[layer] for ref in parts), out.at[layer],
                                      lo, (2 * WIDE, WIDE // 2)[kind]))

    def hooks_from(layer, plan):
        calls = iter(plan)

        def hooks(name, chunk=None):
            wanted, stages = next(calls)
            assert name == wanted
            if chunk is not None:
                add(layer, *chunk)
            queue.pump(*stages)
        return hooks

    backward1 = [('down', ()), ('down', (0,)), ('up', (0,)), ('up', (0,)), ('dctx', (0,)), ('dattn', ()), ('dattn', (1,)),
                 ('dqkv', ()), ('dqkv', (0,))]
    again0 = [('norm', (0,)), ('qkv', ()), ('attn', ()), ('attn', ()), ('out', (1,)), ('up', ()),
              ('mlp', ()), ('mlp', ()), ('mlp', ()), ('mlp', (1,))]
    backward0 = [('down', ()), ('down', (0, 2)), ('up', (0, 1)), ('up', (0, 2)), ('dctx', (0, 1)), ('dattn', (2,)),
                 ('dattn', (1, 3)), ('dqkv', ()), ('dqkv', (0,))]
    d_hidden1[...] = layer_backward(1, hidden1, y_cot, weights, small, tab, saved, grads, small_grads,
                                    hooks_from(1, backward1))
    layer_forward(0, x, weights, small, tab, saved, hooks_from(0, again0))
    x_grad[...] = layer_backward(0, x, d_hidden1, weights, small, tab, saved, grads, small_grads,
                                 hooks_from(0, backward0))
    small_gen = small_reduce_steps(copies, pos, small_grads, small_grad_bufs, small_out)
    queue.drain(2, small_gen)
    for _ in small_gen:
        pass
    copies.finish()


def part_scratch(rows, width):
    return [pltpu.VMEM((LAYERS, 4, 2, 2, rows, width), jnp.float32),
            pltpu.VMEM((LAYERS, 4, 2, rows, width // 2), jnp.float32),
            pltpu.VMEM((LAYERS, 4, 2, rows, width // 2), jnp.float32),
            pltpu.VMEM((LAYERS, 4, rows, width), jnp.float32),
            pltpu.VMEM((LAYERS, 3, rows, width), jnp.float32)]


def step_call(x, y_cot, matrices, vectors, tab):
    tokens, d_model = x.shape
    rows, down_rows = matrices[1].shape[1], matrices[3].shape[1]
    vmem = pl.BlockSpec(memory_space=pltpu.VMEM)
    bf16, f32 = jnp.bfloat16, jnp.float32
    small = (LAYERS * SMALL, d_model)
    n_sems = 6 * 2 + 6 * 23 + 8 * 12
    return pl.pallas_call(
        step_kernel,
        out_shape=(jax.ShapeDtypeStruct(x.shape, bf16), jax.ShapeDtypeStruct(x.shape, bf16),
                   jax.ShapeDtypeStruct((LAYERS, rows, ACOLS), bf16),
                   jax.ShapeDtypeStruct((LAYERS, down_rows, d_model), bf16), jax.ShapeDtypeStruct(small, f32)),
        in_specs=[vmem] * (2 + 4 + 8 + 1), out_specs=(vmem,) * 5,
        scratch_shapes=[
            pltpu.VMEM((LAYERS, rows, ACOLS), bf16),
            pltpu.VMEM((LAYERS, 4, 2, 2, 2, rows, ACOLS), bf16),
            pltpu.VMEM((LAYERS, 4, 2, 2, 2, down_rows, d_model), bf16),
            pltpu.VMEM((4, 2, 2, 2, rows, ACOLS), f32),
            pltpu.VMEM((4, 2, 2, 2, down_rows, d_model), f32),
            *part_scratch(rows, ACOLS), *part_scratch(down_rows, d_model),
            pltpu.VMEM(small, f32),
            pltpu.VMEM(small, f32),
            pltpu.VMEM(small, f32),
            pltpu.VMEM((9,) + small, f32),
            pltpu.VMEM((9,) + small, f32),
            pltpu.VMEM((tokens, d_model), bf16),
            pltpu.VMEM((tokens, d_model), bf16),
            pltpu.VMEM((3, tokens, d_model), bf16),
            pltpu.VMEM((tokens // SEQ, 4, 2, SEQ, SEQ), f32),
            pltpu.VMEM((tokens, d_model), bf16),
            pltpu.VMEM((tokens, 4 * d_model), f32),
            pltpu.VMEM((tokens, 4 * d_model), bf16),
            pltpu.VMEM((tokens, 3 * d_model), bf16),
            pltpu.VMEM((tokens, d_model), bf16),
            pltpu.VMEM((tokens, d_model), bf16),
            pltpu.SemaphoreType.DMA((n_sems,)), pltpu.SemaphoreType.DMA((n_sems,))],
        compiler_params=pltpu.CompilerParams(collective_id=0, has_side_effects=True,
                                             vmem_limit_bytes=67043328),
    )(x, y_cot, *matrices, *vectors, tab)


def finish_kernel(y_in, x_grad_in, wide, down, small, y_out, x_grad, gain1, bias1, qkv_g, qkv_b, out_g, out_b,
                  gain2, bias2, up_g, up_b, down_g, down_b):
    y_out[...] = y_in[...]
    x_grad[...] = x_grad_in[...]
    qkv_g[...] = wide[:, :, :OUT]
    out_g[...] = wide[:, :, OUT:UP]
    up_g[...] = wide[:, :, UP:]
    down_g[...] = down[...]
    rank = lax.axis_index('node') * 8 + lax.axis_index('local')
    for ref, (row, count) in zip((gain1, bias1, qkv_b, out_b, gain2, bias2, up_b, down_b), VECTOR_ROWS):
        sums = []
        for layer in range(LAYERS):
            lines = [small[pl.ds(layer * SMALL + row + i, 1), :] for i in range(count)]
            sums.append(jnp.concatenate(lines, axis=1))
        sums = jnp.concatenate(sums, axis=0).astype(jnp.bfloat16)
        ref[...] = dot_bt(sums, places(rank, ref.shape[1], count * WIDE)).astype(jnp.bfloat16)


def finish_call(y, x_grad, wide, down, small, shapes):
    vmem = pl.BlockSpec(memory_space=pltpu.VMEM)
    return pl.pallas_call(
        finish_kernel, out_shape=tuple(jax.ShapeDtypeStruct(s, jnp.bfloat16) for s in shapes),
        in_specs=[vmem] * 5, out_specs=(vmem,) * len(shapes),
    )(y, x_grad, wide, down, small)


def rope_table(seq_len, rot_dim):
    inv_freq = 1.0 / (np.float32(10000.0) ** (np.arange(0, rot_dim, 2, dtype=np.float32) / np.float32(rot_dim)))
    angles = np.arange(seq_len, dtype=np.float32)[:, None] * inv_freq[None, :].astype(np.float32)
    cos, sin = np.cos(angles), np.sin(angles)
    none = np.zeros_like(sin)
    rest = np.zeros((seq_len, 3 * rot_dim), np.float32)
    parts = ([cos, cos, rest + 1.0], [-sin, none, rest], [none, sin, rest])
    return np.stack([np.tile(np.concatenate(p, axis=-1), (1, 2)) for p in parts]).astype(np.float32)


def solution(mesh):
    shard_axes = ('node', 'local')
    act_spec = P(shard_axes)
    param_spec = P(None, shard_axes)

    def device_step(x, y_cot, ln1_gain, ln1_bias, qkv_weight, qkv_bias, out_weight, out_bias,
                    ln2_gain, ln2_bias, up_weight, up_bias, down_weight, down_bias):
        d_model, rows = x.shape[2], out_weight.shape[1]
        flat = (x.shape[0] * x.shape[1], d_model)
        qkv_flat = (LAYERS, rows, 3 * d_model)
        matrices = (qkv_weight.reshape(qkv_flat), out_weight, up_weight, down_weight)
        vectors = (ln1_gain, ln1_bias, qkv_bias, out_bias, ln2_gain, ln2_bias, up_bias, down_bias)
        sums = step_call(x.reshape(flat), y_cot.reshape(flat), matrices, vectors, rope_table(x.shape[1], qkv_weight.shape[3] // 12))
        shapes = [flat, flat, ln1_gain.shape, ln1_bias.shape, qkv_flat, qkv_bias.shape, out_weight.shape, out_bias.shape,
                  ln2_gain.shape, ln2_bias.shape, up_weight.shape, up_bias.shape, down_weight.shape, down_bias.shape]
        outs = list(finish_call(*sums, shapes))
        outs[0], outs[1], outs[4] = outs[0].reshape(x.shape), outs[1].reshape(x.shape), outs[4].reshape(qkv_weight.shape)
        return tuple(outs)

    return jax.shard_map(device_step, mesh=mesh,
                         in_specs=(act_spec, act_spec) + (param_spec,) * 12,
                         out_specs=(act_spec, act_spec) + (param_spec,) * 12,
                         check_vma=False)
```

```python
import functools
import jax
import numpy as np
import jax.numpy as jnp
from jax import lax
from jax.experimental import pallas as pl
from jax.experimental.pallas import tpu as pltpu
from jax.sharding import PartitionSpec as P

EPSILON = 1e-5
MESH = pl.DeviceIdType.MESH
LAYERS = 2
ROWS = 16
SMALL = 16


def positions():
    z = lax.axis_index('node')
    l = lax.axis_index('local')
    c = l % 2
    x = (l // 2) % 2
    y = l // 4
    partner = (z, l + 1 - 2 * c)
    x_nbr = (z, l + 2 - 4 * x)
    y_nbr = (z, (l + 4) % 8)
    z_others = [z + 1 - 2 * (z % 2), (z + 2) % 4, 3 - z]
    return z, l, c, x, y, partner, x_nbr, y_nbr, z_others


def entry_barrier(pos):
    z, l, c, x, y, partner, x_nbr, y_nbr, z_others = pos
    barrier = pltpu.get_barrier_semaphore()
    for dev in [partner, x_nbr, y_nbr] + [(zo, l) for zo in z_others]:
        pl.semaphore_signal(barrier, inc=1, device_id=dev, device_id_type=MESH)
    pl.semaphore_wait(barrier, 6)


class Copies:
    def __init__(self, send_sems, recv_sems):
        self.send_sems, self.recv_sems, self.used = send_sems, recv_sems, 0
        self.open_sends = []

    def make(self, src, dst, dev):
        idx = self.used
        self.used += 1
        return pltpu.make_async_remote_copy(src_ref=src, dst_ref=dst, send_sem=self.send_sems.at[idx],
                                            recv_sem=self.recv_sems.at[idx], device_id=dev, device_id_type=MESH)

    def start(self, src, dst, dev):
        copy = self.make(src, dst, dev)
        copy.start()
        self.open_sends.append(copy)
        return copy

    def finish(self):
        for copy in self.open_sends:
            copy.wait_send()
        self.open_sends = []


def small_reduce_steps(copies, pos, src, bufs, out):
    z, l, c, x, y, partner, x_nbr, y_nbr, z_others = pos
    held = src
    for step, dev in enumerate((partner, x_nbr, y_nbr)):
        copy = copies.start(held, bufs.at[2 * step], dev)
        yield
        copy.wait_recv()
        bufs[2 * step + 1] = held[...] + bufs[2 * step]
        held = bufs.at[2 * step + 1]
    sends = [copies.start(held, bufs.at[6 + k], (zo, l)) for k, zo in enumerate(z_others)]
    yield
    for copy in sends:
        copy.wait_recv()
    out[...] = (held[...] + bufs[6]) + (bufs[7] + bufs[8])
    yield


def gather_steps(copies, pos, own, full, lo, width):
    z, l, c, x, y, partner, x_nbr, y_nbr, z_others = pos
    half = width // 2
    cols, cols_a, cols_b = pl.ds(lo, width), pl.ds(lo, half), pl.ds(lo + half, half)
    after = ((z + 1) % 4, l)
    z_order = [z, (z + 3) % 4, (z + 2) % 4, (z + 1) % 4]

    def block(zz, yy, xx, cc):
        return full.at[zz, yy, xx, cc, :, cols]

    from_z, from_x, from_y, diag, to_partner = [None] * 4, [None] * 4, [None] * 4, [], []

    def spread(k, got, place):
        if k < 3:
            from_z[k + 1] = copies.start(got, place, after)
        from_x[k] = copies.start(got, place, x_nbr)
        from_y[k] = copies.start(got, place, y_nbr)

    def forward_z(k):
        from_z[k].wait_recv()
        got = block(z_order[k], y, x, c)
        spread(k, got, got)

    def forward_cross(k):
        zz = z_order[k]
        from_x[k].wait_recv()
        got = full.at[zz, y, 1 - x, c, :, cols_a]
        diag.append(copies.start(got, got, y_nbr))
        from_y[k].wait_recv()
        got = full.at[zz, 1 - y, x, c, :, cols_b]
        diag.append(copies.start(got, got, x_nbr))

    def forward_partner(yy, xx):
        got = full.at[:, yy, xx, c, :, cols]
        to_partner.append(copies.start(got, got, partner))

    spread(0, own.at[:, cols], block(z, y, x, c))
    full[z, y, x, c, :, cols] = own[:, cols]
    yield
    forward_z(1)
    yield
    forward_cross(0)
    yield
    forward_z(2)
    yield
    forward_cross(1)
    yield
    forward_z(3)
    forward_partner(y, x)
    yield
    forward_cross(2)
    yield
    forward_cross(3)
    forward_partner(y, 1 - x)
    forward_partner(1 - y, x)
    yield
    for copy in diag:
        copy.wait_recv()
    forward_partner(1 - y, 1 - x)
    yield
    for copy in to_partner:
        copy.wait_recv()
    yield


def gather_plane_first_steps(copies, pos, own, full, lo, width):
    z, l, c, x, y, partner, x_nbr, y_nbr, z_others = pos
    half = width // 2
    cols, cols_a, cols_b = pl.ds(lo, width), pl.ds(lo, half), pl.ds(lo + half, half)
    after = ((z + 1) % 4, l)
    z_order = [z, (z + 3) % 4, (z + 2) % 4, (z + 1) % 4]
    mine, own_cols = full.at[z, y, x, c, :, cols], own.at[:, cols]
    from_x = copies.start(own_cols, mine, x_nbr)
    from_y = copies.start(own_cols, mine, y_nbr)
    full[z, y, x, c, :, cols] = own[:, cols]
    yield
    from_x.wait_recv()
    got = full.at[z, y, 1 - x, c, :, cols_a]
    diag_y = copies.start(got, got, y_nbr)
    from_y.wait_recv()
    got = full.at[z, 1 - y, x, c, :, cols_b]
    diag_x = copies.start(got, got, x_nbr)
    yield
    diag_y.wait_recv()
    diag_x.wait_recv()
    to_partner = []
    for k in range(4):
        got = full.at[z_order[k], :, :, c, :, cols]
        if k < 3:
            from_z = copies.start(got, got, after)
        to_partner.append(copies.start(got, got, partner))
        yield
        if k < 3:
            from_z.wait_recv()
    for copy in to_partner:
        copy.wait_recv()
    yield


GATHER_ORDER = 'afcbacbafcadcbfeaabccdaafbbeccdbbdaecaeddfcbeebddeeddefef'
SMALL_TURNS = (3, 6, 10, 14, 18)
GATHER_PUMPS = ('21211015', '11452044')
SCATTER_ORDER = 'abcabdcbaedcfedagfebhfcighdajiheagkjiflkjgmlkhmlimjgkglm'
SCATTER_PUMPS = ('0402111100', '1040010444', '0202432104')


def turns(letters):
    return [ord(letter) - ord('a') for letter in letters]


def counts_of(digits):
    return iter([int(digit) for digit in digits])


def gather_program(pieces, small_gen, done):
    order = turns(GATHER_ORDER)
    left = [order.count(i) for i in range(len(pieces))]
    for turn, i in enumerate(order):
        if turn in SMALL_TURNS:
            next(small_gen)
        next(pieces[i])
        left[i] -= 1
        if not left[i]:
            done.append(i)
        yield


def scatter_chunk_steps(copies, pos, grads, part0, partx, party, last, partz, out, lo, width):
    z, l, c, x, y, partner, x_nbr, y_nbr, z_others = pos
    half = width // 2
    cols, cols_a, cols_b = pl.ds(lo, width), pl.ds(lo, half), pl.ds(lo + half, half)
    hcols = pl.ds(lo // 2, half)
    swap = copies.make(grads.at[:, :, :, 1 - c, :, cols], part0.at[:, :, :, :, cols], partner)
    swap.start()
    yield
    swap.wait()
    part0[:, :, :, :, cols] = part0[:, :, :, :, cols] + grads[:, :, :, c, :, cols]
    send_a = copies.start(part0.at[:, :, 1 - x, :, cols_a], partx.at[:, :, :, hcols], x_nbr)
    send_b = copies.start(part0.at[:, 1 - y, :, :, cols_b], party.at[:, :, :, hcols], y_nbr)
    yield
    send_a.wait_recv()
    partx[:, :, :, hcols] = partx[:, :, :, hcols] + part0[:, :, x, :, cols_a]
    send_a = copies.start(partx.at[:, 1 - y, :, hcols], last.at[:, :, cols_a], y_nbr)
    send_b.wait_recv()
    party[:, :, :, hcols] = party[:, :, :, hcols] + part0[:, y, :, :, cols_b]
    send_b = copies.start(party.at[:, 1 - x, :, hcols], last.at[:, :, cols_b], x_nbr)
    yield
    send_a.wait_recv()
    send_b.wait_recv()
    last[:, :, cols_a] = last[:, :, cols_a] + partx[:, y, :, hcols]
    last[:, :, cols_b] = last[:, :, cols_b] + party[:, x, :, hcols]
    sends = [copies.start(last.at[zo, :, cols], partz.at[k, :, cols], (zo, l)) for k, zo in enumerate(z_others)]
    yield
    for copy in sends:
        copy.wait_recv()
    total = (last[z, :, cols] + partz[0, :, cols]) + (partz[1, :, cols] + partz[2, :, cols])
    out[:, cols] = total.astype(out.dtype)
    yield


def scatter_z_first_steps(copies, pos, grads, part0, ring, plane, out, lo, width):
    z, l, c, x, y, partner, x_nbr, y_nbr, z_others = pos
    half = width // 2
    cols, cols_a, cols_b = pl.ds(lo, width), pl.ds(lo, half), pl.ds(lo + half, half)
    first_a, first_b = pl.ds(0, half), pl.ds(half, half)
    after = ((z + 1) % 4, l)
    z_order = [z, (z + 3) % 4, (z + 2) % 4, (z + 1) % 4]
    swap = copies.make(grads.at[:, :, :, 1 - c, :, cols], part0.at[:, :, :, :, cols], partner)
    swap.start()
    yield
    swap.wait()
    part0[:, :, :, :, cols] = part0[:, :, :, :, cols] + grads[:, :, :, c, :, cols]
    send = copies.start(part0.at[z_order[1], :, :, :, cols], ring.at[0], after)
    yield
    for k in (1, 2):
        send.wait_recv()
        ring[k - 1] = ring[k - 1] + part0[z_order[k + 1], :, :, :, cols]
        send = copies.start(ring.at[k - 1], ring.at[k], after)
        yield
    send.wait_recv()
    ring[2] = ring[2] + part0[z, :, :, :, cols]
    send_a = copies.start(ring.at[2, :, 1 - x, :, first_a], plane.at[:2, :, first_a], x_nbr)
    send_b = copies.start(ring.at[2, 1 - y, :, :, first_b], plane.at[:2, :, first_b], y_nbr)
    yield
    send_a.wait_recv()
    plane[:2, :, first_a] = plane[:2, :, first_a] + ring[2, :, x, :, first_a]
    send_a = copies.start(plane.at[1 - y, :, first_a], plane.at[2, :, first_a], y_nbr)
    send_b.wait_recv()
    plane[:2, :, first_b] = plane[:2, :, first_b] + ring[2, y, :, :, first_b]
    send_b = copies.start(plane.at[1 - x, :, first_b], plane.at[2, :, first_b], x_nbr)
    yield
    send_a.wait_recv()
    send_b.wait_recv()
    out[:, cols_a] = (plane[y, :, first_a] + plane[2, :, first_a]).astype(out.dtype)
    out[:, cols_b] = (plane[x, :, first_b] + plane[2, :, first_b]).astype(out.dtype)
    yield


class ScatterProgram:
    def __init__(self):
        self.chunks, self.turn, self.order = [], 0, turns(SCATTER_ORDER)

    def add(self, chunk):
        next(chunk)
        self.chunks.append(chunk)

    def pump(self, count):
        while count and self.turn < len(self.order) and self.order[self.turn] < len(self.chunks):
            next(self.chunks[self.order[self.turn]])
            self.turn += 1
            count -= 1

    def ensure(self, idx):
        while idx not in self.order[:self.turn]:
            assert self.order[self.turn] < len(self.chunks)
            self.pump(1)

    def finish(self, between):
        while self.turn < len(self.order):
            next(between, None)
            self.pump(1)


def dot(first, second):
    return lax.dot_general(first, second, (((1,), (0,)), ((), ())), preferred_element_type=jnp.float32)


def dot_bt(first, second):
    return lax.dot_general(first, second, (((1,), (1,)), ((), ())), preferred_element_type=jnp.float32)


def dot_at(first, second):
    return lax.dot_general(first, second, (((0,), (0,)), ((), ())), preferred_element_type=jnp.float32)


WIDE = 512
PAIR = 128
SEQ = 128
OUT, UP, ACOLS = 3 * WIDE, 4 * WIDE, 8 * WIDE


def normalised(hidden32):
    center = hidden32 - jnp.mean(hidden32, axis=-1, keepdims=True)
    rstd = lax.rsqrt(jnp.mean(center * center, axis=-1, keepdims=True) + EPSILON)
    return center * rstd, rstd


def weight(full, layer, lo, width=WIDE):
    return full[layer, :, :, :, :, :, lo:lo + width].reshape(WIDE, width)


def down_weight_part(full, layer, k):
    return full[layer, k].reshape(WIDE, WIDE)


def rotate(piece, tab):
    piece = piece.reshape(-1, SEQ, PAIR)
    up, down = pltpu.roll(piece, PAIR - 8, 2), pltpu.roll(piece, 8, 2)
    return (piece * tab[0] + up * tab[1] + down * tab[2]).reshape(-1, PAIR)


def rotate_back(piece, tab):
    piece = piece.reshape(-1, SEQ, PAIR)
    turned = (piece * tab[0] + pltpu.roll(piece * tab[1], 8, 2) + pltpu.roll(piece * tab[2], PAIR - 8, 2))
    return turned.reshape(-1, PAIR)


def low_half(rows):
    return lax.broadcasted_iota(jnp.int32, (rows, PAIR), 1) < PAIR // 2


def head_masks():
    first = low_half(SEQ)
    return (jnp.where(first, 1.0, 0.0).astype(jnp.bfloat16), jnp.where(first, 0.0, 1.0).astype(jnp.bfloat16))


def attention_blocks(tokens):
    for s in range(tokens // SEQ):
        for j in range(WIDE // PAIR):
            yield s, j, pl.ds(s * SEQ, SEQ), pl.ds(j * PAIR, PAIR)


def layer_forward(layer, hidden, weights, small, tab, saved, hooks):
    n1, n2, qkv, probs, ctx, slope, act, d_qkv = saved
    wide_w, down_w = weights
    tokens = hidden.shape[0]

    def vec(row):
        return small[pl.ds(layer * SMALL + row, 1), :]

    hidden32 = hidden[...].astype(jnp.float32)
    scaled, _ = normalised(hidden32)
    n1[...] = (scaled * vec(0) + vec(1)).astype(jnp.bfloat16)
    n2[...] = (scaled * vec(3) + vec(4)).astype(jnp.bfloat16)
    hooks('norm')
    low = low_half(tokens)
    qkv_bias = jnp.concatenate([vec(10), vec(11), vec(12)], axis=1)
    group = 6 * PAIR
    for i in range(2):
        part = dot(n1[...], weight(wide_w, layer, i * group, group)) + qkv_bias[:, i * group:(i + 1) * group]
        for jj in range(2):
            first, second, third = (part[:, (3 * jj + m) * PAIR:(3 * jj + m + 1) * PAIR] for m in range(3))
            cols = pl.ds((2 * i + jj) * PAIR, PAIR)
            query = jnp.where(low, first, second)
            key = jnp.where(low, pltpu.roll(first, PAIR // 2, 1), pltpu.roll(third, PAIR // 2, 1))
            qkv[0, :, cols] = rotate(query, tab).astype(jnp.bfloat16)
            qkv[1, :, cols] = rotate(key, tab).astype(jnp.bfloat16)
            qkv[2, :, cols] = jnp.where(low, second, third).astype(jnp.bfloat16)
    hooks('qkv')
    causal = (lax.broadcasted_iota(jnp.int32, (SEQ, SEQ), 0) >= lax.broadcasted_iota(jnp.int32, (SEQ, SEQ), 1))
    masks, low = head_masks(), low_half(SEQ)
    for s, j, rows, cols in attention_blocks(tokens):
        query, key, value = qkv[0, rows, cols], qkv[1, rows, cols], qkv[2, rows, cols]
        heads = []
        for h in range(2):
            scores = dot_bt(query * masks[h], key) * 0.125
            scores = jnp.where(causal, scores, -1e30)
            attn = jnp.exp(scores - jnp.max(scores, axis=-1, keepdims=True))
            attn = attn / jnp.sum(attn, axis=-1, keepdims=True)
            probs[s, j, h] = attn
            heads.append(dot(attn.astype(jnp.bfloat16), value))
        ctx[rows, cols] = jnp.where(low, heads[0], heads[1]).astype(jnp.bfloat16)
        if j == 3:
            hooks('attn')
    total = hidden32 + (dot(ctx[...], weight(wide_w, layer, OUT)) + vec(2))
    hooks('out')
    mlp = None
    for k in range(4):
        pre = dot(n2[...], weight(wide_w, layer, UP + k * WIDE)) + vec(6 + k)
        bell = lax.erf(pre * 0.7071067811865476) + 1.0
        act[:, k * WIDE:(k + 1) * WIDE] = (0.5 * pre * bell).astype(jnp.bfloat16)
        slope[:, k * WIDE:(k + 1) * WIDE] = 0.5 * bell + pre * (jnp.exp(-0.5 * pre * pre) * 0.3989422804014327)
        if k == 0:
            hooks('up')
        term = dot(act[:, k * WIDE:(k + 1) * WIDE], down_weight_part(down_w, layer, k))
        mlp = term if mlp is None else mlp + term
        hooks('mlp')
    return (total + (mlp + vec(5))).astype(jnp.bfloat16)


def layer_backward(layer, hidden, d_out, weights, small, tab, saved, grads, small_grads, hooks):
    n1, n2, qkv, probs, ctx, slope, act, d_qkv = saved
    wide_w, down_w = weights
    wide_g, down_g = grads
    tokens = hidden.shape[0]

    def vec(row):
        return small[pl.ds(layer * SMALL + row, 1), :]

    def put_small(row, value):
        small_grads[pl.ds(layer * SMALL + row, 1), :] = jnp.sum(value, axis=0, keepdims=True)

    def put(lo, value):
        wide_g[:, :, :, :, :, lo:lo + WIDE] = value.reshape(wide_g.shape[:5] + (WIDE,))

    d_out32 = d_out[...].astype(jnp.float32)
    put_small(2, d_out32)
    put_small(5, d_out32)
    half = WIDE // 2
    for k in range(2):
        hooks.free(k)
        value = dot_at(act[...], d_out[:, k * half:(k + 1) * half])
        down_g[:, :, :, :, :, k * half:(k + 1) * half] = value.reshape(down_g.shape[:5] + (half,))
        hooks('down', (1, k * half))
    d_n2 = None
    for k in range(4):
        if k % 2 == 0:
            hooks.free(2 + k // 2)
        d_act = dot_bt(d_out[...], down_weight_part(down_w, layer, k)).astype(jnp.bfloat16)
        d_pre = d_act.astype(jnp.float32) * slope[:, k * WIDE:(k + 1) * WIDE]
        put_small(6 + k, d_pre)
        act[:, k * WIDE:(k + 1) * WIDE] = d_pre.astype(jnp.bfloat16)
        d_pre_bf = act[:, k * WIDE:(k + 1) * WIDE]
        put(UP + k * WIDE, dot_at(n2[...], d_pre_bf))
        term = dot_bt(d_pre_bf, weight(wide_w, layer, UP + k * WIDE))
        d_n2 = term if d_n2 is None else d_n2 + term
        if k % 2:
            hooks('up', (0, UP + (k - 1) * WIDE))
    d_n2 = d_n2.astype(jnp.bfloat16)
    hooks.free(4)
    put(OUT, dot_at(ctx[...], d_out[...]))
    ctx[...] = dot_bt(d_out[...], weight(wide_w, layer, OUT)).astype(jnp.bfloat16)
    hooks('dctx')
    masks, low = head_masks(), low_half(SEQ)
    for s, j, rows, cols in attention_blocks(tokens):
        query, key, value = qkv[0, rows, cols], qkv[1, rows, cols], qkv[2, rows, cols]
        d_ctx = ctx[rows, cols]
        d_q, d_k, d_v = [], [], []
        for h in range(2):
            attn = probs[s, j, h]
            d_probs = dot_bt(d_ctx * masks[h], value).astype(jnp.bfloat16).astype(jnp.float32)
            d_v.append(dot_at(attn.astype(jnp.bfloat16), d_ctx))
            inner = jnp.sum(d_probs * attn, axis=-1, keepdims=True)
            d_scores = (attn * (d_probs - inner) * 0.125).astype(jnp.bfloat16)
            d_q.append(dot(d_scores, key))
            d_k.append(dot_at(d_scores, query))
        qkv[0, rows, cols] = jnp.where(low, d_q[0], d_q[1]).astype(jnp.bfloat16)
        qkv[1, rows, cols] = jnp.where(low, d_k[0], d_k[1]).astype(jnp.bfloat16)
        qkv[2, rows, cols] = jnp.where(low, d_v[0], d_v[1]).astype(jnp.bfloat16)
        if j == 3:
            hooks('dattn')
    low = low_half(tokens)
    for j in range(WIDE // PAIR):
        cols = pl.ds(j * PAIR, PAIR)
        d_query, d_key, d_value = (qkv[t, :, cols].astype(jnp.float32) for t in range(3))
        d_query = rotate_back(d_query, tab)
        d_key = pltpu.roll(rotate_back(d_key, tab), PAIR // 2, 1)
        parts = (jnp.where(low, d_query, d_key), jnp.where(low, d_value, d_query), jnp.where(low, d_key, d_value))
        for m, part in enumerate(parts):
            lo = (3 * j + m) * PAIR
            row = layer * SMALL + 10 + lo // WIDE
            small_grads[pl.ds(row, 1), pl.ds(lo % WIDE, PAIR)] = jnp.sum(part, axis=0, keepdims=True)
            d_qkv[:, lo:lo + PAIR] = part.astype(jnp.bfloat16)
    d_n1 = None
    for t in (2, 1, 0):
        if t == 1:
            hooks.free(5)
        piece = d_qkv[:, t * WIDE:(t + 1) * WIDE]
        put(t * WIDE, dot_at(n1[...], piece))
        term = dot_bt(piece, weight(wide_w, layer, t * WIDE))
        d_n1 = term if d_n1 is None else d_n1 + term
        hooks('dqkv', (0, t * WIDE))
    d_n1 = d_n1.astype(jnp.bfloat16).astype(jnp.float32)
    d_n2 = d_n2.astype(jnp.float32)
    scaled, rstd = normalised(hidden[...].astype(jnp.float32))
    put_small(0, d_n1 * scaled)
    put_small(1, d_n1)
    put_small(3, d_n2 * scaled)
    put_small(4, d_n2)
    d_scaled = d_n1 * vec(0) + d_n2 * vec(3)
    d_hidden = rstd * (d_scaled - jnp.mean(d_scaled, axis=-1, keepdims=True)
                       - scaled * jnp.mean(d_scaled * scaled, axis=-1, keepdims=True))
    return (d_out32 + d_hidden).astype(jnp.bfloat16)


def places(rank, part, width):
    shift = lax.broadcasted_iota(jnp.int32, (part, width), 1) - lax.broadcasted_iota(jnp.int32, (part, width), 0)
    return jnp.where(shift == rank * part, 1.0, 0.0).astype(jnp.bfloat16)


VECTOR_ROWS = ((0, 1), (1, 1), (10, 3), (2, 1), (3, 1), (4, 1), (6, 4), (5, 1))


def place_small(rank, vectors, small_own):
    small_own[...] = jnp.zeros_like(small_own)
    for ref, (row, count) in zip(vectors, VECTOR_ROWS):
        wide = dot(ref[...], places(rank, ref.shape[1], count * WIDE))
        for layer in range(LAYERS):
            for i in range(count):
                small_own[pl.ds(layer * SMALL + row + i, 1), :] = wide[layer:layer + 1, i * WIDE:(i + 1) * WIDE]


def step_kernel(x, y_cot, qkv_own, out_own, up_own, down_own, *refs):
    (gain1, bias1, qkv_b, out_b, gain2, bias2, up_b, down_b, tab,
     y_out, x_grad, wide_out, down_out, small_out,
     wide_own, wide_w, down_w, wide_g, down_g) = refs[:19]
    wide_parts, down_parts = refs[19:24], refs[24:29]
    ring, plane = refs[29:31]
    (small_own, small, small_grads, small_bufs, small_grad_bufs,
     n1, n2, qkv, probs, ctx, slope, act, d_qkv, hidden1, d_hidden1, send_sems, recv_sems) = refs[31:]
    saved = (n1, n2, qkv, probs, ctx, slope, act, d_qkv)
    weights, grads = (wide_w, down_w), (wide_g, down_g)
    pos = positions()
    rank = pos[0] * 8 + pos[1]
    wide_own[:, :, :OUT] = qkv_own[...]
    wide_own[:, :, OUT:UP] = out_own[...]
    wide_own[:, :, UP:] = up_own[...]
    place_small(rank, (gain1, bias1, qkv_b, out_b, gain2, bias2, up_b, down_b), small_own)
    small_grads[...] = jnp.zeros_like(small_grads)
    entry_barrier(pos)
    copies = Copies(send_sems, recv_sems)

    small_gen = small_reduce_steps(copies, pos, small_own, small_bufs, small)
    done = []
    pieces = []
    for i in range(LAYERS):
        pieces.append(gather_steps(copies, pos, wide_own.at[i], wide_w.at[i], 0, UP))
        pieces.append(gather_steps(copies, pos, wide_own.at[i], wide_w.at[i], UP, UP))
        steps = gather_plane_first_steps if i else gather_steps
        pieces.append(steps(copies, pos, down_own.at[i], down_w.at[i], 0, WIDE))
    gather = gather_program(pieces, small_gen, done)

    def gather_until(piece):
        while piece not in done:
            next(gather)

    def gather_pump(count):
        for _ in range(count):
            next(gather, None)

    gather_until(0)

    def forward_hooks(layer):
        counts = counts_of(GATHER_PUMPS[layer])

        def hooks(name):
            if name == 'out':
                gather_until(3 * layer + 1)
            elif name == 'up':
                gather_until(3 * layer + 2)
            else:
                gather_pump(next(counts))
        return hooks

    hidden1[...] = layer_forward(0, x, weights, small, tab, saved, forward_hooks(0))
    gather_until(3)
    y_out[...] = layer_forward(1, hidden1, weights, small, tab, saved, forward_hooks(1))
    gather_until(5)

    program = ScatterProgram()

    def add(layer, kind, lo):
        if kind and lo == 0:
            steps = scatter_z_first_steps(copies, pos, down_g, down_parts[0].at[layer], ring.at[layer], plane.at[layer],
                                          down_out.at[layer], lo, WIDE // 2)
        else:
            width = WIDE // 2 if kind else WIDE if layer == 0 and lo < 2 * WIDE else 2 * WIDE
            parts = (wide_parts, down_parts)[kind]
            steps = scatter_chunk_steps(copies, pos, grads[kind], *(ref.at[layer] for ref in parts),
                                        (wide_out, down_out)[kind].at[layer], lo, width)
        program.add(steps)

    class Hooks:
        def __init__(self, layer, counts, reused):
            self.layer, self.counts, self.reused = layer, counts_of(counts), reused

        def free(self, idx):
            if self.reused:
                program.ensure(idx)

        def __call__(self, name, chunk=None):
            if chunk is not None and (self.layer == 0 or chunk != (0, WIDE)):
                add(self.layer, *chunk)
            program.pump(next(self.counts))

    d_hidden1[...] = layer_backward(1, hidden1, y_cot, weights, small, tab, saved, grads, small_grads,
                                    Hooks(1, SCATTER_PUMPS[0], False))
    layer_forward(0, x, weights, small, tab, saved, Hooks(0, SCATTER_PUMPS[1], False))
    x_grad[...] = layer_backward(0, x, d_hidden1, weights, small, tab, saved, grads, small_grads,
                                 Hooks(0, SCATTER_PUMPS[2], True))
    small_gen = small_reduce_steps(copies, pos, small_grads, small_grad_bufs, small_out)
    program.finish(small_gen)
    for _ in small_gen:
        pass
    copies.finish()


def part_scratch(rows, width):
    return [pltpu.VMEM((LAYERS, 4, 2, 2, rows, width), jnp.float32),
            pltpu.VMEM((LAYERS, 4, 2, rows, width // 2), jnp.float32),
            pltpu.VMEM((LAYERS, 4, 2, rows, width // 2), jnp.float32),
            pltpu.VMEM((LAYERS, 4, rows, width), jnp.float32),
            pltpu.VMEM((LAYERS, 3, rows, width), jnp.float32)]


def step_call(x, y_cot, matrices, vectors, tab):
    tokens, d_model = x.shape
    rows, down_rows = matrices[1].shape[1], matrices[3].shape[1]
    vmem = pl.BlockSpec(memory_space=pltpu.VMEM)
    bf16, f32 = jnp.bfloat16, jnp.float32
    small = (LAYERS * SMALL, d_model)
    n_sems = 6 * 2 + 6 * 23 + 8 * 13
    return pl.pallas_call(
        step_kernel,
        out_shape=(jax.ShapeDtypeStruct(x.shape, bf16), jax.ShapeDtypeStruct(x.shape, bf16),
                   jax.ShapeDtypeStruct((LAYERS, rows, ACOLS), bf16),
                   jax.ShapeDtypeStruct((LAYERS, down_rows, d_model), bf16), jax.ShapeDtypeStruct(small, f32)),
        in_specs=[vmem] * (2 + 4 + 8 + 1), out_specs=(vmem,) * 5,
        scratch_shapes=[
            pltpu.VMEM((LAYERS, rows, ACOLS), bf16),
            pltpu.VMEM((LAYERS, 4, 2, 2, 2, rows, ACOLS), bf16),
            pltpu.VMEM((LAYERS, 4, 2, 2, 2, down_rows, d_model), bf16),
            pltpu.VMEM((4, 2, 2, 2, rows, ACOLS), f32),
            pltpu.VMEM((4, 2, 2, 2, down_rows, d_model), f32),
            *part_scratch(rows, ACOLS), *part_scratch(down_rows, d_model),
            pltpu.VMEM((LAYERS, 3, 2, 2, down_rows, d_model // 2), f32),
            pltpu.VMEM((LAYERS, 3, down_rows, d_model // 2), f32),
            pltpu.VMEM(small, f32),
            pltpu.VMEM(small, f32),
            pltpu.VMEM(small, f32),
            pltpu.VMEM((9,) + small, f32),
            pltpu.VMEM((9,) + small, f32),
            pltpu.VMEM((tokens, d_model), bf16),
            pltpu.VMEM((tokens, d_model), bf16),
            pltpu.VMEM((3, tokens, d_model), bf16),
            pltpu.VMEM((tokens // SEQ, 4, 2, SEQ, SEQ), f32),
            pltpu.VMEM((tokens, d_model), bf16),
            pltpu.VMEM((tokens, 4 * d_model), f32),
            pltpu.VMEM((tokens, 4 * d_model), bf16),
            pltpu.VMEM((tokens, 3 * d_model), bf16),
            pltpu.VMEM((tokens, d_model), bf16),
            pltpu.VMEM((tokens, d_model), bf16),
            pltpu.SemaphoreType.DMA((n_sems,)), pltpu.SemaphoreType.DMA((n_sems,))],
        compiler_params=pltpu.CompilerParams(collective_id=0, has_side_effects=True,
                                             vmem_limit_bytes=67043328),
    )(x, y_cot, *matrices, *vectors, tab)


def finish_kernel(y_in, x_grad_in, wide, down, small, y_out, x_grad, gain1, bias1, qkv_g, qkv_b, out_g, out_b,
                  gain2, bias2, up_g, up_b, down_g, down_b):
    y_out[...] = y_in[...]
    x_grad[...] = x_grad_in[...]
    qkv_g[...] = wide[:, :, :OUT]
    out_g[...] = wide[:, :, OUT:UP]
    up_g[...] = wide[:, :, UP:]
    down_g[...] = down[...]
    rank = lax.axis_index('node') * 8 + lax.axis_index('local')
    for ref, (row, count) in zip((gain1, bias1, qkv_b, out_b, gain2, bias2, up_b, down_b), VECTOR_ROWS):
        sums = []
        for layer in range(LAYERS):
            lines = [small[pl.ds(layer * SMALL + row + i, 1), :] for i in range(count)]
            sums.append(jnp.concatenate(lines, axis=1))
        sums = jnp.concatenate(sums, axis=0).astype(jnp.bfloat16)
        ref[...] = dot_bt(sums, places(rank, ref.shape[1], count * WIDE)).astype(jnp.bfloat16)


def finish_call(y, x_grad, wide, down, small, shapes):
    vmem = pl.BlockSpec(memory_space=pltpu.VMEM)
    return pl.pallas_call(
        finish_kernel, out_shape=tuple(jax.ShapeDtypeStruct(s, jnp.bfloat16) for s in shapes),
        in_specs=[vmem] * 5, out_specs=(vmem,) * len(shapes),
    )(y, x_grad, wide, down, small)


def rope_table(seq_len, rot_dim):
    inv_freq = 1.0 / (np.float32(10000.0) ** (np.arange(0, rot_dim, 2, dtype=np.float32) / np.float32(rot_dim)))
    angles = np.arange(seq_len, dtype=np.float32)[:, None] * inv_freq[None, :].astype(np.float32)
    cos, sin = np.cos(angles), np.sin(angles)
    none = np.zeros_like(sin)
    rest = np.zeros((seq_len, 3 * rot_dim), np.float32)
    parts = ([cos, cos, rest + 1.0], [-sin, none, rest], [none, sin, rest])
    return np.stack([np.tile(np.concatenate(p, axis=-1), (1, 2)) for p in parts]).astype(np.float32)


def solution(mesh):
    shard_axes = ('node', 'local')
    act_spec = P(shard_axes)
    param_spec = P(None, shard_axes)

    def device_step(x, y_cot, ln1_gain, ln1_bias, qkv_weight, qkv_bias, out_weight, out_bias,
                    ln2_gain, ln2_bias, up_weight, up_bias, down_weight, down_bias):
        d_model, rows = x.shape[2], out_weight.shape[1]
        flat = (x.shape[0] * x.shape[1], d_model)
        qkv_flat = (LAYERS, rows, 3 * d_model)
        matrices = (qkv_weight.reshape(qkv_flat), out_weight, up_weight, down_weight)
        vectors = (ln1_gain, ln1_bias, qkv_bias, out_bias, ln2_gain, ln2_bias, up_bias, down_bias)
        sums = step_call(x.reshape(flat), y_cot.reshape(flat), matrices, vectors, rope_table(x.shape[1], qkv_weight.shape[3] // 12))
        shapes = [flat, flat, ln1_gain.shape, ln1_bias.shape, qkv_flat, qkv_bias.shape, out_weight.shape, out_bias.shape,
                  ln2_gain.shape, ln2_bias.shape, up_weight.shape, up_bias.shape, down_weight.shape, down_bias.shape]
        outs = list(finish_call(*sums, shapes))
        outs[0], outs[1], outs[4] = outs[0].reshape(x.shape), outs[1].reshape(x.shape), outs[4].reshape(qkv_weight.shape)
        return tuple(outs)

    return jax.shard_map(device_step, mesh=mesh,
                         in_specs=(act_spec, act_spec) + (param_spec,) * 12,
                         out_specs=(act_spec, act_spec) + (param_spec,) * 12,
                         check_vma=False)
```

```python
import functools
import jax
import numpy as np
import jax.numpy as jnp
from jax import lax
from jax.experimental import pallas as pl
from jax.experimental.pallas import tpu as pltpu
from jax.sharding import PartitionSpec as P

EPSILON = 1e-5
MESH = pl.DeviceIdType.MESH
LAYERS = 2
ROWS = 16
SMALL = 16
WIDE = 512
PAIR = 128
SEQ = 128
OUT, UP, ACOLS = 3 * WIDE, 4 * WIDE, 8 * WIDE


def positions():
    z = lax.axis_index('node')
    l = lax.axis_index('local')
    c = l % 2
    x = (l // 2) % 2
    y = l // 4
    partner = (z, l + 1 - 2 * c)
    x_nbr = (z, l + 2 - 4 * x)
    y_nbr = (z, (l + 4) % 8)
    z_others = [z + 1 - 2 * (z % 2), (z + 2) % 4, 3 - z]
    return z, l, c, x, y, partner, x_nbr, y_nbr, z_others


def ring_of(z, l):
    return ((z + 1) % 4, l), [z, (z + 3) % 4, (z + 2) % 4, (z + 1) % 4]


def entry_barrier(pos):
    z, l, c, x, y, partner, x_nbr, y_nbr, z_others = pos
    barrier = pltpu.get_barrier_semaphore()
    for dev in [partner, x_nbr, y_nbr] + [(zo, l) for zo in z_others]:
        pl.semaphore_signal(barrier, inc=1, device_id=dev, device_id_type=MESH)
    pl.semaphore_wait(barrier, 6)


class Copies:
    def __init__(self, send_sems, recv_sems):
        self.send_sems, self.recv_sems, self.used = send_sems, recv_sems, 0
        self.open_sends = []

    def make(self, src, dst, dev):
        idx = self.used
        self.used += 1
        return pltpu.make_async_remote_copy(src_ref=src, dst_ref=dst, send_sem=self.send_sems.at[idx],
                                            recv_sem=self.recv_sems.at[idx], device_id=dev, device_id_type=MESH)

    def start(self, src, dst, dev):
        copy = self.make(src, dst, dev)
        copy.start()
        self.open_sends.append(copy)
        return copy

    def finish(self):
        for copy in self.open_sends:
            copy.wait_send()
        self.open_sends = []


def small_reduce_steps(copies, pos, src, bufs, out):
    z, l, c, x, y, partner, x_nbr, y_nbr, z_others = pos
    held = src
    for step, dev in enumerate((partner, x_nbr, y_nbr)):
        copy = copies.start(held, bufs.at[2 * step], dev)
        yield
        copy.wait_recv()
        bufs[2 * step + 1] = held[...] + bufs[2 * step]
        held = bufs.at[2 * step + 1]
    sends = [copies.start(held, bufs.at[6 + k], (zo, l)) for k, zo in enumerate(z_others)]
    yield
    for copy in sends:
        copy.wait_recv()
    out[...] = (held[...] + bufs[6]) + (bufs[7] + bufs[8])
    yield


def gather_steps(copies, pos, own, full, lo, width):
    z, l, c, x, y, partner, x_nbr, y_nbr, z_others = pos
    half = width // 2
    cols, cols_a, cols_b = pl.ds(lo, width), pl.ds(lo, half), pl.ds(lo + half, half)
    after, z_order = ring_of(z, l)

    def block(zz, yy, xx, cc):
        return full.at[zz, yy, xx, cc, :, cols]

    from_z, from_x, from_y, diag, to_partner = [None] * 4, [None] * 4, [None] * 4, [], []

    def spread(k, got, place):
        if k < 3:
            from_z[k + 1] = copies.start(got, place, after)
        from_x[k] = copies.start(got, place, x_nbr)
        from_y[k] = copies.start(got, place, y_nbr)

    def forward_z(k):
        from_z[k].wait_recv()
        got = block(z_order[k], y, x, c)
        spread(k, got, got)

    def forward_cross(k):
        zz = z_order[k]
        from_x[k].wait_recv()
        got = full.at[zz, y, 1 - x, c, :, cols_a]
        diag.append(copies.start(got, got, y_nbr))
        from_y[k].wait_recv()
        got = full.at[zz, 1 - y, x, c, :, cols_b]
        diag.append(copies.start(got, got, x_nbr))

    def forward_partner(yy, xx):
        got = full.at[:, yy, xx, c, :, cols]
        to_partner.append(copies.start(got, got, partner))

    spread(0, own.at[:, cols], block(z, y, x, c))
    full[z, y, x, c, :, cols] = own[:, cols]
    yield
    forward_z(1)
    yield
    forward_cross(0)
    yield
    forward_z(2)
    yield
    forward_cross(1)
    yield
    forward_z(3)
    forward_partner(y, x)
    yield
    forward_cross(2)
    yield
    forward_cross(3)
    forward_partner(y, 1 - x)
    forward_partner(1 - y, x)
    yield
    for copy in diag:
        copy.wait_recv()
    forward_partner(1 - y, 1 - x)
    yield
    for copy in to_partner:
        copy.wait_recv()
    yield


def gather_plane_first_steps(copies, pos, own, full, lo, width):
    z, l, c, x, y, partner, x_nbr, y_nbr, z_others = pos
    half = width // 2
    cols, cols_a, cols_b = pl.ds(lo, width), pl.ds(lo, half), pl.ds(lo + half, half)
    after, z_order = ring_of(z, l)
    mine, own_cols = full.at[z, y, x, c, :, cols], own.at[:, cols]
    from_x = copies.start(own_cols, mine, x_nbr)
    from_y = copies.start(own_cols, mine, y_nbr)
    full[z, y, x, c, :, cols] = own[:, cols]
    yield
    from_x.wait_recv()
    got = full.at[z, y, 1 - x, c, :, cols_a]
    diag_y = copies.start(got, got, y_nbr)
    from_y.wait_recv()
    got = full.at[z, 1 - y, x, c, :, cols_b]
    diag_x = copies.start(got, got, x_nbr)
    yield
    diag_y.wait_recv()
    diag_x.wait_recv()
    to_partner = []
    for k in range(4):
        got = full.at[z_order[k], :, :, c, :, cols]
        if k < 3:
            from_z = copies.start(got, got, after)
        to_partner.append(copies.start(got, got, partner))
        yield
        if k < 3:
            from_z.wait_recv()
    for copy in to_partner:
        copy.wait_recv()
    yield


GATHER_ORDER = 'acfbacfbdeaaacccfbbbdeacaafccbacabbdddceeebbfdeddeededfef'
SMALL_TURNS = (3, 6, 10, 14, 18)
GATHER_PUMPS = ('14400305', '01100503')
SCATTER_ORDERS = ('abcabdcbaedcbfedacgfebdahgfcaeigdfjhiegkjifhlkjgibmlkhjcnmli', 'khdomjhlenkmfonlgominjoklm')
SCATTER_PUMPS = ('0304101110', '0012002313', '0124432324')
DIRECT = (0, WIDE)


def turns(letters):
    return [ord(letter) - ord('a') for letter in letters]


def counts_of(digits):
    return iter([int(digit) for digit in digits])


def gather_program(pieces, small_gen, done):
    order = turns(GATHER_ORDER)
    left = [order.count(i) for i in range(len(pieces))]
    for turn, i in enumerate(order):
        if turn in SMALL_TURNS:
            next(small_gen)
        next(pieces[i])
        left[i] -= 1
        if not left[i]:
            done.append(i)
        yield


def scatter_chunk_steps(copies, pos, grads, part0, partx, party, last, partz, out, lo, width, direct):
    z, l, c, x, y, partner, x_nbr, y_nbr, z_others = pos
    half = width // 2
    cols, cols_a, cols_b = pl.ds(lo, width), pl.ds(lo, half), pl.ds(lo + half, half)
    after, z_order = ring_of(z, l)
    hcols = pl.ds(lo // 2, half)
    swap = copies.make(grads.at[:, :, :, 1 - c, :, cols], part0.at[:, :, :, :, cols], partner)
    swap.start()
    yield
    swap.wait()
    part0[:, :, :, :, cols] = part0[:, :, :, :, cols] + grads[:, :, :, c, :, cols]
    send_a = copies.start(part0.at[:, :, 1 - x, :, cols_a], partx.at[:, :, :, hcols], x_nbr)
    send_b = copies.start(part0.at[:, 1 - y, :, :, cols_b], party.at[:, :, :, hcols], y_nbr)
    yield
    send_a.wait_recv()
    partx[:, :, :, hcols] = partx[:, :, :, hcols] + part0[:, :, x, :, cols_a]
    send_a = copies.start(partx.at[:, 1 - y, :, hcols], last.at[:, :, cols_a], y_nbr)
    send_b.wait_recv()
    party[:, :, :, hcols] = party[:, :, :, hcols] + part0[:, y, :, :, cols_b]
    send_b = copies.start(party.at[:, 1 - x, :, hcols], last.at[:, :, cols_b], x_nbr)
    yield
    send_a.wait_recv()
    send_b.wait_recv()
    last[:, :, cols_a] = last[:, :, cols_a] + partx[:, y, :, hcols]
    last[:, :, cols_b] = last[:, :, cols_b] + party[:, x, :, hcols]
    if direct:
        sends = [copies.start(last.at[zo, :, cols], partz.at[k, :, cols], (zo, l)) for k, zo in enumerate(z_others)]
        yield
        for copy in sends:
            copy.wait_recv()
        total = (last[z, :, cols] + partz[0, :, cols]) + (partz[1, :, cols] + partz[2, :, cols])
    else:
        send = copies.start(last.at[z_order[1], :, cols], partz.at[0, :, cols], after)
        yield
        for k in (1, 2):
            send.wait_recv()
            partz[k - 1, :, cols] = partz[k - 1, :, cols] + last[z_order[k + 1], :, cols]
            send = copies.start(partz.at[k - 1, :, cols], partz.at[k, :, cols], after)
            yield
        send.wait_recv()
        total = partz[2, :, cols] + last[z, :, cols]
    out[:, cols] = total.astype(out.dtype)
    yield


def scatter_z_first_steps(copies, pos, grads, part0, ring, plane, out, lo, width):
    z, l, c, x, y, partner, x_nbr, y_nbr, z_others = pos
    half = width // 2
    cols, cols_a, cols_b = pl.ds(lo, width), pl.ds(lo, half), pl.ds(lo + half, half)
    first_a, first_b = pl.ds(0, half), pl.ds(half, half)
    after, z_order = ring_of(z, l)
    swap = copies.make(grads.at[:, :, :, 1 - c, :, cols], part0.at[:, :, :, :, cols], partner)
    swap.start()
    yield
    swap.wait()
    part0[:, :, :, :, cols] = part0[:, :, :, :, cols] + grads[:, :, :, c, :, cols]
    send = copies.start(part0.at[z_order[1], :, :, :, cols], ring.at[0], after)
    yield
    for k in (1, 2):
        send.wait_recv()
        ring[k - 1] = ring[k - 1] + part0[z_order[k + 1], :, :, :, cols]
        send = copies.start(ring.at[k - 1], ring.at[k], after)
        yield
    send.wait_recv()
    ring[2] = ring[2] + part0[z, :, :, :, cols]
    send_a = copies.start(ring.at[2, :, 1 - x, :, first_a], plane.at[:2, :, first_a], x_nbr)
    send_b = copies.start(ring.at[2, 1 - y, :, :, first_b], plane.at[:2, :, first_b], y_nbr)
    yield
    send_a.wait_recv()
    plane[:2, :, first_a] = plane[:2, :, first_a] + ring[2, :, x, :, first_a]
    send_a = copies.start(plane.at[1 - y, :, first_a], plane.at[2, :, first_a], y_nbr)
    send_b.wait_recv()
    plane[:2, :, first_b] = plane[:2, :, first_b] + ring[2, y, :, :, first_b]
    send_b = copies.start(plane.at[1 - x, :, first_b], plane.at[2, :, first_b], x_nbr)
    yield
    send_a.wait_recv()
    send_b.wait_recv()
    out[:, cols_a] = (plane[y, :, first_a] + plane[2, :, first_a]).astype(out.dtype)
    out[:, cols_b] = (plane[x, :, first_b] + plane[2, :, first_b]).astype(out.dtype)
    yield


class ScatterProgram:
    def __init__(self):
        self.chunks, self.turn, self.order = [], 0, [chunk for part in SCATTER_ORDERS for chunk in turns(part)]

    def add(self, chunk):
        next(chunk)
        self.chunks.append(chunk)

    def pump(self, count):
        while count and self.turn < len(self.order) and self.order[self.turn] < len(self.chunks):
            next(self.chunks[self.order[self.turn]])
            self.turn += 1
            count -= 1

    def ensure(self, idx):
        while idx not in self.order[:self.turn]:
            assert self.order[self.turn] < len(self.chunks)
            self.pump(1)

    def finish(self, between):
        while self.turn < len(self.order):
            next(between, None)
            self.pump(1)


def dot(first, second):
    return lax.dot_general(first, second, (((1,), (0,)), ((), ())), preferred_element_type=jnp.float32)


def dot_bt(first, second):
    return lax.dot_general(first, second, (((1,), (1,)), ((), ())), preferred_element_type=jnp.float32)


def dot_at(first, second):
    return lax.dot_general(first, second, (((0,), (0,)), ((), ())), preferred_element_type=jnp.float32)


def normalised(hidden32):
    center = hidden32 - jnp.mean(hidden32, axis=-1, keepdims=True)
    rstd = lax.rsqrt(jnp.mean(center * center, axis=-1, keepdims=True) + EPSILON)
    return center * rstd, rstd


def weight(full, layer, lo, width=WIDE):
    return full[layer, :, :, :, :, :, lo:lo + width].reshape(WIDE, width)


def down_weight_part(full, layer, k):
    return full[layer, k].reshape(WIDE, WIDE)


def rotate(piece, tab):
    piece = piece.reshape(-1, SEQ, PAIR)
    up, down = pltpu.roll(piece, PAIR - 8, 2), pltpu.roll(piece, 8, 2)
    return (piece * tab[0] + up * tab[1] + down * tab[2]).reshape(-1, PAIR)


def rotate_back(piece, tab):
    piece = piece.reshape(-1, SEQ, PAIR)
    turned = (piece * tab[0] + pltpu.roll(piece * tab[1], 8, 2) + pltpu.roll(piece * tab[2], PAIR - 8, 2))
    return turned.reshape(-1, PAIR)


def low_half(rows):
    return lax.broadcasted_iota(jnp.int32, (rows, PAIR), 1) < PAIR // 2


def head_masks():
    first = low_half(SEQ)
    return (jnp.where(first, 1.0, 0.0).astype(jnp.bfloat16), jnp.where(first, 0.0, 1.0).astype(jnp.bfloat16))


def attention_blocks(tokens):
    for s in range(tokens // SEQ):
        for j in range(WIDE // PAIR):
            yield s, j, pl.ds(s * SEQ, SEQ), pl.ds(j * PAIR, PAIR)


def layer_forward(layer, hidden, weights, small, tab, saved, hooks):
    n1, n2, qkv, probs, ctx, slope, act, d_qkv = saved
    wide_w, down_w = weights
    tokens = hidden.shape[0]

    def vec(row):
        return small[pl.ds(layer * SMALL + row, 1), :]

    hidden32 = hidden[...].astype(jnp.float32)
    scaled, _ = normalised(hidden32)
    n1[...] = (scaled * vec(0) + vec(1)).astype(jnp.bfloat16)
    n2[...] = (scaled * vec(3) + vec(4)).astype(jnp.bfloat16)
    hooks('norm')
    low = low_half(tokens)
    qkv_bias = jnp.concatenate([vec(10), vec(11), vec(12)], axis=1)
    group = 6 * PAIR
    for i in range(2):
        part = dot(n1[...], weight(wide_w, layer, i * group, group)) + qkv_bias[:, i * group:(i + 1) * group]
        for jj in range(2):
            first, second, third = (part[:, (3 * jj + m) * PAIR:(3 * jj + m + 1) * PAIR] for m in range(3))
            cols = pl.ds((2 * i + jj) * PAIR, PAIR)
            query = jnp.where(low, first, second)
            key = jnp.where(low, pltpu.roll(first, PAIR // 2, 1), pltpu.roll(third, PAIR // 2, 1))
            qkv[0, :, cols] = rotate(query, tab).astype(jnp.bfloat16)
            qkv[1, :, cols] = rotate(key, tab).astype(jnp.bfloat16)
            qkv[2, :, cols] = jnp.where(low, second, third).astype(jnp.bfloat16)
    hooks('qkv')
    causal = (lax.broadcasted_iota(jnp.int32, (SEQ, SEQ), 0) >= lax.broadcasted_iota(jnp.int32, (SEQ, SEQ), 1))
    masks, low = head_masks(), low_half(SEQ)
    for s, j, rows, cols in attention_blocks(tokens):
        query, key, value = qkv[0, rows, cols], qkv[1, rows, cols], qkv[2, rows, cols]
        heads = []
        for h in range(2):
            scores = dot_bt(query * masks[h], key) * 0.125
            scores = jnp.where(causal, scores, -1e30)
            attn = jnp.exp(scores - jnp.max(scores, axis=-1, keepdims=True))
            attn = attn / jnp.sum(attn, axis=-1, keepdims=True)
            probs[s, j, h] = attn
            heads.append(dot(attn.astype(jnp.bfloat16), value))
        ctx[rows, cols] = jnp.where(low, heads[0], heads[1]).astype(jnp.bfloat16)
        if j == 3:
            hooks('attn')
    total = hidden32 + (dot(ctx[...], weight(wide_w, layer, OUT)) + vec(2))
    hooks('out')
    mlp = None
    for k in range(4):
        pre = dot(n2[...], weight(wide_w, layer, UP + k * WIDE)) + vec(6 + k)
        bell = lax.erf(pre * 0.7071067811865476) + 1.0
        act[:, k * WIDE:(k + 1) * WIDE] = (0.5 * pre * bell).astype(jnp.bfloat16)
        slope[:, k * WIDE:(k + 1) * WIDE] = 0.5 * bell + pre * (jnp.exp(-0.5 * pre * pre) * 0.3989422804014327)
        if k == 0:
            hooks('up')
        term = dot(act[:, k * WIDE:(k + 1) * WIDE], down_weight_part(down_w, layer, k))
        mlp = term if mlp is None else mlp + term
        hooks('mlp')
    return (total + (mlp + vec(5))).astype(jnp.bfloat16)


def layer_backward(layer, hidden, d_out, weights, small, tab, saved, grads, small_grads, hooks):
    n1, n2, qkv, probs, ctx, slope, act, d_qkv = saved
    wide_w, down_w = weights
    wide_g, down_g = grads
    tokens = hidden.shape[0]

    def vec(row):
        return small[pl.ds(layer * SMALL + row, 1), :]

    def put_small(row, value):
        small_grads[pl.ds(layer * SMALL + row, 1), :] = jnp.sum(value, axis=0, keepdims=True)

    def put(lo, value):
        wide_g[:, :, :, :, :, lo:lo + WIDE] = value.reshape(wide_g.shape[:5] + (WIDE,))

    d_out32 = d_out[...].astype(jnp.float32)
    put_small(2, d_out32)
    put_small(5, d_out32)
    half = WIDE // 2
    for k in range(2):
        hooks.free(k)
        value = dot_at(act[...], d_out[:, k * half:(k + 1) * half])
        down_g[:, :, :, :, :, k * half:(k + 1) * half] = value.reshape(down_g.shape[:5] + (half,))
        hooks('down', (1, k * half))
    d_n2 = None
    for k in range(4):
        if k % 2 == 0:
            hooks.free(2 + k // 2)
        d_act = dot_bt(d_out[...], down_weight_part(down_w, layer, k)).astype(jnp.bfloat16)
        d_pre = d_act.astype(jnp.float32) * slope[:, k * WIDE:(k + 1) * WIDE]
        put_small(6 + k, d_pre)
        act[:, k * WIDE:(k + 1) * WIDE] = d_pre.astype(jnp.bfloat16)
        d_pre_bf = act[:, k * WIDE:(k + 1) * WIDE]
        put(UP + k * WIDE, dot_at(n2[...], d_pre_bf))
        term = dot_bt(d_pre_bf, weight(wide_w, layer, UP + k * WIDE))
        d_n2 = term if d_n2 is None else d_n2 + term
        if k % 2:
            hooks('up', (0, UP + (k - 1) * WIDE))
    d_n2 = d_n2.astype(jnp.bfloat16)
    hooks.free(4)
    put(OUT, dot_at(ctx[...], d_out[...]))
    ctx[...] = dot_bt(d_out[...], weight(wide_w, layer, OUT)).astype(jnp.bfloat16)
    hooks('dctx', (0, OUT))
    masks, low = head_masks(), low_half(SEQ)
    for s, j, rows, cols in attention_blocks(tokens):
        query, key, value = qkv[0, rows, cols], qkv[1, rows, cols], qkv[2, rows, cols]
        d_ctx = ctx[rows, cols]
        d_q, d_k, d_v = [], [], []
        for h in range(2):
            attn = probs[s, j, h]
            d_probs = dot_bt(d_ctx * masks[h], value).astype(jnp.bfloat16).astype(jnp.float32)
            d_v.append(dot_at(attn.astype(jnp.bfloat16), d_ctx))
            inner = jnp.sum(d_probs * attn, axis=-1, keepdims=True)
            d_scores = (attn * (d_probs - inner) * 0.125).astype(jnp.bfloat16)
            d_q.append(dot(d_scores, key))
            d_k.append(dot_at(d_scores, query))
        qkv[0, rows, cols] = jnp.where(low, d_q[0], d_q[1]).astype(jnp.bfloat16)
        qkv[1, rows, cols] = jnp.where(low, d_k[0], d_k[1]).astype(jnp.bfloat16)
        qkv[2, rows, cols] = jnp.where(low, d_v[0], d_v[1]).astype(jnp.bfloat16)
        if j == 3:
            hooks('dattn')
    low = low_half(tokens)
    for j in range(WIDE // PAIR):
        cols = pl.ds(j * PAIR, PAIR)
        d_query, d_key, d_value = (qkv[t, :, cols].astype(jnp.float32) for t in range(3))
        d_query = rotate_back(d_query, tab)
        d_key = pltpu.roll(rotate_back(d_key, tab), PAIR // 2, 1)
        parts = (jnp.where(low, d_query, d_key), jnp.where(low, d_value, d_query), jnp.where(low, d_key, d_value))
        for m, part in enumerate(parts):
            lo = (3 * j + m) * PAIR
            row = layer * SMALL + 10 + lo // WIDE
            small_grads[pl.ds(row, 1), pl.ds(lo % WIDE, PAIR)] = jnp.sum(part, axis=0, keepdims=True)
            d_qkv[:, lo:lo + PAIR] = part.astype(jnp.bfloat16)
    d_n1 = None
    for t in (2, 1, 0):
        if t:
            hooks.free(7 - t)
        piece = d_qkv[:, t * WIDE:(t + 1) * WIDE]
        put(t * WIDE, dot_at(n1[...], piece))
        term = dot_bt(piece, weight(wide_w, layer, t * WIDE))
        d_n1 = term if d_n1 is None else d_n1 + term
        hooks('dqkv', (0, t * WIDE))
    d_n1 = d_n1.astype(jnp.bfloat16).astype(jnp.float32)
    d_n2 = d_n2.astype(jnp.float32)
    scaled, rstd = normalised(hidden[...].astype(jnp.float32))
    put_small(0, d_n1 * scaled)
    put_small(1, d_n1)
    put_small(3, d_n2 * scaled)
    put_small(4, d_n2)
    d_scaled = d_n1 * vec(0) + d_n2 * vec(3)
    d_hidden = rstd * (d_scaled - jnp.mean(d_scaled, axis=-1, keepdims=True)
                       - scaled * jnp.mean(d_scaled * scaled, axis=-1, keepdims=True))
    return (d_out32 + d_hidden).astype(jnp.bfloat16)


def places(rank, part, width):
    shift = lax.broadcasted_iota(jnp.int32, (part, width), 1) - lax.broadcasted_iota(jnp.int32, (part, width), 0)
    return jnp.where(shift == rank * part, 1.0, 0.0).astype(jnp.bfloat16)


VECTOR_ROWS = ((0, 1), (1, 1), (10, 3), (2, 1), (3, 1), (4, 1), (6, 4), (5, 1))


def place_small(rank, vectors, small_own):
    small_own[...] = jnp.zeros_like(small_own)
    for ref, (row, count) in zip(vectors, VECTOR_ROWS):
        wide = dot(ref[...], places(rank, ref.shape[1], count * WIDE))
        for layer in range(LAYERS):
            for i in range(count):
                small_own[pl.ds(layer * SMALL + row + i, 1), :] = wide[layer:layer + 1, i * WIDE:(i + 1) * WIDE]


def step_kernel(x, y_cot, qkv_own, out_own, up_own, down_own, *refs):
    (gain1, bias1, qkv_b, out_b, gain2, bias2, up_b, down_b, tab,
     y_out, x_grad, wide_out, down_out, small_out,
     wide_own, wide_w, down_w, wide_g, down_g) = refs[:19]
    wide_parts, down_parts = refs[19:24], refs[24:29]
    ring, plane = refs[29:31]
    (small_own, small, small_grads, small_bufs, small_grad_bufs,
     n1, n2, qkv, probs, ctx, slope, act, d_qkv, hidden1, d_hidden1, send_sems, recv_sems) = refs[31:]
    saved = (n1, n2, qkv, probs, ctx, slope, act, d_qkv)
    weights, grads = (wide_w, down_w), (wide_g, down_g)
    pos = positions()
    rank = pos[0] * 8 + pos[1]
    wide_own[:, :, :OUT] = qkv_own[...]
    wide_own[:, :, OUT:UP] = out_own[...]
    wide_own[:, :, UP:] = up_own[...]
    place_small(rank, (gain1, bias1, qkv_b, out_b, gain2, bias2, up_b, down_b), small_own)
    small_grads[...] = jnp.zeros_like(small_grads)
    entry_barrier(pos)
    copies = Copies(send_sems, recv_sems)

    small_gen = small_reduce_steps(copies, pos, small_own, small_bufs, small)
    done = []
    pieces = []
    for i in range(LAYERS):
        pieces.append(gather_steps(copies, pos, wide_own.at[i], wide_w.at[i], 0, UP))
        pieces.append(gather_steps(copies, pos, wide_own.at[i], wide_w.at[i], UP, UP))
        steps = gather_plane_first_steps if i else gather_steps
        pieces.append(steps(copies, pos, down_own.at[i], down_w.at[i], 0, WIDE))
    gather = gather_program(pieces, small_gen, done)

    def gather_until(piece):
        while piece not in done:
            next(gather)

    def gather_pump(count):
        for _ in range(count):
            next(gather, None)

    gather_until(0)

    def forward_hooks(layer):
        counts = counts_of(GATHER_PUMPS[layer])

        def hooks(name):
            if name == 'out':
                gather_until(3 * layer + 1)
            elif name == 'up':
                gather_until(3 * layer + 2)
            else:
                gather_pump(next(counts))
        return hooks

    hidden1[...] = layer_forward(0, x, weights, small, tab, saved, forward_hooks(0))
    gather_until(3)
    y_out[...] = layer_forward(1, hidden1, weights, small, tab, saved, forward_hooks(1))
    gather_until(5)

    program = ScatterProgram()

    def add(layer, kind, lo):
        if kind and lo == 0:
            steps = scatter_z_first_steps(copies, pos, down_g, down_parts[0].at[layer], ring.at[layer], plane.at[layer],
                                          down_out.at[layer], lo, WIDE // 2)
        else:
            width = WIDE // 2 if kind else WIDE if OUT <= lo < UP or (layer == 0 or lo) and lo < OUT else 2 * WIDE
            parts = (wide_parts, down_parts)[kind]
            steps = scatter_chunk_steps(copies, pos, grads[kind], *(ref.at[layer] for ref in parts),
                                        (wide_out, down_out)[kind].at[layer], lo, width, layer == 0 and lo in DIRECT)
        program.add(steps)

    class Hooks:
        def __init__(self, layer, counts, reused):
            self.layer, self.counts, self.reused = layer, counts_of(counts), reused

        def free(self, idx):
            if self.reused:
                program.ensure(idx)

        def __call__(self, name, chunk=None):
            if chunk is not None and (self.layer == 0 or chunk != (0, WIDE)):
                add(self.layer, *chunk)
            program.pump(next(self.counts))

    d_hidden1[...] = layer_backward(1, hidden1, y_cot, weights, small, tab, saved, grads, small_grads,
                                    Hooks(1, SCATTER_PUMPS[0], False))
    layer_forward(0, x, weights, small, tab, saved, Hooks(0, SCATTER_PUMPS[1], False))
    x_grad[...] = layer_backward(0, x, d_hidden1, weights, small, tab, saved, grads, small_grads,
                                 Hooks(0, SCATTER_PUMPS[2], True))
    small_gen = small_reduce_steps(copies, pos, small_grads, small_grad_bufs, small_out)
    program.finish(small_gen)
    for _ in small_gen:
        pass
    copies.finish()


def part_scratch(rows, width):
    return [pltpu.VMEM((LAYERS, 4, 2, 2, rows, width), jnp.float32),
            pltpu.VMEM((LAYERS, 4, 2, rows, width // 2), jnp.float32),
            pltpu.VMEM((LAYERS, 4, 2, rows, width // 2), jnp.float32),
            pltpu.VMEM((LAYERS, 4, rows, width), jnp.float32),
            pltpu.VMEM((LAYERS, 3, rows, width), jnp.float32)]


def step_call(x, y_cot, matrices, vectors, tab):
    tokens, d_model = x.shape
    rows, down_rows = matrices[1].shape[1], matrices[3].shape[1]
    vmem = pl.BlockSpec(memory_space=pltpu.VMEM)
    bf16, f32 = jnp.bfloat16, jnp.float32
    small = (LAYERS * SMALL, d_model)
    n_sems = 12 + 6 * 23 + 8 * 15
    return pl.pallas_call(
        step_kernel,
        out_shape=(jax.ShapeDtypeStruct(x.shape, bf16), jax.ShapeDtypeStruct(x.shape, bf16),
                   jax.ShapeDtypeStruct((LAYERS, rows, ACOLS), bf16),
                   jax.ShapeDtypeStruct((LAYERS, down_rows, d_model), bf16), jax.ShapeDtypeStruct(small, f32)),
        in_specs=[vmem] * (2 + 4 + 8 + 1), out_specs=(vmem,) * 5,
        scratch_shapes=[
            pltpu.VMEM((LAYERS, rows, ACOLS), bf16),
            pltpu.VMEM((LAYERS, 4, 2, 2, 2, rows, ACOLS), bf16),
            pltpu.VMEM((LAYERS, 4, 2, 2, 2, down_rows, d_model), bf16),
            pltpu.VMEM((4, 2, 2, 2, rows, ACOLS), f32),
            pltpu.VMEM((4, 2, 2, 2, down_rows, d_model), f32),
            *part_scratch(rows, ACOLS), *part_scratch(down_rows, d_model),
            pltpu.VMEM((LAYERS, 3, 2, 2, down_rows, d_model // 2), f32),
            pltpu.VMEM((LAYERS, 3, down_rows, d_model // 2), f32),
            pltpu.VMEM(small, f32),
            pltpu.VMEM(small, f32),
            pltpu.VMEM(small, f32),
            pltpu.VMEM((9,) + small, f32),
            pltpu.VMEM((9,) + small, f32),
            pltpu.VMEM((tokens, d_model), bf16),
            pltpu.VMEM((tokens, d_model), bf16),
            pltpu.VMEM((3, tokens, d_model), bf16),
            pltpu.VMEM((tokens // SEQ, 4, 2, SEQ, SEQ), f32),
            pltpu.VMEM((tokens, d_model), bf16),
            pltpu.VMEM((tokens, 4 * d_model), f32),
            pltpu.VMEM((tokens, 4 * d_model), bf16),
            pltpu.VMEM((tokens, 3 * d_model), bf16),
            pltpu.VMEM((tokens, d_model), bf16),
            pltpu.VMEM((tokens, d_model), bf16),
            pltpu.SemaphoreType.DMA((n_sems,)), pltpu.SemaphoreType.DMA((n_sems,))],
        compiler_params=pltpu.CompilerParams(collective_id=0, has_side_effects=True,
                                             vmem_limit_bytes=67043328),
    )(x, y_cot, *matrices, *vectors, tab)


def finish_kernel(y_in, x_grad_in, wide, down, small, y_out, x_grad, gain1, bias1, qkv_g, qkv_b, out_g, out_b,
                  gain2, bias2, up_g, up_b, down_g, down_b):
    y_out[...] = y_in[...]
    x_grad[...] = x_grad_in[...]
    qkv_g[...] = wide[:, :, :OUT]
    out_g[...] = wide[:, :, OUT:UP]
    up_g[...] = wide[:, :, UP:]
    down_g[...] = down[...]
    rank = lax.axis_index('node') * 8 + lax.axis_index('local')
    for ref, (row, count) in zip((gain1, bias1, qkv_b, out_b, gain2, bias2, up_b, down_b), VECTOR_ROWS):
        sums = []
        for layer in range(LAYERS):
            lines = [small[pl.ds(layer * SMALL + row + i, 1), :] for i in range(count)]
            sums.append(jnp.concatenate(lines, axis=1))
        sums = jnp.concatenate(sums, axis=0).astype(jnp.bfloat16)
        ref[...] = dot_bt(sums, places(rank, ref.shape[1], count * WIDE)).astype(jnp.bfloat16)


def finish_call(y, x_grad, wide, down, small, shapes):
    vmem = pl.BlockSpec(memory_space=pltpu.VMEM)
    return pl.pallas_call(
        finish_kernel, out_shape=tuple(jax.ShapeDtypeStruct(s, jnp.bfloat16) for s in shapes),
        in_specs=[vmem] * 5, out_specs=(vmem,) * len(shapes),
    )(y, x_grad, wide, down, small)


def rope_table(seq_len, rot_dim):
    inv_freq = 1.0 / (np.float32(10000.0) ** (np.arange(0, rot_dim, 2, dtype=np.float32) / np.float32(rot_dim)))
    angles = np.arange(seq_len, dtype=np.float32)[:, None] * inv_freq[None, :].astype(np.float32)
    cos, sin = np.cos(angles), np.sin(angles)
    none = np.zeros_like(sin)
    rest = np.zeros((seq_len, 3 * rot_dim), np.float32)
    parts = ([cos, cos, rest + 1.0], [-sin, none, rest], [none, sin, rest])
    return np.stack([np.tile(np.concatenate(p, axis=-1), (1, 2)) for p in parts]).astype(np.float32)


def solution(mesh):
    shard_axes = ('node', 'local')
    act_spec = P(shard_axes)
    param_spec = P(None, shard_axes)

    def device_step(x, y_cot, ln1_gain, ln1_bias, qkv_weight, qkv_bias, out_weight, out_bias,
                    ln2_gain, ln2_bias, up_weight, up_bias, down_weight, down_bias):
        d_model, rows = x.shape[2], out_weight.shape[1]
        flat = (x.shape[0] * x.shape[1], d_model)
        qkv_flat = (LAYERS, rows, 3 * d_model)
        matrices = (qkv_weight.reshape(qkv_flat), out_weight, up_weight, down_weight)
        vectors = (ln1_gain, ln1_bias, qkv_bias, out_bias, ln2_gain, ln2_bias, up_bias, down_bias)
        sums = step_call(x.reshape(flat), y_cot.reshape(flat), matrices, vectors, rope_table(x.shape[1], qkv_weight.shape[3] // 12))
        shapes = [flat, flat, ln1_gain.shape, ln1_bias.shape, qkv_flat, qkv_bias.shape, out_weight.shape, out_bias.shape,
                  ln2_gain.shape, ln2_bias.shape, up_weight.shape, up_bias.shape, down_weight.shape, down_bias.shape]
        outs = list(finish_call(*sums, shapes))
        outs[0], outs[1], outs[4] = outs[0].reshape(x.shape), outs[1].reshape(x.shape), outs[4].reshape(qkv_weight.shape)
        return tuple(outs)

    return jax.shard_map(device_step, mesh=mesh,
                         in_specs=(act_spec, act_spec) + (param_spec,) * 12,
                         out_specs=(act_spec, act_spec) + (param_spec,) * 12,
                         check_vma=False)
```

```python
import functools
import jax
import numpy as np
import jax.numpy as jnp
from jax import lax
from jax.experimental import pallas as pl
from jax.experimental.pallas import tpu as pltpu
from jax.sharding import PartitionSpec as P

EPSILON = 1e-5
MESH = pl.DeviceIdType.MESH
LAYERS = 2
ROWS = 16
SMALL = 16
WIDE = 512
PAIR = 128
SEQ = 128
OUT, UP, ACOLS = 3 * WIDE, 4 * WIDE, 8 * WIDE


def positions():
    z = lax.axis_index('node')
    l = lax.axis_index('local')
    c = l % 2
    x = (l // 2) % 2
    y = l // 4
    partner = (z, l + 1 - 2 * c)
    x_nbr = (z, l + 2 - 4 * x)
    y_nbr = (z, (l + 4) % 8)
    z_others = [z + 1 - 2 * (z % 2), (z + 2) % 4, 3 - z]
    return z, l, c, x, y, partner, x_nbr, y_nbr, z_others


def ring_of(z, l):
    return ((z + 1) % 4, l), [z, (z + 3) % 4, (z + 2) % 4, (z + 1) % 4]


def entry_barrier(pos):
    z, l, c, x, y, partner, x_nbr, y_nbr, z_others = pos
    barrier = pltpu.get_barrier_semaphore()
    for dev in [partner, x_nbr, y_nbr] + [(zo, l) for zo in z_others]:
        pl.semaphore_signal(barrier, inc=1, device_id=dev, device_id_type=MESH)
    pl.semaphore_wait(barrier, 6)


class Copies:
    def __init__(self, send_sems, recv_sems):
        self.send_sems, self.recv_sems, self.used = send_sems, recv_sems, 0
        self.open_sends = []

    def make(self, src, dst, dev):
        idx = self.used
        self.used += 1
        return pltpu.make_async_remote_copy(src_ref=src, dst_ref=dst, send_sem=self.send_sems.at[idx],
                                            recv_sem=self.recv_sems.at[idx], device_id=dev, device_id_type=MESH)

    def start(self, src, dst, dev):
        copy = self.make(src, dst, dev)
        copy.start()
        self.open_sends.append(copy)
        return copy

    def finish(self):
        for copy in self.open_sends:
            copy.wait_send()
        self.open_sends = []


def small_reduce_steps(copies, pos, src, bufs, out):
    z, l, c, x, y, partner, x_nbr, y_nbr, z_others = pos
    held = src
    for step, dev in enumerate((partner, x_nbr, y_nbr)):
        copy = copies.start(held, bufs.at[2 * step], dev)
        yield
        copy.wait_recv()
        bufs[2 * step + 1] = held[...] + bufs[2 * step]
        held = bufs.at[2 * step + 1]
    sends = [copies.start(held, bufs.at[6 + k], (zo, l)) for k, zo in enumerate(z_others)]
    yield
    for copy in sends:
        copy.wait_recv()
    out[...] = (held[...] + bufs[6]) + (bufs[7] + bufs[8])
    yield


def gather_steps(copies, pos, own, full, lo, width):
    z, l, c, x, y, partner, x_nbr, y_nbr, z_others = pos
    half = width // 2
    cols, cols_a, cols_b = pl.ds(lo, width), pl.ds(lo, half), pl.ds(lo + half, half)
    after, z_order = ring_of(z, l)

    def block(zz, yy, xx, cc):
        return full.at[zz, yy, xx, cc, :, cols]

    from_z, from_x, from_y, diag, to_partner = [None] * 4, [None] * 4, [None] * 4, [], []

    def spread(k, got, place):
        if k < 3:
            from_z[k + 1] = copies.start(got, place, after)
        from_x[k] = copies.start(got, place, x_nbr)
        from_y[k] = copies.start(got, place, y_nbr)

    def forward_z(k):
        from_z[k].wait_recv()
        got = block(z_order[k], y, x, c)
        spread(k, got, got)

    def forward_cross(k):
        zz = z_order[k]
        from_x[k].wait_recv()
        got = full.at[zz, y, 1 - x, c, :, cols_a]
        diag.append(copies.start(got, got, y_nbr))
        from_y[k].wait_recv()
        got = full.at[zz, 1 - y, x, c, :, cols_b]
        diag.append(copies.start(got, got, x_nbr))

    def forward_partner(yy, xx):
        got = full.at[:, yy, xx, c, :, cols]
        to_partner.append(copies.start(got, got, partner))

    spread(0, own.at[:, cols], block(z, y, x, c))
    full[z, y, x, c, :, cols] = own[:, cols]
    yield
    forward_z(1)
    yield
    forward_cross(0)
    yield
    forward_z(2)
    yield
    forward_cross(1)
    yield
    forward_z(3)
    forward_partner(y, x)
    yield
    forward_cross(2)
    yield
    forward_cross(3)
    forward_partner(y, 1 - x)
    forward_partner(1 - y, x)
    yield
    for copy in diag:
        copy.wait_recv()
    forward_partner(1 - y, 1 - x)
    yield
    for copy in to_partner:
        copy.wait_recv()
    yield


GATHER_ORDERS = ('azcbdaaccefbzbaaddccbbacbzddefefaadczcbbaefefzcbaddefcbdefde', 'fefef')
GATHER_PUMPS = ('15001211', '10205331')
SCATTER_ORDERS = ('abcabdcbeadcfbedgacbfehdcgfiedgjfebhikgfcjilhagdkjamielknhji', 'fmzlokjgmnlkzomlinzmjohkhlnmoz')
SCATTER_PUMPS = ('0200121000', '1401111220', '4320442144')
DIRECT = (0, WIDE)


SMALL_TURN = ord('z') - ord('a')


def turns(parts):
    return [ord(letter) - ord('a') for part in parts for letter in part]


def counts_of(digits):
    return iter([int(digit) for digit in digits])


def gather_program(pieces, small_gen, done):
    order = turns(GATHER_ORDERS)
    left = [order.count(i) for i in range(len(pieces))]
    for i in order:
        if i == SMALL_TURN:
            next(small_gen)
            continue
        next(pieces[i])
        left[i] -= 1
        if not left[i]:
            done.append(i)
        yield


def scatter_chunk_steps(copies, pos, grads, part0, partx, party, last, partz, out, lo, width, direct):
    z, l, c, x, y, partner, x_nbr, y_nbr, z_others = pos
    half = width // 2
    cols, cols_a, cols_b = pl.ds(lo, width), pl.ds(lo, half), pl.ds(lo + half, half)
    after, z_order = ring_of(z, l)
    hcols = pl.ds(lo // 2, half)
    swap = copies.make(grads.at[:, :, :, 1 - c, :, cols], part0.at[:, :, :, :, cols], partner)
    swap.start()
    yield
    swap.wait()
    part0[:, :, :, :, cols] = part0[:, :, :, :, cols] + grads[:, :, :, c, :, cols]
    send_a = copies.start(part0.at[:, :, 1 - x, :, cols_a], partx.at[:, :, :, hcols], x_nbr)
    send_b = copies.start(part0.at[:, 1 - y, :, :, cols_b], party.at[:, :, :, hcols], y_nbr)
    yield
    send_a.wait_recv()
    partx[:, :, :, hcols] = partx[:, :, :, hcols] + part0[:, :, x, :, cols_a]
    send_a = copies.start(partx.at[:, 1 - y, :, hcols], last.at[:, :, cols_a], y_nbr)
    send_b.wait_recv()
    party[:, :, :, hcols] = party[:, :, :, hcols] + part0[:, y, :, :, cols_b]
    send_b = copies.start(party.at[:, 1 - x, :, hcols], last.at[:, :, cols_b], x_nbr)
    yield
    send_a.wait_recv()
    send_b.wait_recv()
    last[:, :, cols_a] = last[:, :, cols_a] + partx[:, y, :, hcols]
    last[:, :, cols_b] = last[:, :, cols_b] + party[:, x, :, hcols]
    if direct:
        sends = [copies.start(last.at[zo, :, cols], partz.at[k, :, cols], (zo, l)) for k, zo in enumerate(z_others)]
        yield
        for copy in sends:
            copy.wait_recv()
        total = (last[z, :, cols] + partz[0, :, cols]) + (partz[1, :, cols] + partz[2, :, cols])
    else:
        send = copies.start(last.at[z_order[1], :, cols], partz.at[0, :, cols], after)
        yield
        for k in (1, 2):
            send.wait_recv()
            partz[k - 1, :, cols] = partz[k - 1, :, cols] + last[z_order[k + 1], :, cols]
            send = copies.start(partz.at[k - 1, :, cols], partz.at[k, :, cols], after)
            yield
        send.wait_recv()
        total = partz[2, :, cols] + last[z, :, cols]
    out[:, cols] = total.astype(out.dtype)
    yield


def scatter_z_first_steps(copies, pos, grads, part0, ring, plane, out, lo, width):
    z, l, c, x, y, partner, x_nbr, y_nbr, z_others = pos
    half = width // 2
    cols, cols_a, cols_b = pl.ds(lo, width), pl.ds(lo, half), pl.ds(lo + half, half)
    first_a, first_b = pl.ds(0, half), pl.ds(half, half)
    after, z_order = ring_of(z, l)
    swap = copies.make(grads.at[:, :, :, 1 - c, :, cols], part0.at[:, :, :, :, cols], partner)
    swap.start()
    yield
    swap.wait()
    part0[:, :, :, :, cols] = part0[:, :, :, :, cols] + grads[:, :, :, c, :, cols]
    send = copies.start(part0.at[z_order[1], :, :, :, cols], ring.at[0], after)
    yield
    for k in (1, 2):
        send.wait_recv()
        ring[k - 1] = ring[k - 1] + part0[z_order[k + 1], :, :, :, cols]
        send = copies.start(ring.at[k - 1], ring.at[k], after)
        yield
    send.wait_recv()
    ring[2] = ring[2] + part0[z, :, :, :, cols]
    send_a = copies.start(ring.at[2, :, 1 - x, :, first_a], plane.at[:2, :, first_a], x_nbr)
    send_b = copies.start(ring.at[2, 1 - y, :, :, first_b], plane.at[:2, :, first_b], y_nbr)
    yield
    send_a.wait_recv()
    plane[:2, :, first_a] = plane[:2, :, first_a] + ring[2, :, x, :, first_a]
    send_a = copies.start(plane.at[1 - y, :, first_a], plane.at[2, :, first_a], y_nbr)
    send_b.wait_recv()
    plane[:2, :, first_b] = plane[:2, :, first_b] + ring[2, y, :, :, first_b]
    send_b = copies.start(plane.at[1 - x, :, first_b], plane.at[2, :, first_b], x_nbr)
    yield
    send_a.wait_recv()
    send_b.wait_recv()
    out[:, cols_a] = (plane[y, :, first_a] + plane[2, :, first_a]).astype(out.dtype)
    out[:, cols_b] = (plane[x, :, first_b] + plane[2, :, first_b]).astype(out.dtype)
    yield


class ScatterProgram:
    def __init__(self):
        self.chunks, self.turn = {}, 0
        self.order = turns(SCATTER_ORDERS)

    def add(self, chunk, idx=None):
        next(chunk)
        self.chunks[len(self.chunks) if idx is None else idx] = chunk

    def pump(self, count):
        while count and self.turn < len(self.order) and self.order[self.turn] in self.chunks:
            next(self.chunks[self.order[self.turn]])
            self.turn += 1
            count -= 1

    def ensure(self, idx):
        while idx not in self.order[:self.turn]:
            assert self.order[self.turn] in self.chunks
            self.pump(1)


def dot(first, second):
    return lax.dot_general(first, second, (((1,), (0,)), ((), ())), preferred_element_type=jnp.float32)


def dot_bt(first, second):
    return lax.dot_general(first, second, (((1,), (1,)), ((), ())), preferred_element_type=jnp.float32)


def dot_at(first, second):
    return lax.dot_general(first, second, (((0,), (0,)), ((), ())), preferred_element_type=jnp.float32)


def normalised(hidden32):
    center = hidden32 - jnp.mean(hidden32, axis=-1, keepdims=True)
    rstd = lax.rsqrt(jnp.mean(center * center, axis=-1, keepdims=True) + EPSILON)
    return center * rstd, rstd


def weight(full, layer, lo, width=WIDE):
    return full[layer, :, :, :, :, :, lo:lo + width].reshape(WIDE, width)


def down_weight_part(full, layer, k):
    return full[layer, k].reshape(WIDE, WIDE)


def rotate(piece, tab):
    piece = piece.reshape(-1, SEQ, PAIR)
    up, down = pltpu.roll(piece, PAIR - 8, 2), pltpu.roll(piece, 8, 2)
    return (piece * tab[0] + up * tab[1] + down * tab[2]).reshape(-1, PAIR)


def rotate_back(piece, tab):
    piece = piece.reshape(-1, SEQ, PAIR)
    turned = (piece * tab[0] + pltpu.roll(piece * tab[1], 8, 2) + pltpu.roll(piece * tab[2], PAIR - 8, 2))
    return turned.reshape(-1, PAIR)


def low_half(rows):
    return lax.broadcasted_iota(jnp.int32, (rows, PAIR), 1) < PAIR // 2


def head_masks():
    first = low_half(SEQ)
    return (jnp.where(first, 1.0, 0.0).astype(jnp.bfloat16), jnp.where(first, 0.0, 1.0).astype(jnp.bfloat16))


def attention_blocks(tokens):
    for s in range(tokens // SEQ):
        for j in range(WIDE // PAIR):
            yield s, j, pl.ds(s * SEQ, SEQ), pl.ds(j * PAIR, PAIR)


def layer_forward(layer, hidden, weights, small, tab, saved, hooks):
    n1, n2, qkv, probs, ctx, slope, act, d_qkv = saved
    wide_w, down_w = weights
    tokens = hidden.shape[0]

    def vec(row):
        return small[pl.ds(layer * SMALL + row, 1), :]

    hidden32 = hidden[...].astype(jnp.float32)
    scaled, _ = normalised(hidden32)
    n1[...] = (scaled * vec(0) + vec(1)).astype(jnp.bfloat16)
    n2[...] = (scaled * vec(3) + vec(4)).astype(jnp.bfloat16)
    hooks('norm')
    low = low_half(tokens)
    qkv_bias = jnp.concatenate([vec(10), vec(11), vec(12)], axis=1)
    group = 6 * PAIR
    for i in range(2):
        part = dot(n1[...], weight(wide_w, layer, i * group, group)) + qkv_bias[:, i * group:(i + 1) * group]
        for jj in range(2):
            first, second, third = (part[:, (3 * jj + m) * PAIR:(3 * jj + m + 1) * PAIR] for m in range(3))
            cols = pl.ds((2 * i + jj) * PAIR, PAIR)
            query = jnp.where(low, first, second)
            key = jnp.where(low, pltpu.roll(first, PAIR // 2, 1), pltpu.roll(third, PAIR // 2, 1))
            qkv[0, :, cols] = rotate(query, tab).astype(jnp.bfloat16)
            qkv[1, :, cols] = rotate(key, tab).astype(jnp.bfloat16)
            qkv[2, :, cols] = jnp.where(low, second, third).astype(jnp.bfloat16)
    hooks('qkv')
    causal = (lax.broadcasted_iota(jnp.int32, (SEQ, SEQ), 0) >= lax.broadcasted_iota(jnp.int32, (SEQ, SEQ), 1))
    masks, low = head_masks(), low_half(SEQ)
    for s, j, rows, cols in attention_blocks(tokens):
        query, key, value = qkv[0, rows, cols], qkv[1, rows, cols], qkv[2, rows, cols]
        heads = []
        for h in range(2):
            scores = dot_bt(query * masks[h], key) * 0.125
            scores = jnp.where(causal, scores, -1e30)
            attn = jnp.exp(scores - jnp.max(scores, axis=-1, keepdims=True))
            attn = attn / jnp.sum(attn, axis=-1, keepdims=True)
            probs[s, j, h] = attn
            heads.append(dot(attn.astype(jnp.bfloat16), value))
        ctx[rows, cols] = jnp.where(low, heads[0], heads[1]).astype(jnp.bfloat16)
        if j == 3:
            hooks('attn')
    total = hidden32 + (dot(ctx[...], weight(wide_w, layer, OUT)) + vec(2))
    hooks('out')
    mlp = None
    for k in range(4):
        pre = dot(n2[...], weight(wide_w, layer, UP + k * WIDE)) + vec(6 + k)
        bell = lax.erf(pre * 0.7071067811865476) + 1.0
        act[:, k * WIDE:(k + 1) * WIDE] = (0.5 * pre * bell).astype(jnp.bfloat16)
        slope[:, k * WIDE:(k + 1) * WIDE] = 0.5 * bell + pre * (jnp.exp(-0.5 * pre * pre) * 0.3989422804014327)
        if k == 0:
            hooks('up')
        term = dot(act[:, k * WIDE:(k + 1) * WIDE], down_weight_part(down_w, layer, k))
        mlp = term if mlp is None else mlp + term
        hooks('mlp')
    return (total + (mlp + vec(5))).astype(jnp.bfloat16)


def layer_backward(layer, hidden, d_out, weights, small, tab, saved, grads, small_grads, hooks):
    n1, n2, qkv, probs, ctx, slope, act, d_qkv = saved
    wide_w, down_w = weights
    wide_g, down_g = grads
    tokens = hidden.shape[0]

    def vec(row):
        return small[pl.ds(layer * SMALL + row, 1), :]

    def put_small(row, value):
        small_grads[pl.ds(layer * SMALL + row, 1), :] = jnp.sum(value, axis=0, keepdims=True)

    def put(lo, value):
        wide_g[:, :, :, :, :, lo:lo + WIDE] = value.reshape(wide_g.shape[:5] + (WIDE,))

    d_out32 = d_out[...].astype(jnp.float32)
    put_small(2, d_out32)
    put_small(5, d_out32)
    half = WIDE // 2
    for k in range(2):
        hooks.free(k)
        value = dot_at(act[...], d_out[:, k * half:(k + 1) * half])
        down_g[:, :, :, :, :, k * half:(k + 1) * half] = value.reshape(down_g.shape[:5] + (half,))
        hooks('down', (1, k * half))
    d_n2 = None
    for k in range(4):
        if k % 2 == 0:
            hooks.free(2 + k // 2)
        d_act = dot_bt(d_out[...], down_weight_part(down_w, layer, k)).astype(jnp.bfloat16)
        d_pre = d_act.astype(jnp.float32) * slope[:, k * WIDE:(k + 1) * WIDE]
        put_small(6 + k, d_pre)
        act[:, k * WIDE:(k + 1) * WIDE] = d_pre.astype(jnp.bfloat16)
        d_pre_bf = act[:, k * WIDE:(k + 1) * WIDE]
        put(UP + k * WIDE, dot_at(n2[...], d_pre_bf))
        term = dot_bt(d_pre_bf, weight(wide_w, layer, UP + k * WIDE))
        d_n2 = term if d_n2 is None else d_n2 + term
        if k % 2:
            hooks('up', (0, UP + (k - 1) * WIDE))
    d_n2 = d_n2.astype(jnp.bfloat16)
    hooks.free(4)
    put(OUT, dot_at(ctx[...], d_out[...]))
    ctx[...] = dot_bt(d_out[...], weight(wide_w, layer, OUT)).astype(jnp.bfloat16)
    hooks('dctx', (0, OUT))
    masks, low = head_masks(), low_half(SEQ)
    for s, j, rows, cols in attention_blocks(tokens):
        query, key, value = qkv[0, rows, cols], qkv[1, rows, cols], qkv[2, rows, cols]
        d_ctx = ctx[rows, cols]
        d_q, d_k, d_v = [], [], []
        for h in range(2):
            attn = probs[s, j, h]
            d_probs = dot_bt(d_ctx * masks[h], value).astype(jnp.bfloat16).astype(jnp.float32)
            d_v.append(dot_at(attn.astype(jnp.bfloat16), d_ctx))
            inner = jnp.sum(d_probs * attn, axis=-1, keepdims=True)
            d_scores = (attn * (d_probs - inner) * 0.125).astype(jnp.bfloat16)
            d_q.append(dot(d_scores, key))
            d_k.append(dot_at(d_scores, query))
        qkv[0, rows, cols] = jnp.where(low, d_q[0], d_q[1]).astype(jnp.bfloat16)
        qkv[1, rows, cols] = jnp.where(low, d_k[0], d_k[1]).astype(jnp.bfloat16)
        qkv[2, rows, cols] = jnp.where(low, d_v[0], d_v[1]).astype(jnp.bfloat16)
        if j == 3:
            hooks('dattn')
    low = low_half(tokens)
    for j in range(WIDE // PAIR):
        cols = pl.ds(j * PAIR, PAIR)
        d_query, d_key, d_value = (qkv[t, :, cols].astype(jnp.float32) for t in range(3))
        d_query = rotate_back(d_query, tab)
        d_key = pltpu.roll(rotate_back(d_key, tab), PAIR // 2, 1)
        parts = (jnp.where(low, d_query, d_key), jnp.where(low, d_value, d_query), jnp.where(low, d_key, d_value))
        for m, part in enumerate(parts):
            lo = (3 * j + m) * PAIR
            row = layer * SMALL + 10 + lo // WIDE
            small_grads[pl.ds(row, 1), pl.ds(lo % WIDE, PAIR)] = jnp.sum(part, axis=0, keepdims=True)
            d_qkv[:, lo:lo + PAIR] = part.astype(jnp.bfloat16)
    d_n1 = None
    for t in (2, 1, 0):
        if t:
            hooks.free(7 - t)
        piece = d_qkv[:, t * WIDE:(t + 1) * WIDE]
        put(t * WIDE, dot_at(n1[...], piece))
        term = dot_bt(piece, weight(wide_w, layer, t * WIDE))
        d_n1 = term if d_n1 is None else d_n1 + term
        hooks('dqkv', (0, t * WIDE))
    d_n1 = d_n1.astype(jnp.bfloat16).astype(jnp.float32)
    d_n2 = d_n2.astype(jnp.float32)
    scaled, rstd = normalised(hidden[...].astype(jnp.float32))
    put_small(0, d_n1 * scaled)
    put_small(1, d_n1)
    put_small(3, d_n2 * scaled)
    put_small(4, d_n2)
    d_scaled = d_n1 * vec(0) + d_n2 * vec(3)
    d_hidden = rstd * (d_scaled - jnp.mean(d_scaled, axis=-1, keepdims=True)
                       - scaled * jnp.mean(d_scaled * scaled, axis=-1, keepdims=True))
    return (d_out32 + d_hidden).astype(jnp.bfloat16)


def places(rank, part, width):
    shift = lax.broadcasted_iota(jnp.int32, (part, width), 1) - lax.broadcasted_iota(jnp.int32, (part, width), 0)
    return jnp.where(shift == rank * part, 1.0, 0.0).astype(jnp.bfloat16)


VECTOR_ROWS = ((0, 1), (1, 1), (10, 3), (2, 1), (3, 1), (4, 1), (6, 4), (5, 1))


def place_small(rank, vectors, small_own):
    small_own[...] = jnp.zeros_like(small_own)
    for ref, (row, count) in zip(vectors, VECTOR_ROWS):
        wide = dot(ref[...], places(rank, ref.shape[1], count * WIDE))
        for layer in range(LAYERS):
            for i in range(count):
                small_own[pl.ds(layer * SMALL + row + i, 1), :] = wide[layer:layer + 1, i * WIDE:(i + 1) * WIDE]


def step_kernel(x, y_cot, qkv_own, out_own, up_own, down_own, *refs):
    (gain1, bias1, qkv_b, out_b, gain2, bias2, up_b, down_b, tab,
     y_out, x_grad, wide_out, down_out, small_out,
     wide_own, wide_w, down_w, wide_g, down_g) = refs[:19]
    wide_parts, down_parts = refs[19:24], refs[24:29]
    ring, plane = refs[29:31]
    (small_own, small, small_grads, small_bufs, small_grad_bufs,
     n1, n2, qkv, probs, ctx, slope, act, d_qkv, hidden1, d_hidden1, send_sems, recv_sems) = refs[31:]
    saved = (n1, n2, qkv, probs, ctx, slope, act, d_qkv)
    weights, grads = (wide_w, down_w), (wide_g, down_g)
    pos = positions()
    rank = pos[0] * 8 + pos[1]
    wide_own[:, :, :OUT] = qkv_own[...]
    wide_own[:, :, OUT:UP] = out_own[...]
    wide_own[:, :, UP:] = up_own[...]
    place_small(rank, (gain1, bias1, qkv_b, out_b, gain2, bias2, up_b, down_b), small_own)
    small_grads[...] = jnp.zeros_like(small_grads)
    entry_barrier(pos)
    copies = Copies(send_sems, recv_sems)

    small_gen = small_reduce_steps(copies, pos, small_own, small_bufs, small)
    done = []
    pieces = []
    for i in range(LAYERS):
        pieces.append(gather_steps(copies, pos, wide_own.at[i], wide_w.at[i], 0, UP))
        pieces.append(gather_steps(copies, pos, wide_own.at[i], wide_w.at[i], UP, UP))
        pieces.append(gather_steps(copies, pos, down_own.at[i], down_w.at[i], 0, WIDE))
    gather = gather_program(pieces, small_gen, done)

    def gather_until(piece):
        while piece not in done:
            next(gather)

    def gather_pump(count):
        for _ in range(count):
            next(gather, None)

    gather_until(0)

    def forward_hooks(layer):
        counts = counts_of(GATHER_PUMPS[layer])

        def hooks(name):
            if name == 'out':
                gather_until(3 * layer + 1)
            elif name == 'up':
                gather_until(3 * layer + 2)
            else:
                gather_pump(next(counts))
        return hooks

    hidden1[...] = layer_forward(0, x, weights, small, tab, saved, forward_hooks(0))
    gather_until(3)
    y_out[...] = layer_forward(1, hidden1, weights, small, tab, saved, forward_hooks(1))
    gather_until(5)

    program = ScatterProgram()

    def add(layer, kind, lo):
        if kind and lo == 0:
            steps = scatter_z_first_steps(copies, pos, down_g, down_parts[0].at[layer], ring.at[layer], plane.at[layer],
                                          down_out.at[layer], lo, WIDE // 2)
        else:
            width = WIDE // 2 if kind else WIDE if OUT <= lo < UP or (layer == 0 or lo) and lo < OUT else 2 * WIDE
            parts = (wide_parts, down_parts)[kind]
            steps = scatter_chunk_steps(copies, pos, grads[kind], *(ref.at[layer] for ref in parts),
                                        (wide_out, down_out)[kind].at[layer], lo, width, layer == 0 and lo in DIRECT)
        program.add(steps)

    class Hooks:
        def __init__(self, layer, counts, reused):
            self.layer, self.counts, self.reused = layer, counts_of(counts), reused

        def free(self, idx):
            if self.reused:
                program.ensure(idx)

        def __call__(self, name, chunk=None):
            if chunk is not None and (self.layer == 0 or chunk != (0, WIDE)):
                add(self.layer, *chunk)
            program.pump(next(self.counts))

    d_hidden1[...] = layer_backward(1, hidden1, y_cot, weights, small, tab, saved, grads, small_grads,
                                    Hooks(1, SCATTER_PUMPS[0], False))
    layer_forward(0, x, weights, small, tab, saved, Hooks(0, SCATTER_PUMPS[1], False))
    x_grad[...] = layer_backward(0, x, d_hidden1, weights, small, tab, saved, grads, small_grads,
                                 Hooks(0, SCATTER_PUMPS[2], True))
    program.add(small_reduce_steps(copies, pos, small_grads, small_grad_bufs, small_out), SMALL_TURN)
    program.pump(len(program.order))
    copies.finish()


def part_scratch(rows, width):
    return [pltpu.VMEM((LAYERS, 4, 2, 2, rows, width), jnp.float32),
            pltpu.VMEM((LAYERS, 4, 2, rows, width // 2), jnp.float32),
            pltpu.VMEM((LAYERS, 4, 2, rows, width // 2), jnp.float32),
            pltpu.VMEM((LAYERS, 4, rows, width), jnp.float32),
            pltpu.VMEM((LAYERS, 3, rows, width), jnp.float32)]


def step_call(x, y_cot, matrices, vectors, tab):
    tokens, d_model = x.shape
    rows, down_rows = matrices[1].shape[1], matrices[3].shape[1]
    vmem = pl.BlockSpec(memory_space=pltpu.VMEM)
    bf16, f32 = jnp.bfloat16, jnp.float32
    small = (LAYERS * SMALL, d_model)
    n_sems = 12 + 6 * 23 + 8 * 15
    return pl.pallas_call(
        step_kernel,
        out_shape=(jax.ShapeDtypeStruct(x.shape, bf16), jax.ShapeDtypeStruct(x.shape, bf16),
                   jax.ShapeDtypeStruct((LAYERS, rows, ACOLS), bf16),
                   jax.ShapeDtypeStruct((LAYERS, down_rows, d_model), bf16), jax.ShapeDtypeStruct(small, f32)),
        in_specs=[vmem] * (2 + 4 + 8 + 1), out_specs=(vmem,) * 5,
        scratch_shapes=[
            pltpu.VMEM((LAYERS, rows, ACOLS), bf16),
            pltpu.VMEM((LAYERS, 4, 2, 2, 2, rows, ACOLS), bf16),
            pltpu.VMEM((LAYERS, 4, 2, 2, 2, down_rows, d_model), bf16),
            pltpu.VMEM((4, 2, 2, 2, rows, ACOLS), f32),
            pltpu.VMEM((4, 2, 2, 2, down_rows, d_model), f32),
            *part_scratch(rows, ACOLS), *part_scratch(down_rows, d_model),
            pltpu.VMEM((LAYERS, 3, 2, 2, down_rows, d_model // 2), f32),
            pltpu.VMEM((LAYERS, 3, down_rows, d_model // 2), f32),
            pltpu.VMEM(small, f32),
            pltpu.VMEM(small, f32),
            pltpu.VMEM(small, f32),
            pltpu.VMEM((9,) + small, f32),
            pltpu.VMEM((9,) + small, f32),
            pltpu.VMEM((tokens, d_model), bf16),
            pltpu.VMEM((tokens, d_model), bf16),
            pltpu.VMEM((3, tokens, d_model), bf16),
            pltpu.VMEM((tokens // SEQ, 4, 2, SEQ, SEQ), f32),
            pltpu.VMEM((tokens, d_model), bf16),
            pltpu.VMEM((tokens, 4 * d_model), f32),
            pltpu.VMEM((tokens, 4 * d_model), bf16),
            pltpu.VMEM((tokens, 3 * d_model), bf16),
            pltpu.VMEM((tokens, d_model), bf16),
            pltpu.VMEM((tokens, d_model), bf16),
            pltpu.SemaphoreType.DMA((n_sems,)), pltpu.SemaphoreType.DMA((n_sems,))],
        compiler_params=pltpu.CompilerParams(collective_id=0, has_side_effects=True,
                                             vmem_limit_bytes=67043328),
    )(x, y_cot, *matrices, *vectors, tab)


def finish_kernel(y_in, x_grad_in, wide, down, small, y_out, x_grad, gain1, bias1, qkv_g, qkv_b, out_g, out_b,
                  gain2, bias2, up_g, up_b, down_g, down_b):
    y_out[...] = y_in[...]
    x_grad[...] = x_grad_in[...]
    qkv_g[...] = wide[:, :, :OUT]
    out_g[...] = wide[:, :, OUT:UP]
    up_g[...] = wide[:, :, UP:]
    down_g[...] = down[...]
    rank = lax.axis_index('node') * 8 + lax.axis_index('local')
    for ref, (row, count) in zip((gain1, bias1, qkv_b, out_b, gain2, bias2, up_b, down_b), VECTOR_ROWS):
        sums = []
        for layer in range(LAYERS):
            lines = [small[pl.ds(layer * SMALL + row + i, 1), :] for i in range(count)]
            sums.append(jnp.concatenate(lines, axis=1))
        sums = jnp.concatenate(sums, axis=0).astype(jnp.bfloat16)
        ref[...] = dot_bt(sums, places(rank, ref.shape[1], count * WIDE)).astype(jnp.bfloat16)


def finish_call(y, x_grad, wide, down, small, shapes):
    vmem = pl.BlockSpec(memory_space=pltpu.VMEM)
    return pl.pallas_call(
        finish_kernel, out_shape=tuple(jax.ShapeDtypeStruct(s, jnp.bfloat16) for s in shapes),
        in_specs=[vmem] * 5, out_specs=(vmem,) * len(shapes),
    )(y, x_grad, wide, down, small)


def rope_table(seq_len, rot_dim):
    inv_freq = 1.0 / (np.float32(10000.0) ** (np.arange(0, rot_dim, 2, dtype=np.float32) / np.float32(rot_dim)))
    angles = np.arange(seq_len, dtype=np.float32)[:, None] * inv_freq[None, :].astype(np.float32)
    cos, sin = np.cos(angles), np.sin(angles)
    none = np.zeros_like(sin)
    rest = np.zeros((seq_len, 3 * rot_dim), np.float32)
    parts = ([cos, cos, rest + 1.0], [-sin, none, rest], [none, sin, rest])
    return np.stack([np.tile(np.concatenate(p, axis=-1), (1, 2)) for p in parts]).astype(np.float32)


def solution(mesh):
    shard_axes = ('node', 'local')
    act_spec = P(shard_axes)
    param_spec = P(None, shard_axes)

    def device_step(x, y_cot, ln1_gain, ln1_bias, qkv_weight, qkv_bias, out_weight, out_bias,
                    ln2_gain, ln2_bias, up_weight, up_bias, down_weight, down_bias):
        d_model, rows = x.shape[2], out_weight.shape[1]
        flat = (x.shape[0] * x.shape[1], d_model)
        qkv_flat = (LAYERS, rows, 3 * d_model)
        matrices = (qkv_weight.reshape(qkv_flat), out_weight, up_weight, down_weight)
        vectors = (ln1_gain, ln1_bias, qkv_bias, out_bias, ln2_gain, ln2_bias, up_bias, down_bias)
        sums = step_call(x.reshape(flat), y_cot.reshape(flat), matrices, vectors, rope_table(x.shape[1], qkv_weight.shape[3] // 12))
        shapes = [flat, flat, ln1_gain.shape, ln1_bias.shape, qkv_flat, qkv_bias.shape, out_weight.shape, out_bias.shape,
                  ln2_gain.shape, ln2_bias.shape, up_weight.shape, up_bias.shape, down_weight.shape, down_bias.shape]
        outs = list(finish_call(*sums, shapes))
        outs[0], outs[1], outs[4] = outs[0].reshape(x.shape), outs[1].reshape(x.shape), outs[4].reshape(qkv_weight.shape)
        return tuple(outs)

    return jax.shard_map(device_step, mesh=mesh,
                         in_specs=(act_spec, act_spec) + (param_spec,) * 12,
                         out_specs=(act_spec, act_spec) + (param_spec,) * 12,
                         check_vma=False)
```

```python
import functools
import jax
import numpy as np
import jax.numpy as jnp
from jax import lax
from jax.experimental import pallas as pl
from jax.experimental.pallas import tpu as pltpu
from jax.sharding import PartitionSpec as P

EPSILON = 1e-5
MESH = pl.DeviceIdType.MESH
LAYERS = 2
ROWS = 16
SMALL = 16
WIDE = 512
PAIR = 128
SEQ = 128
OUT, UP, ACOLS = 3 * WIDE, 4 * WIDE, 8 * WIDE


def positions():
    z = lax.axis_index('node')
    l = lax.axis_index('local')
    c = l % 2
    x = (l // 2) % 2
    y = l // 4
    partner = (z, l + 1 - 2 * c)
    x_nbr = (z, l + 2 - 4 * x)
    y_nbr = (z, (l + 4) % 8)
    z_others = [z + 1 - 2 * (z % 2), (z + 2) % 4, 3 - z]
    return z, l, c, x, y, partner, x_nbr, y_nbr, z_others


def ring_of(z, l):
    return ((z + 1) % 4, l), [z, (z + 3) % 4, (z + 2) % 4, (z + 1) % 4]


def entry_barrier(pos):
    z, l, c, x, y, partner, x_nbr, y_nbr, z_others = pos
    barrier = pltpu.get_barrier_semaphore()
    for dev in [partner, x_nbr, y_nbr] + [(zo, l) for zo in z_others]:
        pl.semaphore_signal(barrier, inc=1, device_id=dev, device_id_type=MESH)
    pl.semaphore_wait(barrier, 6)


class Copies:
    def __init__(self, send_sems, recv_sems):
        self.send_sems, self.recv_sems, self.used = send_sems, recv_sems, 0
        self.open_sends = []

    def make(self, src, dst, dev):
        idx = self.used
        self.used += 1
        return pltpu.make_async_remote_copy(src_ref=src, dst_ref=dst, send_sem=self.send_sems.at[idx],
                                            recv_sem=self.recv_sems.at[idx], device_id=dev, device_id_type=MESH)

    def start(self, src, dst, dev):
        copy = self.make(src, dst, dev)
        copy.start()
        self.open_sends.append(copy)
        return copy

    def finish(self):
        for copy in self.open_sends:
            copy.wait_send()
        self.open_sends = []


def small_reduce_steps(copies, pos, src, bufs, out):
    z, l, c, x, y, partner, x_nbr, y_nbr, z_others = pos
    held = src
    for step, dev in enumerate((partner, x_nbr, y_nbr)):
        copy = copies.start(held, bufs.at[2 * step], dev)
        yield
        copy.wait_recv()
        bufs[2 * step + 1] = held[...] + bufs[2 * step]
        held = bufs.at[2 * step + 1]
    sends = [copies.start(held, bufs.at[6 + k], (zo, l)) for k, zo in enumerate(z_others)]
    yield
    for copy in sends:
        copy.wait_recv()
    out[...] = (held[...] + bufs[6]) + (bufs[7] + bufs[8])
    yield


def gather_steps(copies, pos, own, full, lo, width):
    z, l, c, x, y, partner, x_nbr, y_nbr, z_others = pos
    half = width // 2
    cols, cols_a, cols_b = pl.ds(lo, width), pl.ds(lo, half), pl.ds(lo + half, half)
    after, z_order = ring_of(z, l)

    def block(zz, yy, xx, cc):
        return full.at[zz, yy, xx, cc, :, cols]

    from_z, from_x, from_y, diag, to_partner = [None] * 4, [None] * 4, [None] * 4, [], []

    def spread(k, got, place):
        if k < 3:
            from_z[k + 1] = copies.start(got, place, after)
        from_x[k] = copies.start(got, place, x_nbr)
        from_y[k] = copies.start(got, place, y_nbr)

    def forward_z(k):
        from_z[k].wait_recv()
        got = block(z_order[k], y, x, c)
        spread(k, got, got)

    def forward_cross(k):
        zz = z_order[k]
        from_x[k].wait_recv()
        got = full.at[zz, y, 1 - x, c, :, cols_a]
        diag.append(copies.start(got, got, y_nbr))
        from_y[k].wait_recv()
        got = full.at[zz, 1 - y, x, c, :, cols_b]
        diag.append(copies.start(got, got, x_nbr))

    def forward_partner(yy, xx):
        got = full.at[:, yy, xx, c, :, cols]
        to_partner.append(copies.start(got, got, partner))

    spread(0, own.at[:, cols], block(z, y, x, c))
    full[z, y, x, c, :, cols] = own[:, cols]
    yield
    forward_z(1)
    yield
    forward_cross(0)
    yield
    forward_z(2)
    yield
    forward_cross(1)
    yield
    forward_z(3)
    forward_partner(y, x)
    yield
    forward_cross(2)
    yield
    forward_cross(3)
    forward_partner(y, 1 - x)
    forward_partner(1 - y, x)
    yield
    for copy in diag:
        copy.wait_recv()
    forward_partner(1 - y, 1 - x)
    yield
    for copy in to_partner:
        copy.wait_recv()
    yield


GATHER_ORDERS = ('zacbdezafcbzaacdbcbazaccdbbdaaeccabbzddefaecbddcbeeffddeeffe', 'ffeff')
GATHER_PUMPS = ('11330204', '11113410')
SCATTER_ORDERS = ('abcabdcbeadcfbedgacbfehdcgfiedgjfehibkgfjiaclhgakjdmilkenhji', 'mlzfokjmgnlkzomlzinmhjohklnmoz')
SCATTER_PUMPS = ('0200121000', '1401111220', '4320440343')
DIRECT = (0, WIDE)


SMALL_TURN = ord('z') - ord('a')


def turns(parts):
    return [ord(letter) - ord('a') for part in parts for letter in part]


def counts_of(digits):
    return iter([int(digit) for digit in digits])


def gather_program(pieces, small_gen, done):
    order = turns(GATHER_ORDERS)
    left = [order.count(i) for i in range(len(pieces))]
    for i in order:
        if i == SMALL_TURN:
            next(small_gen)
            continue
        next(pieces[i])
        left[i] -= 1
        if not left[i]:
            done.append(i)
        yield


def scatter_chunk_steps(copies, pos, grads, part0, partx, party, last, partz, out, lo, width, direct):
    z, l, c, x, y, partner, x_nbr, y_nbr, z_others = pos
    half = width // 2
    cols, cols_a, cols_b = pl.ds(lo, width), pl.ds(lo, half), pl.ds(lo + half, half)
    after, z_order = ring_of(z, l)
    hcols = pl.ds(lo // 2, half)
    swap = copies.make(grads.at[:, :, :, 1 - c, :, cols], part0.at[:, :, :, :, cols], partner)
    swap.start()
    yield
    swap.wait()
    part0[:, :, :, :, cols] = part0[:, :, :, :, cols] + grads[:, :, :, c, :, cols]
    send_a = copies.start(part0.at[:, :, 1 - x, :, cols_a], partx.at[:, :, :, hcols], x_nbr)
    send_b = copies.start(part0.at[:, 1 - y, :, :, cols_b], party.at[:, :, :, hcols], y_nbr)
    yield
    send_a.wait_recv()
    partx[:, :, :, hcols] = partx[:, :, :, hcols] + part0[:, :, x, :, cols_a]
    send_a = copies.start(partx.at[:, 1 - y, :, hcols], last.at[:, :, cols_a], y_nbr)
    send_b.wait_recv()
    party[:, :, :, hcols] = party[:, :, :, hcols] + part0[:, y, :, :, cols_b]
    send_b = copies.start(party.at[:, 1 - x, :, hcols], last.at[:, :, cols_b], x_nbr)
    yield
    send_a.wait_recv()
    send_b.wait_recv()
    last[:, :, cols_a] = last[:, :, cols_a] + partx[:, y, :, hcols]
    last[:, :, cols_b] = last[:, :, cols_b] + party[:, x, :, hcols]
    if direct:
        sends = [copies.start(last.at[zo, :, cols], partz.at[k, :, cols], (zo, l)) for k, zo in enumerate(z_others)]
        yield
        for copy in sends:
            copy.wait_recv()
        total = (last[z, :, cols] + partz[0, :, cols]) + (partz[1, :, cols] + partz[2, :, cols])
    else:
        send = copies.start(last.at[z_order[1], :, cols], partz.at[0, :, cols], after)
        yield
        for k in (1, 2):
            send.wait_recv()
            partz[k - 1, :, cols] = partz[k - 1, :, cols] + last[z_order[k + 1], :, cols]
            send = copies.start(partz.at[k - 1, :, cols], partz.at[k, :, cols], after)
            yield
        send.wait_recv()
        total = partz[2, :, cols] + last[z, :, cols]
    out[:, cols] = total.astype(out.dtype)
    yield


def scatter_z_first_steps(copies, pos, grads, part0, ring, plane, out, lo, width):
    z, l, c, x, y, partner, x_nbr, y_nbr, z_others = pos
    half = width // 2
    cols, cols_a, cols_b = pl.ds(lo, width), pl.ds(lo, half), pl.ds(lo + half, half)
    first_a, first_b = pl.ds(0, half), pl.ds(half, half)
    after, z_order = ring_of(z, l)
    swap = copies.make(grads.at[:, :, :, 1 - c, :, cols], part0.at[:, :, :, :, cols], partner)
    swap.start()
    yield
    swap.wait()
    part0[:, :, :, :, cols] = part0[:, :, :, :, cols] + grads[:, :, :, c, :, cols]
    send = copies.start(part0.at[z_order[1], :, :, :, cols], ring.at[0], after)
    yield
    for k in (1, 2):
        send.wait_recv()
        ring[k - 1] = ring[k - 1] + part0[z_order[k + 1], :, :, :, cols]
        send = copies.start(ring.at[k - 1], ring.at[k], after)
        yield
    send.wait_recv()
    ring[2] = ring[2] + part0[z, :, :, :, cols]
    send_a = copies.start(ring.at[2, :, 1 - x, :, first_a], plane.at[:2, :, first_a], x_nbr)
    send_b = copies.start(ring.at[2, 1 - y, :, :, first_b], plane.at[:2, :, first_b], y_nbr)
    yield
    send_a.wait_recv()
    plane[:2, :, first_a] = plane[:2, :, first_a] + ring[2, :, x, :, first_a]
    send_a = copies.start(plane.at[1 - y, :, first_a], plane.at[2, :, first_a], y_nbr)
    send_b.wait_recv()
    plane[:2, :, first_b] = plane[:2, :, first_b] + ring[2, y, :, :, first_b]
    send_b = copies.start(plane.at[1 - x, :, first_b], plane.at[2, :, first_b], x_nbr)
    yield
    send_a.wait_recv()
    send_b.wait_recv()
    out[:, cols_a] = (plane[y, :, first_a] + plane[2, :, first_a]).astype(out.dtype)
    out[:, cols_b] = (plane[x, :, first_b] + plane[2, :, first_b]).astype(out.dtype)
    yield


class ScatterProgram:
    def __init__(self):
        self.chunks, self.turn = {}, 0
        self.order = turns(SCATTER_ORDERS)

    def add(self, chunk, idx=None):
        next(chunk)
        self.chunks[len(self.chunks) if idx is None else idx] = chunk

    def pump(self, count):
        while count and self.turn < len(self.order) and self.order[self.turn] in self.chunks:
            next(self.chunks[self.order[self.turn]])
            self.turn += 1
            count -= 1

    def ensure(self, idx):
        while idx not in self.order[:self.turn]:
            assert self.order[self.turn] in self.chunks
            self.pump(1)


def dot(first, second):
    return lax.dot_general(first, second, (((1,), (0,)), ((), ())), preferred_element_type=jnp.float32)


def dot_bt(first, second):
    return lax.dot_general(first, second, (((1,), (1,)), ((), ())), preferred_element_type=jnp.float32)


def dot_at(first, second):
    return lax.dot_general(first, second, (((0,), (0,)), ((), ())), preferred_element_type=jnp.float32)


def normalised(hidden32):
    center = hidden32 - jnp.mean(hidden32, axis=-1, keepdims=True)
    rstd = lax.rsqrt(jnp.mean(center * center, axis=-1, keepdims=True) + EPSILON)
    return center * rstd, rstd


def weight(full, layer, lo, width=WIDE):
    return full[layer, :, :, :, :, :, lo:lo + width].reshape(WIDE, width)


def down_weight_part(full, layer, k):
    return full[layer, k].reshape(WIDE, WIDE)


def rotate(piece, tab):
    piece = piece.reshape(-1, SEQ, PAIR)
    up, down = pltpu.roll(piece, PAIR - 8, 2), pltpu.roll(piece, 8, 2)
    return (piece * tab[0] + up * tab[1] + down * tab[2]).reshape(-1, PAIR)


def rotate_back(piece, tab):
    piece = piece.reshape(-1, SEQ, PAIR)
    turned = (piece * tab[0] + pltpu.roll(piece * tab[1], 8, 2) + pltpu.roll(piece * tab[2], PAIR - 8, 2))
    return turned.reshape(-1, PAIR)


def low_half(rows):
    return lax.broadcasted_iota(jnp.int32, (rows, PAIR), 1) < PAIR // 2


def head_masks():
    first = low_half(SEQ)
    return (jnp.where(first, 1.0, 0.0).astype(jnp.bfloat16), jnp.where(first, 0.0, 1.0).astype(jnp.bfloat16))


def pair_block(s, j):
    return pl.ds(s * SEQ, SEQ), pl.ds(pl.multiple_of(j * PAIR, PAIR), PAIR)


def layer_forward(layer, hidden, weights, small, tab, saved, hooks):
    n1, n2, qkv, probs, ctx, slope, act, d_qkv = saved
    wide_w, down_w = weights
    tokens = hidden.shape[0]

    def vec(row):
        return small[pl.ds(layer * SMALL + row, 1), :]

    hidden32 = hidden[...].astype(jnp.float32)
    scaled, _ = normalised(hidden32)
    n1[...] = (scaled * vec(0) + vec(1)).astype(jnp.bfloat16)
    n2[...] = (scaled * vec(3) + vec(4)).astype(jnp.bfloat16)
    hooks('norm')
    low = low_half(tokens)
    qkv_bias = jnp.concatenate([vec(10), vec(11), vec(12)], axis=1)
    group = 6 * PAIR
    for i in range(2):
        part = dot(n1[...], weight(wide_w, layer, i * group, group)) + qkv_bias[:, i * group:(i + 1) * group]
        for jj in range(2):
            first, second, third = (part[:, (3 * jj + m) * PAIR:(3 * jj + m + 1) * PAIR] for m in range(3))
            cols = pl.ds((2 * i + jj) * PAIR, PAIR)
            query = jnp.where(low, first, second)
            key = jnp.where(low, pltpu.roll(first, PAIR // 2, 1), pltpu.roll(third, PAIR // 2, 1))
            qkv[0, :, cols] = rotate(query, tab).astype(jnp.bfloat16)
            qkv[1, :, cols] = rotate(key, tab).astype(jnp.bfloat16)
            qkv[2, :, cols] = jnp.where(low, second, third).astype(jnp.bfloat16)
    hooks('qkv')
    causal = (lax.broadcasted_iota(jnp.int32, (SEQ, SEQ), 0) >= lax.broadcasted_iota(jnp.int32, (SEQ, SEQ), 1))
    masks, low = head_masks(), low_half(SEQ)
    for s in range(tokens // SEQ):
        @pl.loop(0, WIDE // PAIR)
        def attend(j, s=s):
            rows, cols = pair_block(s, j)
            query, key, value = qkv[0, rows, cols], qkv[1, rows, cols], qkv[2, rows, cols]
            heads = []
            for h in range(2):
                scores = dot_bt(query * masks[h], key) * 0.125
                scores = jnp.where(causal, scores, -1e30)
                attn = jnp.exp(scores - jnp.max(scores, axis=-1, keepdims=True))
                attn = attn / jnp.sum(attn, axis=-1, keepdims=True)
                probs[s, j, h] = attn
                heads.append(dot(attn.astype(jnp.bfloat16), value))
            ctx[rows, cols] = jnp.where(low, heads[0], heads[1]).astype(jnp.bfloat16)
        hooks('attn')
    total = hidden32 + (dot(ctx[...], weight(wide_w, layer, OUT)) + vec(2))
    hooks('out')
    for k in range(4):
        pre = dot(n2[...], weight(wide_w, layer, UP + k * WIDE)) + vec(6 + k)
        bell = lax.erf(pre * 0.7071067811865476) + 1.0
        act[:, k * WIDE:(k + 1) * WIDE] = (0.5 * pre * bell).astype(jnp.bfloat16)
        slope[:, k * WIDE:(k + 1) * WIDE] = 0.5 * bell + pre * (jnp.exp(-0.5 * pre * pre) * 0.3989422804014327)
    hooks('up')
    mlp = None
    for k in range(4):
        term = dot(act[:, k * WIDE:(k + 1) * WIDE], down_weight_part(down_w, layer, k))
        mlp = term if mlp is None else mlp + term
        hooks('mlp')
    return (total + (mlp + vec(5))).astype(jnp.bfloat16)


def down_gradients(d_out, act, down_g, hooks):
    half = WIDE // 2
    for k in range(2):
        hooks.free(k)
        value = dot_at(act[...], d_out[:, k * half:(k + 1) * half])
        down_g[:, :, :, :, :, k * half:(k + 1) * half] = value.reshape(down_g.shape[:5] + (half,))
        hooks('down', (1, k * half))


def layer_backward(layer, hidden, d_out, weights, small, tab, saved, grads, small_grads, hooks):
    n1, n2, qkv, probs, ctx, slope, act, d_qkv = saved
    wide_w, down_w = weights
    wide_g, down_g = grads
    tokens = hidden.shape[0]

    def vec(row):
        return small[pl.ds(layer * SMALL + row, 1), :]

    def put_small(row, value):
        small_grads[pl.ds(layer * SMALL + row, 1), :] = jnp.sum(value, axis=0, keepdims=True)

    def put(lo, value):
        wide_g[:, :, :, :, :, lo:lo + WIDE] = value.reshape(wide_g.shape[:5] + (WIDE,))

    d_out32 = d_out[...].astype(jnp.float32)
    put_small(2, d_out32)
    put_small(5, d_out32)
    if layer == 0:
        down_gradients(d_out, act, down_g, hooks)
    d_n2 = None
    for k in range(4):
        if k % 2 == 0:
            hooks.free(2 + k // 2)
        d_act = dot_bt(d_out[...], down_weight_part(down_w, layer, k)).astype(jnp.bfloat16)
        d_pre = d_act.astype(jnp.float32) * slope[:, k * WIDE:(k + 1) * WIDE]
        put_small(6 + k, d_pre)
        act[:, k * WIDE:(k + 1) * WIDE] = d_pre.astype(jnp.bfloat16)
        d_pre_bf = act[:, k * WIDE:(k + 1) * WIDE]
        put(UP + k * WIDE, dot_at(n2[...], d_pre_bf))
        term = dot_bt(d_pre_bf, weight(wide_w, layer, UP + k * WIDE))
        d_n2 = term if d_n2 is None else d_n2 + term
        if k % 2:
            hooks('up', (0, UP + (k - 1) * WIDE))
    d_n2 = d_n2.astype(jnp.bfloat16)
    hooks.free(4)
    put(OUT, dot_at(ctx[...], d_out[...]))
    ctx[...] = dot_bt(d_out[...], weight(wide_w, layer, OUT)).astype(jnp.bfloat16)
    hooks('dctx', (0, OUT))
    masks, low = head_masks(), low_half(SEQ)
    for s in range(tokens // SEQ):
        @pl.loop(0, WIDE // PAIR)
        def attend(j, s=s):
            rows, cols = pair_block(s, j)
            query, key, value = qkv[0, rows, cols], qkv[1, rows, cols], qkv[2, rows, cols]
            d_ctx = ctx[rows, cols]
            d_q, d_k, d_v = [], [], []
            for h in range(2):
                attn = probs[s, j, h]
                d_probs = dot_bt(d_ctx * masks[h], value).astype(jnp.bfloat16).astype(jnp.float32)
                d_v.append(dot_at(attn.astype(jnp.bfloat16), d_ctx))
                inner = jnp.sum(d_probs * attn, axis=-1, keepdims=True)
                d_scores = (attn * (d_probs - inner) * 0.125).astype(jnp.bfloat16)
                d_q.append(dot(d_scores, key))
                d_k.append(dot_at(d_scores, query))
            qkv[0, rows, cols] = jnp.where(low, d_q[0], d_q[1]).astype(jnp.bfloat16)
            qkv[1, rows, cols] = jnp.where(low, d_k[0], d_k[1]).astype(jnp.bfloat16)
            qkv[2, rows, cols] = jnp.where(low, d_v[0], d_v[1]).astype(jnp.bfloat16)
        hooks('dattn')
    low = low_half(tokens)
    for j in range(WIDE // PAIR):
        cols = pl.ds(j * PAIR, PAIR)
        d_query, d_key, d_value = (qkv[t, :, cols].astype(jnp.float32) for t in range(3))
        d_query = rotate_back(d_query, tab)
        d_key = pltpu.roll(rotate_back(d_key, tab), PAIR // 2, 1)
        parts = (jnp.where(low, d_query, d_key), jnp.where(low, d_value, d_query), jnp.where(low, d_key, d_value))
        for m, part in enumerate(parts):
            lo = (3 * j + m) * PAIR
            row = layer * SMALL + 10 + lo // WIDE
            small_grads[pl.ds(row, 1), pl.ds(lo % WIDE, PAIR)] = jnp.sum(part, axis=0, keepdims=True)
            d_qkv[:, lo:lo + PAIR] = part.astype(jnp.bfloat16)
    d_n1 = None
    for t in (2, 1, 0):
        if t:
            hooks.free(7 - t)
        piece = d_qkv[:, t * WIDE:(t + 1) * WIDE]
        put(t * WIDE, dot_at(n1[...], piece))
        term = dot_bt(piece, weight(wide_w, layer, t * WIDE))
        d_n1 = term if d_n1 is None else d_n1 + term
        hooks('dqkv', (0, t * WIDE))
    d_n1 = d_n1.astype(jnp.bfloat16).astype(jnp.float32)
    d_n2 = d_n2.astype(jnp.float32)
    scaled, rstd = normalised(hidden[...].astype(jnp.float32))
    put_small(0, d_n1 * scaled)
    put_small(1, d_n1)
    put_small(3, d_n2 * scaled)
    put_small(4, d_n2)
    d_scaled = d_n1 * vec(0) + d_n2 * vec(3)
    d_hidden = rstd * (d_scaled - jnp.mean(d_scaled, axis=-1, keepdims=True)
                       - scaled * jnp.mean(d_scaled * scaled, axis=-1, keepdims=True))
    return (d_out32 + d_hidden).astype(jnp.bfloat16)


def places(rank, part, width):
    shift = lax.broadcasted_iota(jnp.int32, (part, width), 1) - lax.broadcasted_iota(jnp.int32, (part, width), 0)
    return jnp.where(shift == rank * part, 1.0, 0.0).astype(jnp.bfloat16)


VECTOR_ROWS = ((0, 1), (1, 1), (10, 3), (2, 1), (3, 1), (4, 1), (6, 4), (5, 1))


def place_small(rank, vectors, small_own):
    small_own[...] = jnp.zeros_like(small_own)
    for ref, (row, count) in zip(vectors, VECTOR_ROWS):
        wide = dot(ref[...], places(rank, ref.shape[1], count * WIDE))
        for layer in range(LAYERS):
            for i in range(count):
                small_own[pl.ds(layer * SMALL + row + i, 1), :] = wide[layer:layer + 1, i * WIDE:(i + 1) * WIDE]


def step_kernel(x, y_cot, qkv_own, out_own, up_own, down_own, *refs):
    (gain1, bias1, qkv_b, out_b, gain2, bias2, up_b, down_b, tab,
     y_out, x_grad, wide_out, down_out, small_out,
     wide_own, wide_w, down_w, wide_g, down_g) = refs[:19]
    wide_parts, down_parts = refs[19:24], refs[24:29]
    ring, plane = refs[29:31]
    (small_own, small, small_grads, small_bufs, small_grad_bufs,
     n1, n2, qkv, probs, ctx, slope, act, d_qkv, hidden1, d_hidden1, send_sems, recv_sems) = refs[31:]
    saved = (n1, n2, qkv, probs, ctx, slope, act, d_qkv)
    weights, grads = (wide_w, down_w), (wide_g, down_g)
    pos = positions()
    rank = pos[0] * 8 + pos[1]
    wide_own[:, :, :OUT] = qkv_own[...]
    wide_own[:, :, OUT:UP] = out_own[...]
    wide_own[:, :, UP:] = up_own[...]
    place_small(rank, (gain1, bias1, qkv_b, out_b, gain2, bias2, up_b, down_b), small_own)
    small_grads[...] = jnp.zeros_like(small_grads)
    entry_barrier(pos)
    copies = Copies(send_sems, recv_sems)

    small_gen = small_reduce_steps(copies, pos, small_own, small_bufs, small)
    done = []
    pieces = []
    for i in range(LAYERS):
        pieces.append(gather_steps(copies, pos, wide_own.at[i], wide_w.at[i], 0, UP))
        pieces.append(gather_steps(copies, pos, wide_own.at[i], wide_w.at[i], UP, UP))
        pieces.append(gather_steps(copies, pos, down_own.at[i], down_w.at[i], 0, WIDE))
    gather = gather_program(pieces, small_gen, done)

    def gather_until(piece):
        while piece not in done:
            next(gather)

    def gather_pump(count):
        for _ in range(count):
            next(gather, None)

    program = ScatterProgram()

    def add(layer, kind, lo):
        if kind and lo == 0:
            steps = scatter_z_first_steps(copies, pos, down_g, down_parts[0].at[layer], ring.at[layer], plane.at[layer],
                                          down_out.at[layer], lo, WIDE // 2)
        else:
            width = WIDE // 2 if kind else WIDE if OUT <= lo < UP or (layer == 0 or lo) and lo < OUT else 2 * WIDE
            parts = (wide_parts, down_parts)[kind]
            steps = scatter_chunk_steps(copies, pos, grads[kind], *(ref.at[layer] for ref in parts),
                                        (wide_out, down_out)[kind].at[layer], lo, width, layer == 0 and lo in DIRECT)
        program.add(steps)

    class Hooks:
        def __init__(self, layer, counts, reused):
            self.layer, self.counts, self.reused = layer, counts_of(counts), reused

        def free(self, idx):
            if self.reused:
                program.ensure(idx)

        def __call__(self, name, chunk=None):
            if chunk is not None and (self.layer == 0 or chunk != (0, WIDE)):
                add(self.layer, *chunk)
            program.pump(next(self.counts))

    hooks1 = Hooks(1, SCATTER_PUMPS[0], False)
    gather_until(0)

    def forward_hooks(layer):
        counts = counts_of(GATHER_PUMPS[layer])

        def hooks(name):
            if name == 'out':
                gather_until(3 * layer + 1)
            elif name == 'up':
                if layer == 1:
                    down_gradients(y_cot, act, down_g, hooks1)
                gather_until(3 * layer + 2)
            else:
                gather_pump(next(counts))
        return hooks

    hidden1[...] = layer_forward(0, x, weights, small, tab, saved, forward_hooks(0))
    gather_until(3)
    y_out[...] = layer_forward(1, hidden1, weights, small, tab, saved, forward_hooks(1))
    gather_until(5)

    d_hidden1[...] = layer_backward(1, hidden1, y_cot, weights, small, tab, saved, grads, small_grads,
                                    hooks1)
    layer_forward(0, x, weights, small, tab, saved, Hooks(0, SCATTER_PUMPS[1], False))
    x_grad[...] = layer_backward(0, x, d_hidden1, weights, small, tab, saved, grads, small_grads,
                                 Hooks(0, SCATTER_PUMPS[2], True))
    program.add(small_reduce_steps(copies, pos, small_grads, small_grad_bufs, small_out), SMALL_TURN)
    program.pump(len(program.order))
    copies.finish()


def part_scratch(rows, width):
    return [pltpu.VMEM((LAYERS, 4, 2, 2, rows, width), jnp.float32),
            pltpu.VMEM((LAYERS, 4, 2, rows, width // 2), jnp.float32),
            pltpu.VMEM((LAYERS, 4, 2, rows, width // 2), jnp.float32),
            pltpu.VMEM((LAYERS, 4, rows, width), jnp.float32),
            pltpu.VMEM((LAYERS, 3, rows, width), jnp.float32)]


def step_call(x, y_cot, matrices, vectors, tab):
    tokens, d_model = x.shape
    rows, down_rows = matrices[1].shape[1], matrices[3].shape[1]
    vmem = pl.BlockSpec(memory_space=pltpu.VMEM)
    bf16, f32 = jnp.bfloat16, jnp.float32
    small = (LAYERS * SMALL, d_model)
    n_sems = 12 + 6 * 23 + 8 * 15
    return pl.pallas_call(
        step_kernel,
        out_shape=(jax.ShapeDtypeStruct(x.shape, bf16), jax.ShapeDtypeStruct(x.shape, bf16),
                   jax.ShapeDtypeStruct((LAYERS, rows, ACOLS), bf16),
                   jax.ShapeDtypeStruct((LAYERS, down_rows, d_model), bf16), jax.ShapeDtypeStruct(small, f32)),
        in_specs=[vmem] * (2 + 4 + 8 + 1), out_specs=(vmem,) * 5,
        scratch_shapes=[
            pltpu.VMEM((LAYERS, rows, ACOLS), bf16),
            pltpu.VMEM((LAYERS, 4, 2, 2, 2, rows, ACOLS), bf16),
            pltpu.VMEM((LAYERS, 4, 2, 2, 2, down_rows, d_model), bf16),
            pltpu.VMEM((4, 2, 2, 2, rows, ACOLS), f32),
            pltpu.VMEM((4, 2, 2, 2, down_rows, d_model), f32),
            *part_scratch(rows, ACOLS), *part_scratch(down_rows, d_model),
            pltpu.VMEM((LAYERS, 3, 2, 2, down_rows, d_model // 2), f32),
            pltpu.VMEM((LAYERS, 3, down_rows, d_model // 2), f32),
            pltpu.VMEM(small, f32),
            pltpu.VMEM(small, f32),
            pltpu.VMEM(small, f32),
            pltpu.VMEM((9,) + small, f32),
            pltpu.VMEM((9,) + small, f32),
            pltpu.VMEM((tokens, d_model), bf16),
            pltpu.VMEM((tokens, d_model), bf16),
            pltpu.VMEM((3, tokens, d_model), bf16),
            pltpu.VMEM((tokens // SEQ, 4, 2, SEQ, SEQ), f32),
            pltpu.VMEM((tokens, d_model), bf16),
            pltpu.VMEM((tokens, 4 * d_model), f32),
            pltpu.VMEM((tokens, 4 * d_model), bf16),
            pltpu.VMEM((tokens, 3 * d_model), bf16),
            pltpu.VMEM((tokens, d_model), bf16),
            pltpu.VMEM((tokens, d_model), bf16),
            pltpu.SemaphoreType.DMA((n_sems,)), pltpu.SemaphoreType.DMA((n_sems,))],
        compiler_params=pltpu.CompilerParams(collective_id=0, has_side_effects=True,
                                             vmem_limit_bytes=67043328),
    )(x, y_cot, *matrices, *vectors, tab)


def finish_kernel(y_in, x_grad_in, wide, down, small, y_out, x_grad, gain1, bias1, qkv_g, qkv_b, out_g, out_b,
                  gain2, bias2, up_g, up_b, down_g, down_b):
    y_out[...] = y_in[...]
    x_grad[...] = x_grad_in[...]
    qkv_g[...] = wide[:, :, :OUT]
    out_g[...] = wide[:, :, OUT:UP]
    up_g[...] = wide[:, :, UP:]
    down_g[...] = down[...]
    rank = lax.axis_index('node') * 8 + lax.axis_index('local')
    for ref, (row, count) in zip((gain1, bias1, qkv_b, out_b, gain2, bias2, up_b, down_b), VECTOR_ROWS):
        sums = []
        for layer in range(LAYERS):
            lines = [small[pl.ds(layer * SMALL + row + i, 1), :] for i in range(count)]
            sums.append(jnp.concatenate(lines, axis=1))
        sums = jnp.concatenate(sums, axis=0).astype(jnp.bfloat16)
        ref[...] = dot_bt(sums, places(rank, ref.shape[1], count * WIDE)).astype(jnp.bfloat16)


def finish_call(y, x_grad, wide, down, small, shapes):
    vmem = pl.BlockSpec(memory_space=pltpu.VMEM)
    return pl.pallas_call(
        finish_kernel, out_shape=tuple(jax.ShapeDtypeStruct(s, jnp.bfloat16) for s in shapes),
        in_specs=[vmem] * 5, out_specs=(vmem,) * len(shapes),
    )(y, x_grad, wide, down, small)


def rope_table(seq_len, rot_dim):
    inv_freq = 1.0 / (np.float32(10000.0) ** (np.arange(0, rot_dim, 2, dtype=np.float32) / np.float32(rot_dim)))
    angles = np.arange(seq_len, dtype=np.float32)[:, None] * inv_freq[None, :].astype(np.float32)
    cos, sin = np.cos(angles), np.sin(angles)
    none = np.zeros_like(sin)
    rest = np.zeros((seq_len, 3 * rot_dim), np.float32)
    parts = ([cos, cos, rest + 1.0], [-sin, none, rest], [none, sin, rest])
    return np.stack([np.tile(np.concatenate(p, axis=-1), (1, 2)) for p in parts]).astype(np.float32)


def solution(mesh):
    shard_axes = ('node', 'local')
    act_spec = P(shard_axes)
    param_spec = P(None, shard_axes)

    def device_step(x, y_cot, ln1_gain, ln1_bias, qkv_weight, qkv_bias, out_weight, out_bias,
                    ln2_gain, ln2_bias, up_weight, up_bias, down_weight, down_bias):
        d_model, rows = x.shape[2], out_weight.shape[1]
        flat = (x.shape[0] * x.shape[1], d_model)
        qkv_flat = (LAYERS, rows, 3 * d_model)
        matrices = (qkv_weight.reshape(qkv_flat), out_weight, up_weight, down_weight)
        vectors = (ln1_gain, ln1_bias, qkv_bias, out_bias, ln2_gain, ln2_bias, up_bias, down_bias)
        sums = step_call(x.reshape(flat), y_cot.reshape(flat), matrices, vectors, rope_table(x.shape[1], qkv_weight.shape[3] // 12))
        shapes = [flat, flat, ln1_gain.shape, ln1_bias.shape, qkv_flat, qkv_bias.shape, out_weight.shape, out_bias.shape,
                  ln2_gain.shape, ln2_bias.shape, up_weight.shape, up_bias.shape, down_weight.shape, down_bias.shape]
        outs = list(finish_call(*sums, shapes))
        outs[0], outs[1], outs[4] = outs[0].reshape(x.shape), outs[1].reshape(x.shape), outs[4].reshape(qkv_weight.shape)
        return tuple(outs)

    return jax.shard_map(device_step, mesh=mesh,
                         in_specs=(act_spec, act_spec) + (param_spec,) * 12,
                         out_specs=(act_spec, act_spec) + (param_spec,) * 12,
                         check_vma=False)
```

```python
import functools
import jax
import numpy as np
import jax.numpy as jnp
from jax import lax
from jax.experimental import pallas as pl
from jax.experimental.pallas import tpu as pltpu
from jax.sharding import PartitionSpec as P

EPSILON = 1e-5
MESH = pl.DeviceIdType.MESH
LAYERS = 2
ROWS = 16
SMALL = 16
WIDE = 512
PAIR = 128
SEQ = 128
OUT, UP, ACOLS = 3 * WIDE, 4 * WIDE, 8 * WIDE


def positions():
    z = lax.axis_index('node')
    l = lax.axis_index('local')
    c = l % 2
    x = (l // 2) % 2
    y = l // 4
    partner = (z, l + 1 - 2 * c)
    x_nbr = (z, l + 2 - 4 * x)
    y_nbr = (z, (l + 4) % 8)
    z_others = [z + 1 - 2 * (z % 2), (z + 2) % 4, 3 - z]
    return z, l, c, x, y, partner, x_nbr, y_nbr, z_others


def ring_of(z, l):
    return ((z + 1) % 4, l), [z, (z + 3) % 4, (z + 2) % 4, (z + 1) % 4]


def entry_barrier(pos):
    z, l, c, x, y, partner, x_nbr, y_nbr, z_others = pos
    barrier = pltpu.get_barrier_semaphore()
    for dev in [partner, x_nbr, y_nbr] + [(zo, l) for zo in z_others]:
        pl.semaphore_signal(barrier, inc=1, device_id=dev, device_id_type=MESH)
    pl.semaphore_wait(barrier, 6)


class Copies:
    def __init__(self, send_sems, recv_sems):
        self.send_sems, self.recv_sems, self.used = send_sems, recv_sems, 0
        self.open_sends = []

    def make(self, src, dst, dev):
        idx = self.used
        self.used += 1
        return pltpu.make_async_remote_copy(src_ref=src, dst_ref=dst, send_sem=self.send_sems.at[idx],
                                            recv_sem=self.recv_sems.at[idx], device_id=dev, device_id_type=MESH)

    def start(self, src, dst, dev):
        copy = self.make(src, dst, dev)
        copy.start()
        self.open_sends.append(copy)
        return copy

    def finish(self):
        for copy in self.open_sends:
            copy.wait_send()
        self.open_sends = []


def small_reduce_steps(copies, pos, src, bufs, out):
    z, l, c, x, y, partner, x_nbr, y_nbr, z_others = pos
    held = src
    for step, dev in enumerate((partner, x_nbr, y_nbr)):
        copy = copies.start(held, bufs.at[2 * step], dev)
        yield
        copy.wait_recv()
        bufs[2 * step + 1] = held[...] + bufs[2 * step]
        held = bufs.at[2 * step + 1]
    sends = [copies.start(held, bufs.at[6 + k], (zo, l)) for k, zo in enumerate(z_others)]
    yield
    for copy in sends:
        copy.wait_recv()
    out[...] = (held[...] + bufs[6]) + (bufs[7] + bufs[8])
    yield


def gather_steps(copies, pos, own, full, lo, width):
    z, l, c, x, y, partner, x_nbr, y_nbr, z_others = pos
    half = width // 2
    cols, cols_a, cols_b = pl.ds(lo, width), pl.ds(lo, half), pl.ds(lo + half, half)
    after, z_order = ring_of(z, l)

    def block(zz, yy, xx, cc):
        return full.at[zz, yy, xx, cc, :, cols]

    from_z, from_x, from_y, diag, to_partner = [None] * 4, [None] * 4, [None] * 4, [], []

    def spread(k, got, place):
        if k < 3:
            from_z[k + 1] = copies.start(got, place, after)
        from_x[k] = copies.start(got, place, x_nbr)
        from_y[k] = copies.start(got, place, y_nbr)

    def forward_z(k):
        from_z[k].wait_recv()
        got = block(z_order[k], y, x, c)
        spread(k, got, got)

    def forward_cross(k):
        zz = z_order[k]
        from_x[k].wait_recv()
        got = full.at[zz, y, 1 - x, c, :, cols_a]
        diag.append(copies.start(got, got, y_nbr))
        from_y[k].wait_recv()
        got = full.at[zz, 1 - y, x, c, :, cols_b]
        diag.append(copies.start(got, got, x_nbr))

    def forward_partner(yy, xx):
        got = full.at[:, yy, xx, c, :, cols]
        to_partner.append(copies.start(got, got, partner))

    spread(0, own.at[:, cols], block(z, y, x, c))
    full[z, y, x, c, :, cols] = own[:, cols]
    yield
    forward_z(1)
    yield
    forward_cross(0)
    yield
    forward_z(2)
    yield
    forward_cross(1)
    yield
    forward_z(3)
    forward_partner(y, x)
    yield
    forward_cross(2)
    yield
    forward_cross(3)
    forward_partner(y, 1 - x)
    forward_partner(1 - y, x)
    yield
    for copy in diag:
        copy.wait_recv()
    forward_partner(1 - y, 1 - x)
    yield
    for copy in to_partner:
        copy.wait_recv()
    yield


GATHER_ORDERS = ('zacbdezafcbzaacdbcbazaccdbbdaaeccabbzddefaecbddcbeeffddeeffe', 'ffeff')
GATHER_PUMPS = ('11330204', '11113410')
SCATTER_ORDERS = ('abcabdcbeadcfbedgacbfehdcgfiedgjfehibkgfjiaclhgakjdmilkenhji', 'mlzfokjmgnlkzomlzinmhjohklnmoz')
SCATTER_PUMPS = ('0200121000', '1401111220', '4320440343')
DIRECT = (0, WIDE)


SMALL_TURN = ord('z') - ord('a')


def turns(parts):
    return [ord(letter) - ord('a') for part in parts for letter in part]


def counts_of(digits):
    return iter([int(digit) for digit in digits])


def gather_program(pieces, small_gen, done):
    order = turns(GATHER_ORDERS)
    left = [order.count(i) for i in range(len(pieces))]
    for i in order:
        if i == SMALL_TURN:
            next(small_gen)
            continue
        next(pieces[i])
        left[i] -= 1
        if not left[i]:
            done.append(i)
        yield


def scatter_chunk_steps(copies, pos, grads, part0, partx, party, last, partz, out, lo, width, direct):
    z, l, c, x, y, partner, x_nbr, y_nbr, z_others = pos
    half = width // 2
    cols, cols_a, cols_b = pl.ds(lo, width), pl.ds(lo, half), pl.ds(lo + half, half)
    after, z_order = ring_of(z, l)
    hcols = pl.ds(lo // 2, half)
    swap = copies.make(grads.at[:, :, :, 1 - c, :, cols], part0.at[:, :, :, :, cols], partner)
    swap.start()
    yield
    swap.wait()
    part0[:, :, :, :, cols] = part0[:, :, :, :, cols] + grads[:, :, :, c, :, cols]
    send_a = copies.start(part0.at[:, :, 1 - x, :, cols_a], partx.at[:, :, :, hcols], x_nbr)
    send_b = copies.start(part0.at[:, 1 - y, :, :, cols_b], party.at[:, :, :, hcols], y_nbr)
    yield
    send_a.wait_recv()
    partx[:, :, :, hcols] = partx[:, :, :, hcols] + part0[:, :, x, :, cols_a]
    send_a = copies.start(partx.at[:, 1 - y, :, hcols], last.at[:, :, cols_a], y_nbr)
    send_b.wait_recv()
    party[:, :, :, hcols] = party[:, :, :, hcols] + part0[:, y, :, :, cols_b]
    send_b = copies.start(party.at[:, 1 - x, :, hcols], last.at[:, :, cols_b], x_nbr)
    yield
    send_a.wait_recv()
    send_b.wait_recv()
    last[:, :, cols_a] = last[:, :, cols_a] + partx[:, y, :, hcols]
    last[:, :, cols_b] = last[:, :, cols_b] + party[:, x, :, hcols]
    if direct:
        sends = [copies.start(last.at[zo, :, cols], partz.at[k, :, cols], (zo, l)) for k, zo in enumerate(z_others)]
        yield
        for copy in sends:
            copy.wait_recv()
        total = (last[z, :, cols] + partz[0, :, cols]) + (partz[1, :, cols] + partz[2, :, cols])
    else:
        send = copies.start(last.at[z_order[1], :, cols], partz.at[0, :, cols], after)
        yield
        for k in (1, 2):
            send.wait_recv()
            partz[k - 1, :, cols] = partz[k - 1, :, cols] + last[z_order[k + 1], :, cols]
            send = copies.start(partz.at[k - 1, :, cols], partz.at[k, :, cols], after)
            yield
        send.wait_recv()
        total = partz[2, :, cols] + last[z, :, cols]
    out[:, cols] = total.astype(out.dtype)
    yield


def scatter_z_first_steps(copies, pos, grads, part0, ring, plane, out, lo, width):
    z, l, c, x, y, partner, x_nbr, y_nbr, z_others = pos
    half = width // 2
    cols, cols_a, cols_b = pl.ds(lo, width), pl.ds(lo, half), pl.ds(lo + half, half)
    first_a, first_b = pl.ds(0, half), pl.ds(half, half)
    after, z_order = ring_of(z, l)
    swap = copies.make(grads.at[:, :, :, 1 - c, :, cols], part0.at[:, :, :, :, cols], partner)
    swap.start()
    yield
    swap.wait()
    part0[:, :, :, :, cols] = part0[:, :, :, :, cols] + grads[:, :, :, c, :, cols]
    send = copies.start(part0.at[z_order[1], :, :, :, cols], ring.at[0], after)
    yield
    for k in (1, 2):
        send.wait_recv()
        ring[k - 1] = ring[k - 1] + part0[z_order[k + 1], :, :, :, cols]
        send = copies.start(ring.at[k - 1], ring.at[k], after)
        yield
    send.wait_recv()
    ring[2] = ring[2] + part0[z, :, :, :, cols]
    send_a = copies.start(ring.at[2, :, 1 - x, :, first_a], plane.at[:2, :, first_a], x_nbr)
    send_b = copies.start(ring.at[2, 1 - y, :, :, first_b], plane.at[:2, :, first_b], y_nbr)
    yield
    send_a.wait_recv()
    plane[:2, :, first_a] = plane[:2, :, first_a] + ring[2, :, x, :, first_a]
    send_a = copies.start(plane.at[1 - y, :, first_a], plane.at[2, :, first_a], y_nbr)
    send_b.wait_recv()
    plane[:2, :, first_b] = plane[:2, :, first_b] + ring[2, y, :, :, first_b]
    send_b = copies.start(plane.at[1 - x, :, first_b], plane.at[2, :, first_b], x_nbr)
    yield
    send_a.wait_recv()
    send_b.wait_recv()
    out[:, cols_a] = (plane[y, :, first_a] + plane[2, :, first_a]).astype(out.dtype)
    out[:, cols_b] = (plane[x, :, first_b] + plane[2, :, first_b]).astype(out.dtype)
    yield


class ScatterProgram:
    def __init__(self):
        self.chunks, self.turn = {}, 0
        self.order = turns(SCATTER_ORDERS)

    def add(self, chunk, idx=None):
        next(chunk)
        self.chunks[len(self.chunks) if idx is None else idx] = chunk

    def pump(self, count):
        while count and self.turn < len(self.order) and self.order[self.turn] in self.chunks:
            next(self.chunks[self.order[self.turn]])
            self.turn += 1
            count -= 1

    def ensure(self, idx):
        while idx not in self.order[:self.turn]:
            assert self.order[self.turn] in self.chunks
            self.pump(1)


def dot(first, second):
    return lax.dot_general(first, second, (((1,), (0,)), ((), ())), preferred_element_type=jnp.float32)


def dot_bt(first, second):
    return lax.dot_general(first, second, (((1,), (1,)), ((), ())), preferred_element_type=jnp.float32)


def dot_at(first, second):
    return lax.dot_general(first, second, (((0,), (0,)), ((), ())), preferred_element_type=jnp.float32)


def normalised(hidden32):
    center = hidden32 - jnp.mean(hidden32, axis=-1, keepdims=True)
    rstd = lax.rsqrt(jnp.mean(center * center, axis=-1, keepdims=True) + EPSILON)
    return center * rstd, rstd


def weight(full, layer, lo, width=WIDE):
    return full[layer, :, :, :, :, :, lo:lo + width].reshape(WIDE, width)


def down_weight_part(full, layer, k):
    return full[layer, k].reshape(WIDE, WIDE)


def rotate(piece, tab):
    piece = piece.reshape(-1, SEQ, PAIR)
    up, down = pltpu.roll(piece, PAIR - 8, 2), pltpu.roll(piece, 8, 2)
    return (piece * tab[0] + up * tab[1] + down * tab[2]).reshape(-1, PAIR)


def rotate_back(piece, tab):
    piece = piece.reshape(-1, SEQ, PAIR)
    turned = (piece * tab[0] + pltpu.roll(piece * tab[1], 8, 2) + pltpu.roll(piece * tab[2], PAIR - 8, 2))
    return turned.reshape(-1, PAIR)


def low_half(rows):
    return lax.broadcasted_iota(jnp.int32, (rows, PAIR), 1) < PAIR // 2


def head_masks():
    first = low_half(SEQ)
    return (jnp.where(first, 1.0, 0.0).astype(jnp.bfloat16), jnp.where(first, 0.0, 1.0).astype(jnp.bfloat16))


def pair_block(s, j):
    return pl.ds(s * SEQ, SEQ), pl.ds(pl.multiple_of(j * PAIR, PAIR), PAIR)


def layer_forward(layer, hidden, weights, small, tab, saved, hooks):
    n1, n2, qkv, probs, ctx, slope, act, d_qkv = saved
    wide_w, down_w = weights
    tokens = hidden.shape[0]

    def vec(row):
        return small[pl.ds(layer * SMALL + row, 1), :]

    hidden32 = hidden[...].astype(jnp.float32)
    scaled, _ = normalised(hidden32)
    n1[...] = (scaled * vec(0) + vec(1)).astype(jnp.bfloat16)
    n2[...] = (scaled * vec(3) + vec(4)).astype(jnp.bfloat16)
    hooks('norm')
    low = low_half(tokens)
    qkv_bias = jnp.concatenate([vec(10), vec(11), vec(12)], axis=1)
    group = 6 * PAIR
    for i in range(2):
        part = dot(n1[...], weight(wide_w, layer, i * group, group)) + qkv_bias[:, i * group:(i + 1) * group]
        for jj in range(2):
            first, second, third = (part[:, (3 * jj + m) * PAIR:(3 * jj + m + 1) * PAIR] for m in range(3))
            cols = pl.ds((2 * i + jj) * PAIR, PAIR)
            query = jnp.where(low, first, second)
            key = jnp.where(low, pltpu.roll(first, PAIR // 2, 1), pltpu.roll(third, PAIR // 2, 1))
            qkv[0, :, cols] = rotate(query, tab).astype(jnp.bfloat16)
            qkv[1, :, cols] = rotate(key, tab).astype(jnp.bfloat16)
            qkv[2, :, cols] = jnp.where(low, second, third).astype(jnp.bfloat16)
    hooks('qkv')
    causal = (lax.broadcasted_iota(jnp.int32, (SEQ, SEQ), 0) >= lax.broadcasted_iota(jnp.int32, (SEQ, SEQ), 1))
    masks, low = head_masks(), low_half(SEQ)
    for s in range(tokens // SEQ):
        @pl.loop(0, WIDE // PAIR, unroll=True)
        def attend(j, s=s):
            rows, cols = pair_block(s, j)
            query, key, value = qkv[0, rows, cols], qkv[1, rows, cols], qkv[2, rows, cols]
            heads = []
            for h in range(2):
                scores = dot_bt(query * masks[h], key) * 0.125
                scores = jnp.where(causal, scores, -1e30)
                attn = jnp.exp(scores - jnp.max(scores, axis=-1, keepdims=True))
                attn = attn / jnp.sum(attn, axis=-1, keepdims=True)
                probs[s, j, h] = attn
                heads.append(dot(attn.astype(jnp.bfloat16), value))
            ctx[rows, cols] = jnp.where(low, heads[0], heads[1]).astype(jnp.bfloat16)
        hooks('attn')
    total = hidden32 + (dot(ctx[...], weight(wide_w, layer, OUT)) + vec(2))
    hooks('out')
    for k in range(4):
        pre = dot(n2[...], weight(wide_w, layer, UP + k * WIDE)) + vec(6 + k)
        bell = lax.erf(pre * 0.7071067811865476) + 1.0
        act[:, k * WIDE:(k + 1) * WIDE] = (0.5 * pre * bell).astype(jnp.bfloat16)
        slope[:, k * WIDE:(k + 1) * WIDE] = 0.5 * bell + pre * (jnp.exp(-0.5 * pre * pre) * 0.3989422804014327)
    hooks('up')
    mlp = None
    for k in range(4):
        term = dot(act[:, k * WIDE:(k + 1) * WIDE], down_weight_part(down_w, layer, k))
        mlp = term if mlp is None else mlp + term
        hooks('mlp')
    return (total + (mlp + vec(5))).astype(jnp.bfloat16)


def down_gradients(d_out, act, down_g, hooks):
    half = WIDE // 2
    for k in range(2):
        hooks.free(k)
        value = dot_at(act[...], d_out[:, k * half:(k + 1) * half])
        down_g[:, :, :, :, :, k * half:(k + 1) * half] = value.reshape(down_g.shape[:5] + (half,))
        hooks('down', (1, k * half))


def layer_backward(layer, hidden, d_out, weights, small, tab, saved, grads, small_grads, hooks):
    n1, n2, qkv, probs, ctx, slope, act, d_qkv = saved
    wide_w, down_w = weights
    wide_g, down_g = grads
    tokens = hidden.shape[0]

    def vec(row):
        return small[pl.ds(layer * SMALL + row, 1), :]

    def put_small(row, value):
        small_grads[pl.ds(layer * SMALL + row, 1), :] = jnp.sum(value, axis=0, keepdims=True)

    def put(lo, value):
        wide_g[:, :, :, :, :, lo:lo + WIDE] = value.reshape(wide_g.shape[:5] + (WIDE,))

    d_out32 = d_out[...].astype(jnp.float32)
    put_small(2, d_out32)
    put_small(5, d_out32)
    if layer == 0:
        down_gradients(d_out, act, down_g, hooks)
    d_n2 = None
    for k in range(4):
        if k % 2 == 0:
            hooks.free(2 + k // 2)
        d_act = dot_bt(d_out[...], down_weight_part(down_w, layer, k)).astype(jnp.bfloat16)
        d_pre = d_act.astype(jnp.float32) * slope[:, k * WIDE:(k + 1) * WIDE]
        put_small(6 + k, d_pre)
        act[:, k * WIDE:(k + 1) * WIDE] = d_pre.astype(jnp.bfloat16)
        d_pre_bf = act[:, k * WIDE:(k + 1) * WIDE]
        put(UP + k * WIDE, dot_at(n2[...], d_pre_bf))
        term = dot_bt(d_pre_bf, weight(wide_w, layer, UP + k * WIDE))
        d_n2 = term if d_n2 is None else d_n2 + term
        if k % 2:
            hooks('up', (0, UP + (k - 1) * WIDE))
    d_n2 = d_n2.astype(jnp.bfloat16)
    hooks.free(4)
    put(OUT, dot_at(ctx[...], d_out[...]))
    ctx[...] = dot_bt(d_out[...], weight(wide_w, layer, OUT)).astype(jnp.bfloat16)
    hooks('dctx', (0, OUT))
    masks, low = head_masks(), low_half(SEQ)
    for s in range(tokens // SEQ):
        @pl.loop(0, WIDE // PAIR, unroll=True)
        def attend(j, s=s):
            rows, cols = pair_block(s, j)
            query, key, value = qkv[0, rows, cols], qkv[1, rows, cols], qkv[2, rows, cols]
            d_ctx = ctx[rows, cols]
            d_q, d_k, d_v = [], [], []
            for h in range(2):
                attn = probs[s, j, h]
                d_probs = dot_bt(d_ctx * masks[h], value).astype(jnp.bfloat16).astype(jnp.float32)
                d_v.append(dot_at(attn.astype(jnp.bfloat16), d_ctx))
                inner = jnp.sum(d_probs * attn, axis=-1, keepdims=True)
                d_scores = (attn * (d_probs - inner) * 0.125).astype(jnp.bfloat16)
                d_q.append(dot(d_scores, key))
                d_k.append(dot_at(d_scores, query))
            qkv[0, rows, cols] = jnp.where(low, d_q[0], d_q[1]).astype(jnp.bfloat16)
            qkv[1, rows, cols] = jnp.where(low, d_k[0], d_k[1]).astype(jnp.bfloat16)
            qkv[2, rows, cols] = jnp.where(low, d_v[0], d_v[1]).astype(jnp.bfloat16)
        hooks('dattn')
    low = low_half(tokens)
    for j in range(WIDE // PAIR):
        cols = pl.ds(j * PAIR, PAIR)
        d_query, d_key, d_value = (qkv[t, :, cols].astype(jnp.float32) for t in range(3))
        d_query = rotate_back(d_query, tab)
        d_key = pltpu.roll(rotate_back(d_key, tab), PAIR // 2, 1)
        parts = (jnp.where(low, d_query, d_key), jnp.where(low, d_value, d_query), jnp.where(low, d_key, d_value))
        for m, part in enumerate(parts):
            lo = (3 * j + m) * PAIR
            row = layer * SMALL + 10 + lo // WIDE
            small_grads[pl.ds(row, 1), pl.ds(lo % WIDE, PAIR)] = jnp.sum(part, axis=0, keepdims=True)
            d_qkv[:, lo:lo + PAIR] = part.astype(jnp.bfloat16)
    d_n1 = None
    for t in (2, 1, 0):
        if t:
            hooks.free(7 - t)
        piece = d_qkv[:, t * WIDE:(t + 1) * WIDE]
        put(t * WIDE, dot_at(n1[...], piece))
        term = dot_bt(piece, weight(wide_w, layer, t * WIDE))
        d_n1 = term if d_n1 is None else d_n1 + term
        hooks('dqkv', (0, t * WIDE))
    d_n1 = d_n1.astype(jnp.bfloat16).astype(jnp.float32)
    d_n2 = d_n2.astype(jnp.float32)
    scaled, rstd = normalised(hidden[...].astype(jnp.float32))
    put_small(0, d_n1 * scaled)
    put_small(1, d_n1)
    put_small(3, d_n2 * scaled)
    put_small(4, d_n2)
    d_scaled = d_n1 * vec(0) + d_n2 * vec(3)
    d_hidden = rstd * (d_scaled - jnp.mean(d_scaled, axis=-1, keepdims=True)
                       - scaled * jnp.mean(d_scaled * scaled, axis=-1, keepdims=True))
    return (d_out32 + d_hidden).astype(jnp.bfloat16)


def places(rank, part, width):
    shift = lax.broadcasted_iota(jnp.int32, (part, width), 1) - lax.broadcasted_iota(jnp.int32, (part, width), 0)
    return jnp.where(shift == rank * part, 1.0, 0.0).astype(jnp.bfloat16)


VECTOR_ROWS = ((0, 1), (1, 1), (10, 3), (2, 1), (3, 1), (4, 1), (6, 4), (5, 1))


def place_small(rank, vectors, small_own):
    small_own[...] = jnp.zeros_like(small_own)
    for ref, (row, count) in zip(vectors, VECTOR_ROWS):
        wide = dot(ref[...], places(rank, ref.shape[1], count * WIDE))
        for layer in range(LAYERS):
            for i in range(count):
                small_own[pl.ds(layer * SMALL + row + i, 1), :] = wide[layer:layer + 1, i * WIDE:(i + 1) * WIDE]


def step_kernel(x, y_cot, qkv_own, out_own, up_own, down_own, *refs):
    (gain1, bias1, qkv_b, out_b, gain2, bias2, up_b, down_b, tab,
     y_out, x_grad, wide_out, down_out, small_out,
     wide_own, wide_w, down_w, wide_g, down_g) = refs[:19]
    wide_parts, down_parts = refs[19:24], refs[24:29]
    ring, plane = refs[29:31]
    (small_own, small, small_grads, small_bufs, small_grad_bufs,
     n1, n2, qkv, probs, ctx, slope, act, d_qkv, hidden1, d_hidden1, send_sems, recv_sems) = refs[31:]
    saved = (n1, n2, qkv, probs, ctx, slope, act, d_qkv)
    weights, grads = (wide_w, down_w), (wide_g, down_g)
    pos = positions()
    rank = pos[0] * 8 + pos[1]
    wide_own[:, :, :OUT] = qkv_own[...]
    wide_own[:, :, OUT:UP] = out_own[...]
    wide_own[:, :, UP:] = up_own[...]
    place_small(rank, (gain1, bias1, qkv_b, out_b, gain2, bias2, up_b, down_b), small_own)
    small_grads[...] = jnp.zeros_like(small_grads)
    entry_barrier(pos)
    copies = Copies(send_sems, recv_sems)

    small_gen = small_reduce_steps(copies, pos, small_own, small_bufs, small)
    done = []
    pieces = []
    for i in range(LAYERS):
        pieces.append(gather_steps(copies, pos, wide_own.at[i], wide_w.at[i], 0, UP))
        pieces.append(gather_steps(copies, pos, wide_own.at[i], wide_w.at[i], UP, UP))
        pieces.append(gather_steps(copies, pos, down_own.at[i], down_w.at[i], 0, WIDE))
    gather = gather_program(pieces, small_gen, done)

    def gather_until(piece):
        while piece not in done:
            next(gather)

    def gather_pump(count):
        for _ in range(count):
            next(gather, None)

    program = ScatterProgram()

    def add(layer, kind, lo):
        if kind and lo == 0:
            steps = scatter_z_first_steps(copies, pos, down_g, down_parts[0].at[layer], ring.at[layer], plane.at[layer],
                                          down_out.at[layer], lo, WIDE // 2)
        else:
            width = WIDE // 2 if kind else WIDE if OUT <= lo < UP or (layer == 0 or lo) and lo < OUT else 2 * WIDE
            parts = (wide_parts, down_parts)[kind]
            steps = scatter_chunk_steps(copies, pos, grads[kind], *(ref.at[layer] for ref in parts),
                                        (wide_out, down_out)[kind].at[layer], lo, width, layer == 0 and lo in DIRECT)
        program.add(steps)

    class Hooks:
        def __init__(self, layer, counts, reused):
            self.layer, self.counts, self.reused = layer, counts_of(counts), reused

        def free(self, idx):
            if self.reused:
                program.ensure(idx)

        def __call__(self, name, chunk=None):
            if chunk is not None and (self.layer == 0 or chunk != (0, WIDE)):
                add(self.layer, *chunk)
            program.pump(next(self.counts))

    hooks1 = Hooks(1, SCATTER_PUMPS[0], False)
    gather_until(0)

    def forward_hooks(layer):
        counts = counts_of(GATHER_PUMPS[layer])

        def hooks(name):
            if name == 'out':
                gather_until(3 * layer + 1)
            elif name == 'up':
                if layer == 1:
                    down_gradients(y_cot, act, down_g, hooks1)
                gather_until(3 * layer + 2)
            else:
                gather_pump(next(counts))
        return hooks

    hidden1[...] = layer_forward(0, x, weights, small, tab, saved, forward_hooks(0))
    gather_until(3)
    y_out[...] = layer_forward(1, hidden1, weights, small, tab, saved, forward_hooks(1))
    gather_until(5)

    d_hidden1[...] = layer_backward(1, hidden1, y_cot, weights, small, tab, saved, grads, small_grads,
                                    hooks1)
    layer_forward(0, x, weights, small, tab, saved, Hooks(0, SCATTER_PUMPS[1], False))
    x_grad[...] = layer_backward(0, x, d_hidden1, weights, small, tab, saved, grads, small_grads,
                                 Hooks(0, SCATTER_PUMPS[2], True))
    program.add(small_reduce_steps(copies, pos, small_grads, small_grad_bufs, small_out), SMALL_TURN)
    program.pump(len(program.order))
    copies.finish()


def part_scratch(rows, width):
    return [pltpu.VMEM((LAYERS, 4, 2, 2, rows, width), jnp.float32),
            pltpu.VMEM((LAYERS, 4, 2, rows, width // 2), jnp.float32),
            pltpu.VMEM((LAYERS, 4, 2, rows, width // 2), jnp.float32),
            pltpu.VMEM((LAYERS, 4, rows, width), jnp.float32),
            pltpu.VMEM((LAYERS, 3, rows, width), jnp.float32)]


def step_call(x, y_cot, matrices, vectors, tab):
    tokens, d_model = x.shape
    rows, down_rows = matrices[1].shape[1], matrices[3].shape[1]
    vmem = pl.BlockSpec(memory_space=pltpu.VMEM)
    bf16, f32 = jnp.bfloat16, jnp.float32
    small = (LAYERS * SMALL, d_model)
    n_sems = 12 + 6 * 23 + 8 * 15
    return pl.pallas_call(
        step_kernel,
        out_shape=(jax.ShapeDtypeStruct(x.shape, bf16), jax.ShapeDtypeStruct(x.shape, bf16),
                   jax.ShapeDtypeStruct((LAYERS, rows, ACOLS), bf16),
                   jax.ShapeDtypeStruct((LAYERS, down_rows, d_model), bf16), jax.ShapeDtypeStruct(small, f32)),
        in_specs=[vmem] * (2 + 4 + 8 + 1), out_specs=(vmem,) * 5,
        scratch_shapes=[
            pltpu.VMEM((LAYERS, rows, ACOLS), bf16),
            pltpu.VMEM((LAYERS, 4, 2, 2, 2, rows, ACOLS), bf16),
            pltpu.VMEM((LAYERS, 4, 2, 2, 2, down_rows, d_model), bf16),
            pltpu.VMEM((4, 2, 2, 2, rows, ACOLS), f32),
            pltpu.VMEM((4, 2, 2, 2, down_rows, d_model), f32),
            *part_scratch(rows, ACOLS), *part_scratch(down_rows, d_model),
            pltpu.VMEM((LAYERS, 3, 2, 2, down_rows, d_model // 2), f32),
            pltpu.VMEM((LAYERS, 3, down_rows, d_model // 2), f32),
            pltpu.VMEM(small, f32),
            pltpu.VMEM(small, f32),
            pltpu.VMEM(small, f32),
            pltpu.VMEM((9,) + small, f32),
            pltpu.VMEM((9,) + small, f32),
            pltpu.VMEM((tokens, d_model), bf16),
            pltpu.VMEM((tokens, d_model), bf16),
            pltpu.VMEM((3, tokens, d_model), bf16),
            pltpu.VMEM((tokens // SEQ, 4, 2, SEQ, SEQ), f32),
            pltpu.VMEM((tokens, d_model), bf16),
            pltpu.VMEM((tokens, 4 * d_model), f32),
            pltpu.VMEM((tokens, 4 * d_model), bf16),
            pltpu.VMEM((tokens, 3 * d_model), bf16),
            pltpu.VMEM((tokens, d_model), bf16),
            pltpu.VMEM((tokens, d_model), bf16),
            pltpu.SemaphoreType.DMA((n_sems,)), pltpu.SemaphoreType.DMA((n_sems,))],
        compiler_params=pltpu.CompilerParams(collective_id=0, has_side_effects=True,
                                             vmem_limit_bytes=67043328),
    )(x, y_cot, *matrices, *vectors, tab)


def finish_kernel(y_in, x_grad_in, wide, down, small, y_out, x_grad, gain1, bias1, qkv_g, qkv_b, out_g, out_b,
                  gain2, bias2, up_g, up_b, down_g, down_b):
    y_out[...] = y_in[...]
    x_grad[...] = x_grad_in[...]
    qkv_g[...] = wide[:, :, :OUT]
    out_g[...] = wide[:, :, OUT:UP]
    up_g[...] = wide[:, :, UP:]
    down_g[...] = down[...]
    rank = lax.axis_index('node') * 8 + lax.axis_index('local')
    for ref, (row, count) in zip((gain1, bias1, qkv_b, out_b, gain2, bias2, up_b, down_b), VECTOR_ROWS):
        sums = []
        for layer in range(LAYERS):
            lines = [small[pl.ds(layer * SMALL + row + i, 1), :] for i in range(count)]
            sums.append(jnp.concatenate(lines, axis=1))
        sums = jnp.concatenate(sums, axis=0).astype(jnp.bfloat16)
        ref[...] = dot_bt(sums, places(rank, ref.shape[1], count * WIDE)).astype(jnp.bfloat16)


def finish_call(y, x_grad, wide, down, small, shapes):
    vmem = pl.BlockSpec(memory_space=pltpu.VMEM)
    return pl.pallas_call(
        finish_kernel, out_shape=tuple(jax.ShapeDtypeStruct(s, jnp.bfloat16) for s in shapes),
        in_specs=[vmem] * 5, out_specs=(vmem,) * len(shapes),
    )(y, x_grad, wide, down, small)


def rope_table(seq_len, rot_dim):
    inv_freq = 1.0 / (np.float32(10000.0) ** (np.arange(0, rot_dim, 2, dtype=np.float32) / np.float32(rot_dim)))
    angles = np.arange(seq_len, dtype=np.float32)[:, None] * inv_freq[None, :].astype(np.float32)
    cos, sin = np.cos(angles), np.sin(angles)
    none = np.zeros_like(sin)
    rest = np.zeros((seq_len, 3 * rot_dim), np.float32)
    parts = ([cos, cos, rest + 1.0], [-sin, none, rest], [none, sin, rest])
    return np.stack([np.tile(np.concatenate(p, axis=-1), (1, 2)) for p in parts]).astype(np.float32)


def solution(mesh):
    shard_axes = ('node', 'local')
    act_spec = P(shard_axes)
    param_spec = P(None, shard_axes)

    def device_step(x, y_cot, ln1_gain, ln1_bias, qkv_weight, qkv_bias, out_weight, out_bias,
                    ln2_gain, ln2_bias, up_weight, up_bias, down_weight, down_bias):
        d_model, rows = x.shape[2], out_weight.shape[1]
        flat = (x.shape[0] * x.shape[1], d_model)
        qkv_flat = (LAYERS, rows, 3 * d_model)
        matrices = (qkv_weight.reshape(qkv_flat), out_weight, up_weight, down_weight)
        vectors = (ln1_gain, ln1_bias, qkv_bias, out_bias, ln2_gain, ln2_bias, up_bias, down_bias)
        sums = step_call(x.reshape(flat), y_cot.reshape(flat), matrices, vectors, rope_table(x.shape[1], qkv_weight.shape[3] // 12))
        shapes = [flat, flat, ln1_gain.shape, ln1_bias.shape, qkv_flat, qkv_bias.shape, out_weight.shape, out_bias.shape,
                  ln2_gain.shape, ln2_bias.shape, up_weight.shape, up_bias.shape, down_weight.shape, down_bias.shape]
        outs = list(finish_call(*sums, shapes))
        outs[0], outs[1], outs[4] = outs[0].reshape(x.shape), outs[1].reshape(x.shape), outs[4].reshape(qkv_weight.shape)
        return tuple(outs)

    return jax.shard_map(device_step, mesh=mesh,
                         in_specs=(act_spec, act_spec) + (param_spec,) * 12,
                         out_specs=(act_spec, act_spec) + (param_spec,) * 12,
                         check_vma=False)
```
